32 devices in a mesh: pairs: 16 (over z, y, x), side: 2 (over core).
Axes of the slice: x: 2, y: 2, z: 4, core: 2. Of those that a mesh axis runs over, the one named last changes fastest.
Arguments:
- features: bfloat16 [16, 196, 768], P('pairs', None, 'side'), may hold values from -6 to 6
- image_slot: int32 [16], replicated, may hold values from 0 to 15, as said below
- slot_images: int32 [48, 2], P('pairs'), may hold values from 0 to 15, as said below
- slot_count: int32 [16], P('pairs'), may hold values from 1 to 3, as said below
- gain_self: float32 [2, 768], P('side'), may hold values from 0.5 to 1.5
- gain_query: float32 [2, 768], P('side'), may hold values from 0.5 to 1.5
- gain_memory: float32 [2, 768], P('side'), may hold values from 0.5 to 1.5
- gain_mlp: float32 [2, 768], P('side'), may hold values from 0.5 to 1.5
- gain_head: float32 [2, 768], P('side'), may hold values from 0.5 to 1.5
- w_qkv: bfloat16 [2, 768, 2304], P('side'), may hold values from -0.21875 to 0.21875
- w_self_out: bfloat16 [2, 768, 768], P('side'), may hold values from -0.21875 to 0.21875
- w_query: bfloat16 [2, 768, 768], P('side'), may hold values from -0.21875 to 0.21875
- w_memory: bfloat16 [2, 768, 1536], P('side'), may hold values from -0.21875 to 0.21875
- w_cross_out: bfloat16 [2, 768, 768], P('side'), may hold values from -0.21875 to 0.21875
- w_fc1: bfloat16 [2, 3072, 768], P('side', 'pairs'), may hold values from -0.21875 to 0.21875
- w_fc2: bfloat16 [2, 3072, 768], P('side', 'pairs'), may hold values from -0.109375 to 0.109375
- w_head: bfloat16 [2, 768, 1024], P('side'), may hold values from -0.21875 to 0.21875
Outputs:
- merged_points: bfloat16 [16, 196, 768], P('pairs', None, 'side')
The draws below stay inside these ranges and needn't reach their ends.
Inputs may be any that keep to these rules, and one draw needn't show every extreme that they name: A permutation: image i is storage row image_slot[i] of features, held by device image_slot[i] // 1 of pairs. `slot_images`: slot j belongs to device j // 3 of pairs; its two images are distinct, and each is held by device (j // 3 + k) mod the size of pairs for some 0 <= k < 4; k = 3 occurs. `slot_count`: the counts sum to 32; 3 is reached on a quarter of the devices.
All inputs are finite; a program needn't handle non-finite values.
Results may differ from the reference program's by a relative error of at most 0.015.
Values may be sent and summed in bfloat16 or wider, within the bound.
A program may use at most 128 MiB of HBM per device.

```python
import jax
import jax.numpy as jnp
from jax import lax

D = 768
HEADS = 12
FF = 3072
HEAD_DIM = 64
TOKI = 196
PIXELS = 256
WINDOW = 4
IMG_DEV = 1
PAIR_DEV = 2
PAIR_MAX = 3
IMAGES = 16
SLOTS = 48


def routing_tables(key):
    n_dev = IMAGES // IMG_DEV
    keys = jax.random.split(jax.random.fold_in(key, 31), 4)
    image_slot = jax.random.permutation(keys[0], IMAGES).astype(jnp.int32)
    row_image = jnp.zeros((IMAGES,), jnp.int32).at[image_slot].set(jnp.arange(IMAGES, dtype=jnp.int32))
    order = jax.random.permutation(keys[1], n_dev).astype(jnp.int32)
    ranking = jnp.zeros((n_dev,), jnp.int32).at[order].set(jnp.arange(n_dev, dtype=jnp.int32))
    quarter = n_dev // 4
    halfway = PAIR_DEV // 2
    counts = PAIR_DEV + jnp.where(ranking < quarter, halfway, 0) - jnp.where((ranking >= quarter) & (ranking < 2 * quarter), halfway, 0)
    offsets = jax.random.randint(keys[2], (SLOTS, 2), 0, WINDOW).astype(jnp.int32)
    offsets = offsets.at[0, 0].set(WINDOW - 1)
    within = jax.random.randint(keys[3], (SLOTS, 2), 0, IMG_DEV).astype(jnp.int32)
    clash = (offsets[:, 0] == offsets[:, 1]) & (within[:, 0] == within[:, 1])
    second = jnp.where(clash, (offsets[:, 1] + 1) % WINDOW, offsets[:, 1])
    offsets = jnp.stack([offsets[:, 0], second], axis=1)
    device = (jnp.arange(SLOTS, dtype=jnp.int32) // PAIR_MAX)[:, None]
    holder = (device + offsets) % n_dev
    slot_images = row_image[holder * IMG_DEV + within]
    return (image_slot, slot_images.astype(jnp.int32), counts.astype(jnp.int32))


def draw_image_slot(key, part):
    return routing_tables(key)[0]


def draw_slot_images(key, part):
    return routing_tables(key)[1]


def draw_slot_count(key, part):
    return routing_tables(key)[2]


def shard_levels(stream_key, dims, pieces, least, top_value):
    loudness = 1.0
    for dim, blocks in pieces:
        draws = jax.random.uniform(jax.random.fold_in(jax.random.fold_in(stream_key, 6), dim), (blocks,), jnp.float32, least / len(pieces), top_value / len(pieces))
        loudness = loudness * jnp.repeat(jnp.exp(draws), dims[dim] // blocks).reshape((-1,) + (1,) * (len(dims) - 1 - dim))
    return loudness


def bell_draw(rng, extent, width, limit, cuts=(), kind=jnp.bfloat16):
    entries = width * jax.random.normal(rng, extent, jnp.float32)
    if cuts:
        entries = entries * shard_levels(rng, extent, cuts, -0.22, 0.18)
    return jnp.clip(entries, -limit, limit).astype(kind)


def setup_inputs(seed: int = 0) -> dict:
    key_list = jax.random.split(jax.random.key(seed), 18)
    features = bell_draw(key_list[0], (IMAGES, TOKI, D), 1.0, 6.0, ((0, 16), (2, 2)))
    image_slot = draw_image_slot(jax.random.fold_in(key_list[17], 71), 0)
    slot_images = draw_slot_images(jax.random.fold_in(key_list[17], 71), 0)
    slot_count = draw_slot_count(jax.random.fold_in(key_list[17], 71), 0)
    gain_self = jnp.clip(1.0 + 0.1 * jax.random.normal(key_list[4], (2, D), jnp.float32), 0.5, 1.5)
    gain_query = jnp.clip(1.0 + 0.1 * jax.random.normal(key_list[5], (2, D), jnp.float32), 0.5, 1.5)
    gain_memory = jnp.clip(1.0 + 0.1 * jax.random.normal(key_list[6], (2, D), jnp.float32), 0.5, 1.5)
    gain_mlp = jnp.clip(1.0 + 0.1 * jax.random.normal(key_list[7], (2, D), jnp.float32), 0.5, 1.5)
    gain_head = jnp.clip(1.0 + 0.1 * jax.random.normal(key_list[8], (2, D), jnp.float32), 0.5, 1.5)
    w_qkv = bell_draw(key_list[9], (2, D, 3 * D), D ** -0.5, 0.21875, ((0, 2),))
    w_self_out = bell_draw(key_list[10], (2, D, D), D ** -0.5, 0.21875, ((0, 2),))
    w_query = bell_draw(key_list[11], (2, D, D), D ** -0.5, 0.21875, ((0, 2),))
    w_memory = bell_draw(key_list[12], (2, D, 2 * D), D ** -0.5, 0.21875, ((0, 2),))
    w_cross_out = bell_draw(key_list[13], (2, D, D), D ** -0.5, 0.21875, ((0, 2),))
    w_fc1 = bell_draw(key_list[14], (2, FF, D), D ** -0.5, 0.21875, ((0, 2), (1, 16)))
    w_fc2 = bell_draw(key_list[15], (2, FF, D), FF ** -0.5, 0.109375, ((0, 2), (1, 16)))
    w_head = bell_draw(key_list[16], (2, D, 4 * PIXELS), D ** -0.5, 0.21875, ((0, 2),))
    return dict(features=features, image_slot=image_slot, slot_images=slot_images, slot_count=slot_count, gain_self=gain_self, gain_query=gain_query, gain_memory=gain_memory, gain_mlp=gain_mlp, gain_head=gain_head, w_qkv=w_qkv, w_self_out=w_self_out, w_query=w_query, w_memory=w_memory, w_cross_out=w_cross_out, w_fc1=w_fc1, w_fc2=w_fc2, w_head=w_head)


def layer_norm(values, gain):
    center = values - lax.optimization_barrier(jnp.mean(values, axis=-1, keepdims=True))
    spread = lax.optimization_barrier(jnp.mean(center * center, axis=-1, keepdims=True))
    return center * lax.rsqrt(spread + 1e-06) * gain

def attend(queries, key_rows, value_rows):
    length = queries.shape[0]
    key_len = key_rows.shape[0]
    q_heads = queries.astype(jnp.float32).reshape(length, HEADS, HEAD_DIM)
    k_heads = key_rows.astype(jnp.float32).reshape(key_len, HEADS, HEAD_DIM)
    v_heads = value_rows.astype(jnp.float32).reshape(key_len, HEADS, HEAD_DIM)
    scores = jnp.einsum('qhd,khd->hqk', q_heads, k_heads) * HEAD_DIM ** (-0.5)
    expon = jnp.exp(scores)
    weights = (expon / lax.optimization_barrier(jnp.sum(expon, axis=-1, keepdims=True))).astype(jnp.bfloat16)
    mixed = jnp.einsum('hqk,khd->qhd', weights.astype(jnp.float32), v_heads)
    return mixed.astype(jnp.bfloat16).reshape(length, D)

def decode(tokens, memory, gains, mats):
    g_self, g_query, g_memory, g_mlp, g_head = gains
    m_qkv, m_self_out, m_query, m_memory, m_cross_out, m_fc_in, m_fc_out, m_head = mats
    hidden = layer_norm(tokens.astype(jnp.float32), g_self).astype(jnp.bfloat16)
    triple = jnp.dot(hidden, m_qkv, preferred_element_type=jnp.float32).astype(jnp.bfloat16)
    attended = attend(triple[:, :D], triple[:, D:2 * D], triple[:, 2 * D:])
    first = tokens.astype(jnp.float32) + jnp.dot(attended, m_self_out, preferred_element_type=jnp.float32)
    query_in = layer_norm(first, g_query).astype(jnp.bfloat16)
    memory_in = layer_norm(memory.astype(jnp.float32), g_memory).astype(jnp.bfloat16)
    queries = jnp.dot(query_in, m_query, preferred_element_type=jnp.float32).astype(jnp.bfloat16)
    key_value = jnp.dot(memory_in, m_memory, preferred_element_type=jnp.float32).astype(jnp.bfloat16)
    crossed = attend(queries, key_value[:, :D], key_value[:, D:])
    second = first + jnp.dot(crossed, m_cross_out, preferred_element_type=jnp.float32)
    mlp_in = layer_norm(second, g_mlp).astype(jnp.bfloat16)
    pre_act = jnp.dot(mlp_in, m_fc_in.T, preferred_element_type=jnp.float32)
    activated = jax.nn.gelu(pre_act, approximate=False).astype(jnp.bfloat16)
    third = second + jnp.dot(activated, m_fc_out, preferred_element_type=jnp.float32)
    final = layer_norm(third, g_head).astype(jnp.bfloat16)
    return jnp.dot(final, m_head, preferred_element_type=jnp.float32)

def map_terms(raw):
    lead = raw.shape[:-1]
    parts = raw.reshape(lead + (2, 4, PIXELS // 2))
    conf = 1.0 + jnp.exp(parts[..., 3, :])
    joined = jnp.concatenate([conf[..., None, :] * parts[..., :3, :], conf[..., None, :]], axis=-2)
    return joined.reshape(lead + (4 * PIXELS,))

def reference(features, image_slot, slot_images, slot_count, gain_self, gain_query, gain_memory, gain_mlp, gain_head, w_qkv, w_self_out, w_query, w_memory, w_cross_out, w_fc1, w_fc2, w_head):
    gain_list = [gain_self, gain_query, gain_memory, gain_mlp, gain_head]
    mat_list = [w_qkv, w_self_out, w_query, w_memory, w_cross_out, w_fc1, w_fc2, w_head]

    def one_slot(sums, index):
        live = (index % PAIR_MAX < slot_count[index // PAIR_MAX]).astype(jnp.float32)
        stored = image_slot[slot_images[index]].astype(jnp.int32)
        views = [lax.dynamic_index_in_dim(features, stored[which], 0, keepdims=False) for which in range(2)]
        for which in range(2):
            result = decode(views[which], views[1 - which], [g[which] for g in gain_list], [m[which] for m in mat_list])
            sums = sums.at[stored[which]].add(live * map_terms(result))
        return (sums, None)
    start = jnp.zeros((IMAGES, TOKI, 4 * PIXELS), jnp.float32)
    sums, _ = lax.scan(one_slot, start, jnp.arange(SLOTS, dtype=jnp.int32))
    parts = sums.reshape(IMAGES, TOKI, 2, 4, PIXELS // 2)
    merged = parts[:, :, :, :3] / jnp.maximum(parts[:, :, :, 3:], 1.0)
    return merged.reshape(IMAGES, TOKI, 3 * PIXELS).astype(jnp.bfloat16)
```

```python
import functools

import jax
import jax.numpy as jnp
from jax import lax
from jax.experimental import pallas as pl
from jax.experimental.pallas import tpu as pltpu
from jax.sharding import PartitionSpec as P

HEAD_DIM = 64
WINDOW = 4
PAIR = 2 * HEAD_DIM
BLOCKS = 4
REACH = WINDOW + 1
VMEM_LIMIT = 63 * 1024 * 1024
MESH = pl.DeviceIdType.MESH


def padded(rows):
    return -(-rows // 16) * 16


def layer_norm(values, gain):
    center = values - jnp.mean(values, axis=-1, keepdims=True)
    spread = jnp.mean(center * center, axis=-1, keepdims=True)
    return center * lax.rsqrt(spread + 1e-06) * gain


def matmul(left, right):
    return jnp.dot(left, right, preferred_element_type=jnp.float32)


def matmul_t(left, right):
    return lax.dot_general(
        left, right, (((1,), (1,)), ((), ())), preferred_element_type=jnp.float32
    )


def attend(q_ref, k_ref, v_ref, k_at, v_at, o_ref, width, comm):
    rows = q_ref.shape[0]
    low = lax.broadcasted_iota(jnp.int32, (rows, PAIR), 1) < HEAD_DIM
    for pair in range(width // PAIR):
        if pair * PAIR == width // 2:
            comm()
        q = q_ref[:, pair * PAIR : (pair + 1) * PAIR]
        k = k_ref[:, k_at + pair * PAIR : k_at + (pair + 1) * PAIR]
        v = v_ref[:, v_at + pair * PAIR : v_at + (pair + 1) * PAIR]
        mixed = None
        for keep in (low, jnp.logical_not(low)):
            q_head = jnp.where(keep, q, jnp.zeros_like(q))
            v_head = jnp.where(keep, v, jnp.zeros_like(v))
            scores = matmul_t(q_head, k) * HEAD_DIM ** (-0.5)
            expon = jnp.exp(scores)
            weights = (expon / jnp.sum(expon, axis=-1, keepdims=True)).astype(jnp.bfloat16)
            part = matmul(weights, v_head)
            mixed = part if mixed is None else mixed + part
        o_ref[:, pair * PAIR : (pair + 1) * PAIR] = mixed.astype(jnp.bfloat16)


def remote(src, dst, send, recv, device):
    return pltpu.make_async_remote_copy(
        src_ref=src, dst_ref=dst, send_sem=send, recv_sem=recv, device_id=device,
        device_id_type=MESH,
    )


def decoder_kernel(
    image_slot, features, slot_images, slot_count,
    g_self, g_query, g_memory, g_mlp, g_head,
    w_qkv, w_self_out, w_query, w_memory, w_cross_out, w_fc1, w_fc2, w_head,
    out,
    win, table, counts, gains, m_qkv, m_self_out, m_query, m_memory, m_cross_out, m_head, ring_w,
    triple, kv, queries, mixed, second, hidden, raw, term, term_away, term_in, far_out, far_in,
    f_local, f_send, f_recv, fr_send, fr_recv, t_send, t_recv, g_send, g_recv, w_send, w_recv,
    s_send, r_send, r_recv, x_send, x_recv, a_send, a_recv, b_send, b_recv,
):
    devices = lax.axis_size("pairs")
    chips = devices // 2
    here = lax.axis_index("pairs")
    s = lax.axis_index("side")
    x = lax.rem(here, 2)
    q = lax.div(here, 2)
    rows = features.shape[1]
    width = m_qkv.shape[0]
    slots = second.shape[0]
    tall = second.shape[1]
    per = chips // BLOCKS
    shard = ring_w.shape[2]
    split = 2 if shard % 32 == 0 else 1
    kinds = 2 * split
    part = shard // split
    total_pieces = kinds * chips

    sibling = (here, 1 - s)
    partner = (2 * q + s, x)
    at_home = x == s

    def pair_of(step, flip):
        chip = lax.rem(q + (step + chips), chips)
        return 2 * chip + (1 - x if flip else x)

    up = jnp.where(
        lax.rem(q, 2) == 0,
        jnp.where(q + 2 < chips, q + 2, chips - 1),
        jnp.where(q >= 3, q - 2, 0),
    )
    down = jnp.where(
        lax.rem(q, 2) == 0,
        jnp.where(q == 0, 1, q - 2),
        jnp.where(q + 2 < chips, q + 2, chips - 2),
    )
    onward = (2 * jnp.where(s == 0, up, down) + x, s)

    mats = (
        (w_qkv, m_qkv), (w_self_out, m_self_out), (w_memory, m_memory), (w_query, m_query),
        (w_cross_out, m_cross_out),
    )
    half = w_head.shape[2] // 2
    weights = [(src.at[0], dst) for src, dst in mats]
    weights += [(w_head.at[0, :, h * half : (h + 1) * half], m_head.at[h]) for h in range(2)]
    gain_refs = (g_self, g_query, g_memory, g_mlp, g_head)
    fcs = (w_fc1, w_fc2)

    def slot_at(step, ring):
        return lax.div(step, per) * (2 * per) + ring * per + lax.rem(step, per)

    def ring_view(step, kind, ring):
        place = ring_w.at[lax.div(kind, split), slot_at(step, ring)]
        if split == 1:
            return place
        start = pl.multiple_of(lax.rem(kind, split) * part, part)
        return place.at[pl.ds(start, part)]

    def own_fc(kind):
        return fcs[kind // split].at[0, pl.ds((kind % split) * part, part)]

    own_win = pltpu.make_async_copy(features.at[0], win.at[x, s], f_local)
    own_win.start()

    @pl.when(at_home)
    def _():
        pltpu.make_async_copy(slot_images, table, t_recv.at[0]).start()
        pltpu.make_async_copy(slot_count, counts, t_recv.at[1]).start()
        for at, ref in enumerate(gain_refs):
            pltpu.make_async_copy(ref, gains.at[at], g_recv.at[at]).start()
        for kind in range(kinds):
            pltpu.make_async_copy(own_fc(kind), ring_view(0, kind, s), r_recv.at[0, kind]).start()
        for at, (src, dst) in enumerate(weights):
            pltpu.make_async_copy(src, dst, w_recv.at[at]).start()

    barrier = pltpu.get_barrier_semaphore()
    for step in range(-2, 3):
        for flip in range(2):
            if step or flip:
                pl.semaphore_signal(
                    barrier, inc=1, device_id=(pair_of(step, flip), s), device_id_type=MESH
                )
    pl.semaphore_signal(barrier, inc=1, device_id=sibling, device_id_type=MESH)

    @pl.when(jnp.logical_not(at_home))
    def _():
        pl.semaphore_signal(barrier, inc=1, device_id=partner, device_id_type=MESH)

    pl.semaphore_wait(barrier, 10 + (1 - at_home.astype(jnp.int32)))

    table_out = [
        remote(slot_images, table, t_send.at[0], t_recv.at[0], partner),
        remote(slot_count, counts, t_send.at[1], t_recv.at[1], partner),
    ]
    fc_out = [
        remote(own_fc(kind), ring_view(0, kind, x), s_send.at[kind], r_recv.at[0, kind], partner)
        for kind in range(kinds)
    ]
    gains_out = [
        remote(ref, gains.at[at], g_send.at[at], g_recv.at[at], sibling)
        for at, ref in enumerate(gain_refs)
    ]
    weights_out = [
        remote(src, dst, w_send.at[at], w_recv.at[at], sibling)
        for at, (src, dst) in enumerate(weights)
    ]

    def feature_out(step, flip):
        place = x + 2 * step
        return remote(
            features.at[0], win.at[place, s], f_send.at[2 * step + flip - 1], f_recv.at[place],
            (pair_of(-step, flip), s),
        )

    def relay(place):
        block = win.at[place, s]
        return remote(block, block, fr_send.at[place], fr_recv.at[place], sibling)

    @pl.when(jnp.logical_not(at_home))
    def _():
        for copy in table_out:
            copy.start()

    for step, flip in ((0, 1), (1, 0), (1, 1)):
        feature_out(step, flip).start()

    @pl.when(x == 0)
    def _():
        feature_out(2, 0).start()
        feature_out(2, 1).start()

    own_win.wait()
    relay(x).start()

    @pl.when(at_home)
    def _():
        for copy in gains_out:
            copy.start()
        weights_out[0].start()

    @pl.when(jnp.logical_not(at_home))
    def _():
        for copy in fc_out:
            copy.start()

    def piece(number):
        step, kind = lax.div(number, kinds), lax.rem(number, kinds)
        block = ring_view(step, kind, s)
        pltpu.make_async_copy(block, block, r_recv.at[step, kind]).wait()

        @pl.when(step < chips - 1)
        def _():
            remote(
                block, ring_view(step + 1, kind, s), r_send.at[step, kind],
                r_recv.at[step + 1, kind], onward,
            ).start()

        remote(block, block, x_send.at[step, kind], x_recv.at[step, kind], sibling).start()

    def pieces(low, high):
        def body(number, carry):
            piece(number)
            return carry

        lax.fori_loop(low, high, body, 0)

    pieces(0, kinds)

    @pl.when(at_home)
    def _():
        for copy in weights_out[1:]:
            copy.start()

    def arrived(place):
        block = win.at[place, s]
        pltpu.make_async_copy(block, block, f_recv.at[place]).wait()
        relay(place).start()

    arrived(1 - x)
    for place in range(2, REACH):
        arrived(place)
    early = 2 * kinds
    pieces(kinds, early)
    for place in range(REACH):
        block = win.at[place, 1 - s]
        pltpu.make_async_copy(block, block, fr_recv.at[place]).wait()
    pltpu.make_async_copy(slot_images, table, t_recv.at[0]).wait()
    pltpu.make_async_copy(slot_count, counts, t_recv.at[1]).wait()
    for at, ref in enumerate(gain_refs):
        pltpu.make_async_copy(ref, gains.at[at], g_recv.at[at]).wait()

    def weight_wait(at):
        src, dst = weights[at]
        pltpu.make_async_copy(src, dst, w_recv.at[at]).wait()

    def first_wait(slot, at):
        @pl.when(slot == 0)
        def _():
            weight_wait(at)

    def place_of(slot, column):
        stored = image_slot[table[slot, column]]
        ahead = lax.rem(stored - (2 * q + s) + devices, devices)
        return jnp.minimum(ahead, WINDOW - 1) + s

    def tokens_of(place):
        return jnp.concatenate([win[place, 0], win[place, 1]], axis=-1).astype(jnp.float32)

    stops = 6 * slots
    each = max((total_pieces * 26 // 32 - early) // stops, 0)
    fronted = early + each * stops

    def front(slot, carry):
        told = [0]

        def comm():
            base = early + (6 * slot + told[0]) * each
            told[0] += 1
            for at in range(each):
                piece(base + at)

        first_wait(slot, 0)
        tokens = tokens_of(place_of(slot, x))
        state = layer_norm(tokens, gains[0]).astype(jnp.bfloat16)
        triple[...] = matmul(state, m_qkv[...]).astype(jnp.bfloat16)
        comm()
        attend(triple, triple, triple, width, 2 * width, mixed, width, comm)
        first_wait(slot, 1)
        first = tokens + matmul(mixed[...], m_self_out[...])
        second[slot, 0:rows, :] = first
        comm()
        first_wait(slot, 2)
        first_wait(slot, 3)
        query_in = layer_norm(first, gains[1]).astype(jnp.bfloat16)
        memory = tokens_of(place_of(slot, 1 - x))
        memory_in = layer_norm(memory, gains[2]).astype(jnp.bfloat16)
        queries[...] = matmul(query_in, m_query[...]).astype(jnp.bfloat16)
        kv[...] = matmul(memory_in, m_memory[...]).astype(jnp.bfloat16)
        comm()
        attend(queries, kv, kv, 0, width, mixed, width, comm)
        first_wait(slot, 4)
        result = second[slot, 0:rows, :] + matmul(mixed[...], m_cross_out[...])
        second[slot, 0:rows, :] = result
        hidden[slot, 0:rows, :] = layer_norm(result, gains[3]).astype(jnp.bfloat16)
        comm()
        return carry

    second[...] = jnp.zeros_like(second)
    hidden[...] = jnp.zeros_like(hidden)
    lax.fori_loop(0, slots, front, 0)

    def relayed(block):
        def body(at, carry):
            step, kind = block * per + lax.div(at, kinds), lax.rem(at, kinds)
            view = ring_view(step, kind, 1 - s)
            pltpu.make_async_copy(view, view, x_recv.at[step, kind]).wait()
            return carry

        lax.fori_loop(0, per * kinds, body, 0)

    def expand(block, slot):
        wide = 2 * per * shard
        if shard % 16 == 0:
            fc1 = ring_w[0, pl.ds(block * 2 * per, 2 * per)].reshape(wide, width)
            fc2 = ring_w[1, pl.ds(block * 2 * per, 2 * per)].reshape(wide, width)
            groups = [(fc1, fc2)]
        else:
            groups = [
                (ring_w[0, block * 2 * per + at], ring_w[1, block * 2 * per + at])
                for at in range(2 * per)
            ]
        total = second[slot]
        for fc1, fc2 in groups:
            pre = matmul_t(hidden[slot], fc1)
            act = (pre * (1.0 + lax.erf(pre * 0.5**0.5)) * 0.5).astype(jnp.bfloat16)
            total = total + matmul(act, fc2)
        second[slot] = total

    left = total_pieces - fronted
    places = (BLOCKS - 1) * slots

    def expand_early(turn, carry):
        block, slot = lax.div(turn, slots), lax.rem(turn, slots)

        @pl.when(slot == 0)
        def _():
            relayed(block)

        expand(block, slot)
        pieces(fronted + lax.div(turn * left, places), fronted + lax.div((turn + 1) * left, places))
        return carry

    lax.fori_loop(0, places, expand_early, 0)
    relayed(BLOCKS - 1)

    def expand_last(slot, carry):
        expand(BLOCKS - 1, slot)
        hidden[slot] = layer_norm(second[slot], gains[4]).astype(jnp.bfloat16)
        return carry

    lax.fori_loop(0, slots, expand_last, 0)
    weight_wait(5)
    weight_wait(6)
    pix = half // 4

    def terms(which, target):
        for slot in range(slots):
            raw[slot] = matmul(hidden[slot], m_head[which])
        own = [place_of(slot, x) for slot in range(slots)]
        live = [slot < counts[0] for slot in range(slots)]
        for slot in range(slots):
            raw[slot, :, 3 * pix :] = 1.0 + jnp.exp(raw[slot, :, 3 * pix :])
        for comp in range(4):
            at = slice(comp * pix, (comp + 1) * pix)
            for place in range(REACH):
                sums = jnp.zeros((rows, pix), jnp.float32)
                for slot in range(slots):
                    conf = raw[slot, 0:rows, 3 * pix :]
                    value = conf if comp == 3 else conf * raw[slot, 0:rows, at]
                    chosen = jnp.logical_and(own[slot] == place, live[slot])
                    sums = sums + jnp.where(chosen, value, 0.0)
                target[place, :, at] = sums.astype(target.dtype)

    terms(1 - s, term_away)
    away = remote(term_away, term_in, a_send, a_recv, sibling)
    away.start()
    terms(s, term)
    away.wait_recv()

    def far_copy(place):
        step, to = place // 2, place % 2
        other = jnp.where(x == to, 0, 1)
        chip = lax.rem(q + step, chips)
        return remote(
            far_out.at[place], far_in.at[2 * step + other], b_send.at[place],
            b_recv.at[2 * step + other], (2 * chip + to, s),
        )

    for place in reversed(range(REACH)):
        joined = term[place] + term_in[place].astype(jnp.float32)
        if place < 2:
            term[place] = joined
        far_out[place] = joined.astype(jnp.bfloat16)
        if place < 2:

            @pl.when(x != place)
            def _(place=place):
                far_copy(place).start()

        else:
            far_copy(place).start()

    def far_wait(at):
        block = far_in.at[at]
        pltpu.make_async_copy(block, block, b_recv.at[at]).wait()

    total = term[x]
    for at in (1, 2, 3):
        far_wait(at)
        total = total + far_in[at].astype(jnp.float32)
    term[2] = total

    @pl.when(x == 0)
    def _():
        for at in (4, 5):
            far_wait(at)
        term[2] = term[2] + far_in[4].astype(jnp.float32) + far_in[5].astype(jnp.float32)

    conf = jnp.maximum(term[2, :, 3 * pix :], 1.0)
    for comp in range(3):
        at = slice(comp * pix, (comp + 1) * pix)
        out[0, :, at] = (term[2, :, at] / conf).astype(jnp.bfloat16)

    for step, flip in ((0, 1), (1, 0), (1, 1)):
        feature_out(step, flip).wait_send()

    @pl.when(x == 0)
    def _():
        feature_out(2, 0).wait_send()
        feature_out(2, 1).wait_send()

    for place in range(REACH):
        relay(place).wait_send()

    @pl.when(at_home)
    def _():
        for copy in gains_out + weights_out:
            copy.wait_send()

    @pl.when(jnp.logical_not(at_home))
    def _():
        for copy in table_out + fc_out:
            copy.wait_send()

    def drain(number, carry):
        step, kind = lax.div(number, kinds), lax.rem(number, kinds)
        block = ring_view(step, kind, s)

        @pl.when(step < chips - 1)
        def _():
            remote(
                block, block, r_send.at[step, kind], r_recv.at[step, kind], onward
            ).wait_send()

        remote(block, block, x_send.at[step, kind], x_recv.at[step, kind], sibling).wait_send()
        return carry

    lax.fori_loop(0, total_pieces, drain, 0)
    away.wait_send()
    for place in range(REACH):
        if place < 2:

            @pl.when(x != place)
            def _(place=place):
                far_copy(place).wait_send()

        else:
            far_copy(place).wait_send()


def on_device(
    features, image_slot, slot_images, slot_count, gain_self, gain_query, gain_memory, gain_mlp,
    gain_head, w_qkv, w_self_out, w_query, w_memory, w_cross_out, w_fc1, w_fc2, w_head,
):
    devices = lax.axis_size("pairs")
    chips = devices // 2
    blocks, rows, part = features.shape
    if blocks != 1 or chips % BLOCKS:
        raise ValueError("unsupported split")
    width = w_qkv.shape[1]
    slots = slot_images.shape[0]
    tall = padded(rows)
    shard = w_fc1.shape[1]
    kinds = 2 * (2 if shard % 32 == 0 else 1)
    half = w_head.shape[2] // 2
    bf16, f32 = jnp.bfloat16, jnp.float32
    dma = pltpu.SemaphoreType.DMA
    anywhere = pl.BlockSpec(memory_space=pl.ANY)
    return pl.pallas_call(
        decoder_kernel,
        out_shape=jax.ShapeDtypeStruct((1, rows, half * 3 // 4), bf16),
        in_specs=[pl.BlockSpec(memory_space=pltpu.SMEM)] + [anywhere] * 16,
        out_specs=pl.BlockSpec(memory_space=pltpu.VMEM),
        scratch_shapes=[
            pltpu.VMEM((REACH, 2, rows, part), bf16),
            pltpu.SMEM(slot_images.shape, jnp.int32),
            pltpu.SMEM(slot_count.shape, jnp.int32),
            pltpu.VMEM((5, 1, width), f32),
            pltpu.VMEM(w_qkv.shape[1:], bf16),
            pltpu.VMEM(w_self_out.shape[1:], bf16),
            pltpu.VMEM(w_query.shape[1:], bf16),
            pltpu.VMEM(w_memory.shape[1:], bf16),
            pltpu.VMEM(w_cross_out.shape[1:], bf16),
            pltpu.VMEM((2, width, half), bf16),
            pltpu.VMEM((2, devices, shard, width), bf16),
            pltpu.VMEM((rows, 3 * width), bf16),
            pltpu.VMEM((rows, 2 * width), bf16),
            pltpu.VMEM((rows, width), bf16),
            pltpu.VMEM((rows, width), bf16),
            pltpu.VMEM((slots, tall, width), f32),
            pltpu.VMEM((slots, tall, width), bf16),
            pltpu.VMEM((slots, tall, half), f32),
            pltpu.VMEM((REACH, rows, half), f32),
            pltpu.VMEM((REACH, rows, half), bf16),
            pltpu.VMEM((REACH, rows, half), bf16),
            pltpu.VMEM((REACH, rows, half), bf16),
            pltpu.VMEM((REACH + 1, rows, half), bf16),
            dma, dma((5,)), dma((REACH,)), dma((REACH,)), dma((REACH,)),
            dma((2,)), dma((2,)), dma((5,)), dma((5,)), dma((7,)), dma((7,)),
            dma((kinds,)), dma((chips, kinds)), dma((chips, kinds)), dma((chips, kinds)),
            dma((chips, kinds)), dma, dma, dma((REACH,)), dma((REACH + 1,)),
        ],
        compiler_params=pltpu.CompilerParams(
            collective_id=0, has_side_effects=True, vmem_limit_bytes=VMEM_LIMIT
        ),
    )(
        image_slot, features, slot_images, slot_count, gain_self, gain_query, gain_memory,
        gain_mlp, gain_head, w_qkv, w_self_out, w_query, w_memory, w_cross_out, w_fc1, w_fc2,
        w_head,
    )


def solution(mesh):
    placed = (
        P("pairs", None, "side"),
        P(),
        P("pairs", None),
        P("pairs"),
        P("side", None),
        P("side", None),
        P("side", None),
        P("side", None),
        P("side", None),
        P("side", None, None),
        P("side", None, None),
        P("side", None, None),
        P("side", None, None),
        P("side", None, None),
        P("side", "pairs", None),
        P("side", "pairs", None),
        P("side", None, None),
    )
    return jax.shard_map(
        on_device, mesh=mesh, in_specs=placed, out_specs=P("pairs", None, "side"), check_vma=False
    )
```

```python
import functools

import jax
import jax.numpy as jnp
from jax import lax
from jax.experimental import pallas as pl
from jax.experimental.pallas import tpu as pltpu
from jax.sharding import PartitionSpec as P

HEAD_DIM = 64
WINDOW = 4
PAIR = 2 * HEAD_DIM
BLOCKS = 4
REACH = WINDOW + 1
VMEM_LIMIT = 63 * 1024 * 1024
MESH = pl.DeviceIdType.MESH


def padded(rows):
    return -(-rows // 16) * 16


def layer_norm(values, gain):
    center = values - jnp.mean(values, axis=-1, keepdims=True)
    spread = jnp.mean(center * center, axis=-1, keepdims=True)
    return center * lax.rsqrt(spread + 1e-06) * gain


def matmul(left, right):
    return jnp.dot(left, right, preferred_element_type=jnp.float32)


def matmul_t(left, right):
    return lax.dot_general(
        left, right, (((1,), (1,)), ((), ())), preferred_element_type=jnp.float32
    )


def attend(q_ref, k_ref, v_ref, k_at, v_at, o_ref, width, comm):
    rows = q_ref.shape[0]
    low = lax.broadcasted_iota(jnp.int32, (rows, PAIR), 1) < HEAD_DIM
    for pair in range(width // PAIR):
        if pair * PAIR == width // 2:
            comm()
        q = q_ref[:, pair * PAIR : (pair + 1) * PAIR]
        k = k_ref[:, k_at + pair * PAIR : k_at + (pair + 1) * PAIR]
        v = v_ref[:, v_at + pair * PAIR : v_at + (pair + 1) * PAIR]
        mixed = None
        for keep in (low, jnp.logical_not(low)):
            q_head = jnp.where(keep, q, jnp.zeros_like(q))
            v_head = jnp.where(keep, v, jnp.zeros_like(v))
            scores = matmul_t(q_head, k) * HEAD_DIM ** (-0.5)
            expon = jnp.exp(scores)
            weights = (expon / jnp.sum(expon, axis=-1, keepdims=True)).astype(jnp.bfloat16)
            part = matmul(weights, v_head)
            mixed = part if mixed is None else mixed + part
        o_ref[:, pair * PAIR : (pair + 1) * PAIR] = mixed.astype(jnp.bfloat16)


def remote(src, dst, send, recv, device):
    return pltpu.make_async_remote_copy(
        src_ref=src, dst_ref=dst, send_sem=send, recv_sem=recv, device_id=device,
        device_id_type=MESH,
    )


def decoder_kernel(
    image_slot, slot_images, slot_count, features,
    g_self, g_query, g_memory, g_mlp, g_head,
    w_qkv, w_self_out, w_query, w_memory, w_cross_out, w_fc1, w_fc2, w_head,
    out,
    win, table, counts, gains, m_qkv, m_self_out, m_query, m_memory, m_cross_out, m_head, ring_w,
    triple, kv, queries, mixed, second, hidden, raw, term, term_away, term_in, far_out, far_in,
    f_local, f_send, f_recv, fr_send, fr_recv, t_send, t_recv, g_send, g_recv, w_send, w_recv,
    s_send, r_send, r_recv, x_send, x_recv, a_send, a_recv, b_send, b_recv,
):
    devices = lax.axis_size("pairs")
    chips = devices // 2
    here = lax.axis_index("pairs")
    s = lax.axis_index("side")
    x = lax.rem(here, 2)
    q = lax.div(here, 2)
    rows = features.shape[1]
    width = m_qkv.shape[0]
    slots = second.shape[0]
    tall = second.shape[1]
    per = chips // BLOCKS
    shard = ring_w.shape[2]
    split = 2 if shard % 32 == 0 else 1
    kinds = 2 * split
    rank = shard // split
    total_pieces = kinds * chips

    sibling = (here, 1 - s)
    partner = (2 * q + s, x)
    at_home = x == s

    def pair_of(step, flip):
        chip = lax.rem(q + (step + chips), chips)
        return 2 * chip + (1 - x if flip else x)

    up = jnp.where(
        lax.rem(q, 2) == 0,
        jnp.where(q + 2 < chips, q + 2, chips - 1),
        jnp.where(q >= 3, q - 2, 0),
    )
    down = jnp.where(
        lax.rem(q, 2) == 0,
        jnp.where(q == 0, 1, q - 2),
        jnp.where(q + 2 < chips, q + 2, chips - 2),
    )
    onward = (2 * jnp.where(s == 0, up, down) + x, s)

    mats = (
        (w_qkv, m_qkv), (w_self_out, m_self_out), (w_memory, m_memory), (w_query, m_query),
        (w_cross_out, m_cross_out),
    )
    half = w_head.shape[2] // 2
    weights = [(src.at[0], dst) for src, dst in mats]
    weights += [(w_head.at[0, :, h * half : (h + 1) * half], m_head.at[h]) for h in range(2)]
    gain_refs = (g_self, g_query, g_memory, g_mlp, g_head)
    fcs = (w_fc1, w_fc2)

    def slot_at(step, ring):
        return lax.div(step, per) * (2 * per) + ring * per + lax.rem(step, per)

    def ring_view(step, kind, ring):
        place = ring_w.at[lax.rem(kind, 2), slot_at(step, ring)]
        if split == 1:
            return place
        return place.at[pl.ds(pl.multiple_of(lax.div(kind, 2) * rank, rank), rank)]

    def own_fc(which, piece):
        if split == 1:
            return fcs[which].at[0]
        return fcs[which].at[0, pl.ds(pl.multiple_of(piece * rank, rank), rank)]

    own_win = pltpu.make_async_copy(features.at[0], win.at[x, s], f_local)
    own_win.start()

    @pl.when(at_home)
    def _():
        for slot in range(slots):
            for column in range(2):
                table[slot, column] = slot_images[slot, column]
        counts[0] = slot_count[0]
        for at, ref in enumerate(gain_refs):
            pltpu.make_async_copy(ref, gains.at[at], g_recv.at[at]).start()
        for which in range(2):
            pltpu.make_async_copy(
                own_fc(which, s), ring_view(0, which, s), r_recv.at[0, which]
            ).start()
        for at, (src, dst) in enumerate(weights):
            pltpu.make_async_copy(src, dst, w_recv.at[at]).start()

    barrier = pltpu.get_barrier_semaphore()
    for step in range(-2, 3):
        for flip in range(2):
            if step or flip:
                pl.semaphore_signal(
                    barrier, inc=1, device_id=(pair_of(step, flip), s), device_id_type=MESH
                )
    pl.semaphore_signal(barrier, inc=1, device_id=sibling, device_id_type=MESH)

    @pl.when(jnp.logical_not(at_home))
    def _():
        pl.semaphore_signal(barrier, inc=1, device_id=partner, device_id_type=MESH)

    pl.semaphore_wait(barrier, 10 + (1 - at_home.astype(jnp.int32)))

    table_out = [
        remote(slot_images, table, t_send.at[0], t_recv.at[0], partner),
        remote(slot_count, counts, t_send.at[1], t_recv.at[1], partner),
    ]
    across = (2 * q + s, s)
    if split == 1:
        fc_home = []
        fc_out = [
            remote(own_fc(f, 0), ring_view(0, f, x), s_send.at[f], r_recv.at[0, f], partner)
            for f in range(2)
        ]
    else:
        fc_home = [
            remote(
                own_fc(f, 1 - s), ring_view(0, f, 1 - s), s_send.at[f], r_recv.at[0, f], sibling
            )
            for f in range(2)
        ]
        fc_out = [
            remote(
                own_fc(f, ring), ring_view(0, 2 + f, ring), s_send.at[2 * f + to],
                r_recv.at[0, 2 + f], device,
            )
            for f in range(2)
            for to, (ring, device) in enumerate(((x, partner), (s, across)))
        ]
    gains_out = [
        remote(ref, gains.at[at], g_send.at[at], g_recv.at[at], sibling)
        for at, ref in enumerate(gain_refs)
    ]
    weights_out = [
        remote(src, dst, w_send.at[at], w_recv.at[at], sibling)
        for at, (src, dst) in enumerate(weights)
    ]

    def feature_out(block, place, step, flip, at):
        return remote(
            block, win.at[place, s], f_send.at[at], f_recv.at[place], (pair_of(-step, flip), s)
        )

    own = features.at[0]
    passed = win.at[1 - x, s]
    feature_first = [feature_out(own, x, 0, 1, 0), feature_out(own, x + 2, 1, 0, 1)]
    feature_next = feature_out(passed, 3 - x, 1, 0, 2)
    far_own = feature_out(own, WINDOW, 2, 0, 3)
    far_passed = feature_out(passed, WINDOW, 2, 0, 3)

    def relay(place, block=None):
        target = win.at[place, s]
        return remote(
            target if block is None else block, target, fr_send.at[place], fr_recv.at[place],
            sibling,
        )

    for copy in feature_first:
        copy.start()

    @pl.when(x == 0)
    def _():
        far_own.start()

    relay(x, own).start()

    @pl.when(at_home)
    def _():
        for copy in fc_home + gains_out:
            copy.start()
        weights_out[0].start()

    @pl.when(jnp.logical_not(at_home))
    def _():
        for copy in table_out + fc_out:
            copy.start()

    def piece(number):
        step, kind = lax.div(number, kinds), lax.rem(number, kinds)
        block = ring_view(step, kind, s)
        pltpu.make_async_copy(block, block, r_recv.at[step, kind]).wait()

        @pl.when(step < chips - 1)
        def _():
            remote(
                block, ring_view(step + 1, kind, s), r_send.at[step, kind],
                r_recv.at[step + 1, kind], onward,
            ).start()

        remote(block, block, x_send.at[step, kind], x_recv.at[step, kind], sibling).start()

    def pieces(low, high):
        def body(number, carry):
            piece(number)
            return carry

        lax.fori_loop(low, high, body, 0)

    def arrived(place):
        block = win.at[place, s]
        pltpu.make_async_copy(block, block, f_recv.at[place]).wait()
        relay(place).start()

    pieces(0, kinds // 2)
    arrived(1 - x)
    feature_next.start()

    @pl.when(x == 1)
    def _():
        far_passed.start()

    arrived(2 + x)
    pieces(kinds // 2, kinds)
    arrived(3 - x)
    arrived(4)

    @pl.when(at_home)
    def _():
        for copy in weights_out[1:]:
            copy.start()

    early = 2 * kinds
    pieces(kinds, early)
    own_win.wait()
    for place in range(REACH):
        block = win.at[place, 1 - s]
        pltpu.make_async_copy(block, block, fr_recv.at[place]).wait()

    @pl.when(jnp.logical_not(at_home))
    def _():
        for copy in table_out:
            copy.wait_recv()

    for at, ref in enumerate(gain_refs):
        pltpu.make_async_copy(ref, gains.at[at], g_recv.at[at]).wait()

    def weight_wait(at):
        src, dst = weights[at]
        pltpu.make_async_copy(src, dst, w_recv.at[at]).wait()

    def first_wait(slot, at):
        @pl.when(slot == 0)
        def _():
            weight_wait(at)

    def place_of(slot, column):
        stored = image_slot[table[slot, column]]
        ahead = lax.rem(stored - (2 * q + s) + devices, devices)
        return jnp.minimum(ahead, WINDOW - 1) + s

    def tokens_of(place):
        return jnp.concatenate([win[place, 0], win[place, 1]], axis=-1).astype(jnp.float32)

    stops = 6 * slots
    each = max((total_pieces * 26 // 32 - early) // stops, 0)
    fronted = early + each * stops

    def front(slot, carry):
        told = [0]

        def comm():
            base = early + (6 * slot + told[0]) * each
            told[0] += 1
            for at in range(each):
                piece(base + at)

        first_wait(slot, 0)
        tokens = tokens_of(place_of(slot, x))
        state = layer_norm(tokens, gains[0]).astype(jnp.bfloat16)
        triple[...] = matmul(state, m_qkv[...]).astype(jnp.bfloat16)
        comm()
        attend(triple, triple, triple, width, 2 * width, mixed, width, comm)
        first_wait(slot, 1)
        first = tokens + matmul(mixed[...], m_self_out[...])
        second[slot, 0:rows, :] = first
        comm()
        first_wait(slot, 2)
        first_wait(slot, 3)
        query_in = layer_norm(first, gains[1]).astype(jnp.bfloat16)
        memory = tokens_of(place_of(slot, 1 - x))
        memory_in = layer_norm(memory, gains[2]).astype(jnp.bfloat16)
        queries[...] = matmul(query_in, m_query[...]).astype(jnp.bfloat16)
        kv[...] = matmul(memory_in, m_memory[...]).astype(jnp.bfloat16)
        comm()
        attend(queries, kv, kv, 0, width, mixed, width, comm)
        first_wait(slot, 4)
        result = second[slot, 0:rows, :] + matmul(mixed[...], m_cross_out[...])
        second[slot, 0:rows, :] = result
        hidden[slot, 0:rows, :] = layer_norm(result, gains[3]).astype(jnp.bfloat16)
        comm()
        return carry

    second[...] = jnp.zeros_like(second)
    hidden[...] = jnp.zeros_like(hidden)
    lax.fori_loop(0, slots, front, 0)

    def relayed(block):
        def body(at, carry):
            step, kind = block * per + lax.div(at, kinds), lax.rem(at, kinds)
            view = ring_view(step, kind, 1 - s)
            pltpu.make_async_copy(view, view, x_recv.at[step, kind]).wait()
            return carry

        lax.fori_loop(0, per * kinds, body, 0)

    def expand(block, slot):
        wide = 2 * per * shard
        if shard % 16 == 0:
            fc1 = ring_w[0, pl.ds(block * 2 * per, 2 * per)].reshape(wide, width)
            fc2 = ring_w[1, pl.ds(block * 2 * per, 2 * per)].reshape(wide, width)
            groups = [(fc1, fc2)]
        else:
            groups = [
                (ring_w[0, block * 2 * per + at], ring_w[1, block * 2 * per + at])
                for at in range(2 * per)
            ]
        total = second[slot]
        for fc1, fc2 in groups:
            pre = matmul_t(hidden[slot], fc1)
            act = (pre * (1.0 + lax.erf(pre * 0.5**0.5)) * 0.5).astype(jnp.bfloat16)
            total = total + matmul(act, fc2)
        second[slot] = total

    left = total_pieces - fronted
    places = (BLOCKS - 1) * slots

    def expand_early(turn, carry):
        block, slot = lax.div(turn, slots), lax.rem(turn, slots)

        @pl.when(slot == 0)
        def _():
            relayed(block)

        expand(block, slot)
        pieces(fronted + lax.div(turn * left, places), fronted + lax.div((turn + 1) * left, places))
        return carry

    lax.fori_loop(0, places, expand_early, 0)
    relayed(BLOCKS - 1)

    def expand_last(slot, carry):
        expand(BLOCKS - 1, slot)
        hidden[slot] = layer_norm(second[slot], gains[4]).astype(jnp.bfloat16)
        return carry

    lax.fori_loop(0, slots, expand_last, 0)
    weight_wait(5)
    weight_wait(6)
    pix = half // 4

    def terms(which, target):
        for slot in range(slots):
            raw[slot] = matmul(hidden[slot], m_head[which])
        own = [place_of(slot, x) for slot in range(slots)]
        live = [slot < counts[0] for slot in range(slots)]
        for slot in range(slots):
            raw[slot, :, 3 * pix :] = 1.0 + jnp.exp(raw[slot, :, 3 * pix :])
        for comp in range(4):
            at = slice(comp * pix, (comp + 1) * pix)
            for place in range(REACH):
                sums = jnp.zeros((rows, pix), jnp.float32)
                for slot in range(slots):
                    conf = raw[slot, 0:rows, 3 * pix :]
                    value = conf if comp == 3 else conf * raw[slot, 0:rows, at]
                    chosen = jnp.logical_and(own[slot] == place, live[slot])
                    sums = sums + jnp.where(chosen, value, 0.0)
                target[place, :, at] = sums.astype(target.dtype)

    terms(1 - s, term_away)
    away = remote(term_away, term_in, a_send, a_recv, sibling)
    away.start()
    terms(s, term)
    away.wait_recv()

    def far_copy(place):
        step, to = place // 2, place % 2
        other = jnp.where(x == to, 0, 1)
        chip = lax.rem(q + step, chips)
        return remote(
            far_out.at[place], far_in.at[2 * step + other], b_send.at[place],
            b_recv.at[2 * step + other], (2 * chip + to, s),
        )

    for place in reversed(range(REACH)):
        joined = term[place] + term_in[place].astype(jnp.float32)
        if place < 2:
            term[place] = joined
        far_out[place] = joined.astype(jnp.bfloat16)
        if place < 2:

            @pl.when(x != place)
            def _(place=place):
                far_copy(place).start()

        else:
            far_copy(place).start()

    def far_wait(at):
        block = far_in.at[at]
        pltpu.make_async_copy(block, block, b_recv.at[at]).wait()

    total = term[x]
    for at in (1, 2, 3):
        far_wait(at)
        total = total + far_in[at].astype(jnp.float32)
    term[2] = total

    @pl.when(x == 0)
    def _():
        for at in (4, 5):
            far_wait(at)
        term[2] = term[2] + far_in[4].astype(jnp.float32) + far_in[5].astype(jnp.float32)

    conf = jnp.maximum(term[2, :, 3 * pix :], 1.0)
    for comp in range(3):
        at = slice(comp * pix, (comp + 1) * pix)
        out[0, :, at] = (term[2, :, at] / conf).astype(jnp.bfloat16)

    for copy in feature_first + [feature_next, far_own]:
        copy.wait_send()

    for place in range(REACH):
        relay(place).wait_send()

    @pl.when(at_home)
    def _():
        for copy in fc_home + gains_out + weights_out:
            copy.wait_send()

    @pl.when(jnp.logical_not(at_home))
    def _():
        for copy in table_out + fc_out:
            copy.wait_send()

    def drain(number, carry):
        step, kind = lax.div(number, kinds), lax.rem(number, kinds)
        block = ring_view(step, kind, s)

        @pl.when(step < chips - 1)
        def _():
            remote(
                block, block, r_send.at[step, kind], r_recv.at[step, kind], onward
            ).wait_send()

        remote(block, block, x_send.at[step, kind], x_recv.at[step, kind], sibling).wait_send()
        return carry

    lax.fori_loop(0, total_pieces, drain, 0)
    away.wait_send()
    for place in range(REACH):
        if place < 2:

            @pl.when(x != place)
            def _(place=place):
                far_copy(place).wait_send()

        else:
            far_copy(place).wait_send()


def on_device(
    features, image_slot, slot_images, slot_count, gain_self, gain_query, gain_memory, gain_mlp,
    gain_head, w_qkv, w_self_out, w_query, w_memory, w_cross_out, w_fc1, w_fc2, w_head,
):
    devices = lax.axis_size("pairs")
    chips = devices // 2
    blocks, rows, part = features.shape
    if blocks != 1 or chips % BLOCKS:
        raise ValueError("unsupported split")
    width = w_qkv.shape[1]
    slots = slot_images.shape[0]
    tall = padded(rows)
    shard = w_fc1.shape[1]
    kinds = 2 * (2 if shard % 32 == 0 else 1)
    half = w_head.shape[2] // 2
    bf16, f32 = jnp.bfloat16, jnp.float32
    dma = pltpu.SemaphoreType.DMA
    anywhere = pl.BlockSpec(memory_space=pl.ANY)
    return pl.pallas_call(
        decoder_kernel,
        out_shape=jax.ShapeDtypeStruct((1, rows, half * 3 // 4), bf16),
        in_specs=[pl.BlockSpec(memory_space=pltpu.SMEM)] * 3 + [anywhere] * 14,
        out_specs=pl.BlockSpec(memory_space=pltpu.VMEM),
        scratch_shapes=[
            pltpu.VMEM((REACH, 2, rows, part), bf16),
            pltpu.SMEM(slot_images.shape, jnp.int32),
            pltpu.SMEM(slot_count.shape, jnp.int32),
            pltpu.VMEM((5, 1, width), f32),
            pltpu.VMEM(w_qkv.shape[1:], bf16),
            pltpu.VMEM(w_self_out.shape[1:], bf16),
            pltpu.VMEM(w_query.shape[1:], bf16),
            pltpu.VMEM(w_memory.shape[1:], bf16),
            pltpu.VMEM(w_cross_out.shape[1:], bf16),
            pltpu.VMEM((2, width, half), bf16),
            pltpu.VMEM((2, devices, shard, width), bf16),
            pltpu.VMEM((rows, 3 * width), bf16),
            pltpu.VMEM((rows, 2 * width), bf16),
            pltpu.VMEM((rows, width), bf16),
            pltpu.VMEM((rows, width), bf16),
            pltpu.VMEM((slots, tall, width), f32),
            pltpu.VMEM((slots, tall, width), bf16),
            pltpu.VMEM((slots, tall, half), f32),
            pltpu.VMEM((REACH, rows, half), f32),
            pltpu.VMEM((REACH, rows, half), bf16),
            pltpu.VMEM((REACH, rows, half), bf16),
            pltpu.VMEM((REACH, rows, half), bf16),
            pltpu.VMEM((REACH + 1, rows, half), bf16),
            dma, dma((5,)), dma((REACH,)), dma((REACH,)), dma((REACH,)),
            dma((2,)), dma((2,)), dma((5,)), dma((5,)), dma((7,)), dma((7,)),
            dma((kinds,)), dma((chips, kinds)), dma((chips, kinds)), dma((chips, kinds)),
            dma((chips, kinds)), dma, dma, dma((REACH,)), dma((REACH + 1,)),
        ],
        compiler_params=pltpu.CompilerParams(
            collective_id=0, has_side_effects=True, vmem_limit_bytes=VMEM_LIMIT
        ),
    )(
        image_slot, slot_images, slot_count, features, gain_self, gain_query, gain_memory,
        gain_mlp, gain_head, w_qkv, w_self_out, w_query, w_memory, w_cross_out, w_fc1, w_fc2,
        w_head,
    )


def solution(mesh):
    placed = (
        P("pairs", None, "side"),
        P(),
        P("pairs", None),
        P("pairs"),
        P("side", None),
        P("side", None),
        P("side", None),
        P("side", None),
        P("side", None),
        P("side", None, None),
        P("side", None, None),
        P("side", None, None),
        P("side", None, None),
        P("side", None, None),
        P("side", "pairs", None),
        P("side", "pairs", None),
        P("side", None, None),
    )
    return jax.shard_map(
        on_device, mesh=mesh, in_specs=placed, out_specs=P("pairs", None, "side"), check_vma=False
    )
```

```python
import functools

import jax
import jax.numpy as jnp
from jax import lax
from jax.experimental import pallas as pl
from jax.experimental.pallas import tpu as pltpu
from jax.sharding import PartitionSpec as P

HEAD_DIM = 64
WINDOW = 4
PAIR = 2 * HEAD_DIM
BLOCKS = 4
REACH = WINDOW + 1
VMEM_LIMIT = 63 * 1024 * 1024
MESH = pl.DeviceIdType.MESH


def padded(rows):
    return -(-rows // 16) * 16


def layer_norm(values, gain):
    center = values - jnp.mean(values, axis=-1, keepdims=True)
    spread = jnp.mean(center * center, axis=-1, keepdims=True)
    return center * lax.rsqrt(spread + 1e-06) * gain


def matmul(left, right):
    return jnp.dot(left, right, preferred_element_type=jnp.float32)


def matmul_t(left, right):
    return lax.dot_general(
        left, right, (((1,), (1,)), ((), ())), preferred_element_type=jnp.float32
    )


def attend(q_ref, k_ref, v_ref, k_at, v_at, o_ref, width, comm):
    rows = q_ref.shape[0]
    low = lax.broadcasted_iota(jnp.int32, (rows, PAIR), 1) < HEAD_DIM
    for pair in range(width // PAIR):
        if pair * PAIR == width // 2:
            comm()
        q = q_ref[:, pair * PAIR : (pair + 1) * PAIR]
        k = k_ref[:, k_at + pair * PAIR : k_at + (pair + 1) * PAIR]
        v = v_ref[:, v_at + pair * PAIR : v_at + (pair + 1) * PAIR]
        mixed = None
        for keep in (low, jnp.logical_not(low)):
            q_head = jnp.where(keep, q, jnp.zeros_like(q))
            v_head = jnp.where(keep, v, jnp.zeros_like(v))
            scores = matmul_t(q_head, k) * HEAD_DIM ** (-0.5)
            expon = jnp.exp(scores)
            weights = (expon / jnp.sum(expon, axis=-1, keepdims=True)).astype(jnp.bfloat16)
            part = matmul(weights, v_head)
            mixed = part if mixed is None else mixed + part
        o_ref[:, pair * PAIR : (pair + 1) * PAIR] = mixed.astype(jnp.bfloat16)


def remote(src, dst, send, recv, device):
    return pltpu.make_async_remote_copy(
        src_ref=src, dst_ref=dst, send_sem=send, recv_sem=recv, device_id=device,
        device_id_type=MESH,
    )


def decoder_kernel(
    image_slot, slot_images, slot_count, features,
    g_self, g_query, g_memory, g_mlp, g_head,
    w_qkv, w_self_out, w_query, w_memory, w_cross_out, w_fc1, w_fc2, w_head,
    out,
    win, table, counts, gains, m_qkv, m_self_out, m_query, m_memory, m_cross_out, m_head, ring_w,
    triple, kv, queries, mixed, second, hidden, raw, term, term_away, term_in, far_out, far_in,
    final,
    f_local, f_send, f_recv, fr_send, fr_recv, t_send, t_recv, g_send, g_recv, w_send, w_recv,
    s_send, r_send, r_recv, x_send, x_recv, a_send, a_recv, b_send, b_recv,
):
    devices = lax.axis_size("pairs")
    chips = devices // 2
    here = lax.axis_index("pairs")
    s = lax.axis_index("side")
    x = lax.rem(here, 2)
    q = lax.div(here, 2)
    rows = features.shape[1]
    width = m_qkv.shape[0]
    slots = second.shape[0]
    tall = second.shape[1]
    per = chips // BLOCKS
    shard = ring_w.shape[2]
    split = 2 if shard % 32 == 0 else 1
    kinds = 2 * split
    rank = shard // split
    total_pieces = kinds * chips

    sibling = (here, 1 - s)
    partner = (2 * q + s, x)
    at_home = x == s

    def pair_of(step, flip):
        chip = lax.rem(q + (step + chips), chips)
        return 2 * chip + (1 - x if flip else x)

    up = jnp.where(
        lax.rem(q, 2) == 0,
        jnp.where(q + 2 < chips, q + 2, chips - 1),
        jnp.where(q >= 3, q - 2, 0),
    )
    down = jnp.where(
        lax.rem(q, 2) == 0,
        jnp.where(q == 0, 1, q - 2),
        jnp.where(q + 2 < chips, q + 2, chips - 2),
    )
    onward = (2 * jnp.where(s == 0, up, down) + x, s)

    mats = (
        (w_qkv, m_qkv), (w_self_out, m_self_out), (w_memory, m_memory), (w_query, m_query),
        (w_cross_out, m_cross_out),
    )
    half = w_head.shape[2] // 2
    weights = [(src.at[0], dst) for src, dst in mats]
    weights += [(w_head.at[0, :, h * half : (h + 1) * half], m_head.at[h]) for h in range(2)]
    gain_refs = (g_self, g_query, g_memory, g_mlp, g_head)
    fcs = (w_fc1, w_fc2)

    def slot_at(step, ring):
        return 2 * step + ring

    def ring_view(step, kind, ring):
        place = ring_w.at[lax.rem(kind, 2), slot_at(step, ring)]
        if split == 1:
            return place
        return place.at[pl.ds(pl.multiple_of(lax.div(kind, 2) * rank, rank), rank)]

    def own_fc(which, piece):
        if split == 1:
            return fcs[which].at[0]
        return fcs[which].at[0, pl.ds(pl.multiple_of(piece * rank, rank), rank)]

    own_win = pltpu.make_async_copy(features.at[0], win.at[x, s], f_local)
    own_win.start()

    @pl.when(at_home)
    def _():
        for at, ref in enumerate(gain_refs):
            pltpu.make_async_copy(ref, gains.at[at], g_recv.at[at]).start()
        for which in range(2):
            pltpu.make_async_copy(
                own_fc(which, s), ring_view(0, which, s), r_recv.at[0, which]
            ).start()
        for at, (src, dst) in enumerate(weights):
            pltpu.make_async_copy(src, dst, w_recv.at[at]).start()

    barrier = pltpu.get_barrier_semaphore()
    for step in range(-2, 3):
        for flip in range(2):
            if step or flip:
                pl.semaphore_signal(
                    barrier, inc=1, device_id=(pair_of(step, flip), s), device_id_type=MESH
                )
    pl.semaphore_signal(barrier, inc=1, device_id=sibling, device_id_type=MESH)

    @pl.when(jnp.logical_not(at_home))
    def _():
        pl.semaphore_signal(barrier, inc=1, device_id=partner, device_id_type=MESH)

    pl.semaphore_wait(barrier, 10 + (1 - at_home.astype(jnp.int32)))

    table_out = [
        remote(slot_images, table, t_send.at[0], t_recv.at[0], (pair_of(0, 1), s)),
        remote(slot_count, counts, t_send.at[1], t_recv.at[1], (pair_of(0, 1), s)),
    ]
    across = (2 * q + s, s)
    if split == 1:
        fc_home = []
        fc_out = [
            remote(own_fc(f, 0), ring_view(0, f, x), s_send.at[f], r_recv.at[0, f], partner)
            for f in range(2)
        ]
    else:
        fc_home = [
            remote(
                own_fc(f, 1 - s), ring_view(0, f, 1 - s), s_send.at[f], r_recv.at[0, f], sibling
            )
            for f in range(2)
        ]
        fc_out = [
            remote(
                own_fc(f, ring), ring_view(0, 2 + f, ring), s_send.at[2 * f + to],
                r_recv.at[0, 2 + f], device,
            )
            for f in range(2)
            for to, (ring, device) in enumerate(((x, partner), (s, across)))
        ]
    gains_out = [
        remote(ref, gains.at[at], g_send.at[at], g_recv.at[at], sibling)
        for at, ref in enumerate(gain_refs)
    ]
    weights_out = [
        remote(src, dst, w_send.at[at], w_recv.at[at], sibling)
        for at, (src, dst) in enumerate(weights)
    ]

    def feature_out(block, place, step, flip, at):
        return remote(
            block, win.at[place, s], f_send.at[at], f_recv.at[place], (pair_of(-step, flip), s)
        )

    own = features.at[0]
    passed = win.at[1 - x, s]
    even = lax.rem(q, 2) == 0
    feature_across = feature_out(own, x, 0, 1, 0)
    near_zero = [feature_out(block, 2, 1, 0, 1) for block in (own, passed)]
    near_one = [feature_out(block, 3, 1, 0, 2) for block in (passed, own)]
    far_zero = [feature_out(block, WINDOW, 2, 0, 3) for block in (own, passed)]
    onto_next = feature_out(win.at[WINDOW, s], 2, -1, 0, 4)

    def zero_start(at):
        far_zero[at].start()

        @pl.when(jnp.logical_not(even))
        def _():
            near_zero[at].start()

    def relay(place, block=None):
        target = win.at[place, s]
        return remote(
            target if block is None else block, target, fr_send.at[place], fr_recv.at[place],
            sibling,
        )

    for copy in table_out:
        copy.start()
    feature_across.start()

    @pl.when(x == 0)
    def _():
        zero_start(0)

    @pl.when(x == 1)
    def _():
        near_one[1].start()

    relay(x, own).start()

    @pl.when(at_home)
    def _():
        for copy in fc_home + gains_out:
            copy.start()
        weights_out[0].start()

    @pl.when(jnp.logical_not(at_home))
    def _():
        for copy in fc_out:
            copy.start()

    def piece(number):
        turn = lax.div(number, kinds // 2)
        last = turn == 2 * chips - 1
        ahead = jnp.logical_or(turn == 0, jnp.logical_and(lax.rem(turn, 2) == 1, turn < 2 * chips - 1))
        step = jnp.where(
            turn == 0,
            0,
            jnp.where(last, chips - 1, jnp.where(ahead, lax.div(turn + 1, 2), lax.div(turn, 2) - 1)),
        )
        kind = lax.rem(number, kinds // 2) + jnp.where(ahead, 0, kinds // 2)
        block = ring_view(step, kind, s)
        pltpu.make_async_copy(block, block, r_recv.at[step, kind]).wait()

        @pl.when(step < chips - 1)
        def _():
            remote(
                block, ring_view(step + 1, kind, s), r_send.at[step, kind],
                r_recv.at[step + 1, kind], onward,
            ).start()

        remote(block, block, x_send.at[step, kind], x_recv.at[step, kind], sibling).start()

    def pieces(low, high):
        def body(number, carry):
            piece(number)
            return carry

        lax.fori_loop(low, high, body, 0)

    def arrived(place):
        block = win.at[place, s]
        pltpu.make_async_copy(block, block, f_recv.at[place]).wait()
        relay(place).start()

    group = kinds // 2
    early = 4 * group
    pieces(0, group)
    arrived(1 - x)

    @pl.when(x == 0)
    def _():
        near_one[0].start()

    @pl.when(x == 1)
    def _():
        zero_start(1)

    pieces(group, 2 * group)
    arrived(WINDOW)

    @pl.when(even)
    def _():
        onto_next.start()

    arrived(3)
    pieces(2 * group, 3 * group)

    @pl.when(at_home)
    def _():
        for copy in weights_out[1:2]:
            copy.start()

    pieces(3 * group, early)
    arrived(2)

    @pl.when(at_home)
    def _():
        for copy in weights_out[2:]:
            copy.start()

    own_win.wait()
    for place in range(REACH):
        block = win.at[place, 1 - s]
        pltpu.make_async_copy(block, block, fr_recv.at[place]).wait()
    for copy in table_out:
        copy.wait_recv()
    for at, ref in enumerate(gain_refs):
        pltpu.make_async_copy(ref, gains.at[at], g_recv.at[at]).wait()

    def weight_wait(at):
        src, dst = weights[at]
        pltpu.make_async_copy(src, dst, w_recv.at[at]).wait()

    def first_wait(slot, at):
        @pl.when(slot == 0)
        def _():
            weight_wait(at)

    def entry(slot, column, core):
        local = slot_images[slot, column]
        return jnp.where(x == core, local, table[slot, column])

    def place_of(slot, column, core=None):
        core = s if core is None else core
        stored = image_slot[entry(slot, column, core)]
        ahead = lax.rem(stored - (2 * q + core) + devices, devices)
        return jnp.minimum(ahead, WINDOW - 1) + core

    def tokens_of(place):
        return jnp.concatenate([win[place, 0], win[place, 1]], axis=-1).astype(jnp.float32)

    stops = 6 * slots
    each = max((total_pieces * 26 // 32 - early) // stops, 0)
    fronted = early + each * stops

    def front(slot, carry):
        told = [0]

        def comm():
            base = early + (6 * slot + told[0]) * each
            told[0] += 1
            for at in range(each):
                piece(base + at)

        first_wait(slot, 0)
        tokens = tokens_of(place_of(slot, x))
        state = layer_norm(tokens, gains[0]).astype(jnp.bfloat16)
        triple[...] = matmul(state, m_qkv[...]).astype(jnp.bfloat16)
        comm()
        attend(triple, triple, triple, width, 2 * width, mixed, width, comm)
        first_wait(slot, 1)
        first = tokens + matmul(mixed[...], m_self_out[...])
        second[slot, 0:rows, :] = first
        comm()
        first_wait(slot, 2)
        first_wait(slot, 3)
        query_in = layer_norm(first, gains[1]).astype(jnp.bfloat16)
        memory = tokens_of(place_of(slot, 1 - x))
        memory_in = layer_norm(memory, gains[2]).astype(jnp.bfloat16)
        queries[...] = matmul(query_in, m_query[...]).astype(jnp.bfloat16)
        kv[...] = matmul(memory_in, m_memory[...]).astype(jnp.bfloat16)
        comm()
        attend(queries, kv, kv, 0, width, mixed, width, comm)
        first_wait(slot, 4)
        result = second[slot, 0:rows, :] + matmul(mixed[...], m_cross_out[...])
        second[slot, 0:rows, :] = result
        hidden[slot, 0:rows, :] = layer_norm(result, gains[3]).astype(jnp.bfloat16)
        comm()
        return carry

    second[...] = jnp.zeros_like(second)
    hidden[...] = jnp.zeros_like(hidden)
    lax.fori_loop(0, slots, front, 0)

    def relayed(first, steps):
        def body(at, carry):
            step, kind = first + lax.div(at, kinds), lax.rem(at, kinds)
            view = ring_view(step, kind, 1 - s)
            pltpu.make_async_copy(view, view, x_recv.at[step, kind]).wait()
            return carry

        lax.fori_loop(0, steps * kinds, body, 0)

    def expand(first, steps, slot):
        count = 2 * steps
        if shard % 16 == 0:
            groups = [
                [ring_w[f, pl.ds(2 * first, count)].reshape(count * shard, width) for f in range(2)]
            ]
        else:
            groups = [[ring_w[f, 2 * first + at] for f in range(2)] for at in range(count)]
        total = second[slot]
        for fc1, fc2 in groups:
            pre = matmul_t(hidden[slot], fc1)
            act = (pre * (1.0 + lax.erf(pre * 0.5**0.5)) * 0.5).astype(jnp.bfloat16)
            total = total + matmul(act, fc2)
        second[slot] = total

    whole = total_pieces - group
    left = whole - fronted
    places = (BLOCKS - 1) * slots

    def expand_early(turn, carry):
        block, slot = lax.div(turn, slots), lax.rem(turn, slots)

        @pl.when(slot == 0)
        def _():
            relayed(block * per, per)

        expand(block * per, per, slot)
        pieces(fronted + lax.div(turn * left, places), fronted + lax.div((turn + 1) * left, places))
        return carry

    lax.fori_loop(0, places, expand_early, 0)
    relayed((BLOCKS - 1) * per, per - 1)

    def expand_late(slot, carry):
        expand((BLOCKS - 1) * per, per - 1, slot)
        pieces(
            whole + lax.div(slot * group, slots), whole + lax.div((slot + 1) * group, slots)
        )
        return carry

    lax.fori_loop(0, slots, expand_late, 0)
    weight_wait(5)
    weight_wait(6)
    relayed(chips - 1, 1)
    pix = half // 4

    def terms(slot, which, target):
        raw[...] = matmul(hidden[slot], m_head[which])
        conf = 1.0 + jnp.exp(raw[0:rows, 3 * pix :])
        for comp in range(4):
            at = slice(comp * pix, (comp + 1) * pix)
            value = conf if comp == 3 else conf * raw[0:rows, at]
            target[slot, :, at] = value.astype(target.dtype)

    def away(slot):
        return remote(
            term_away.at[slot], term_in.at[slot], a_send.at[slot], a_recv.at[slot], sibling
        )

    def expand_last(slot, carry):
        expand(chips - 1, 1, slot)
        hidden[slot] = layer_norm(second[slot], gains[4]).astype(jnp.bfloat16)
        terms(slot, 1 - s, term_away)
        away(slot).start()
        return carry

    def own_terms(slot, carry):
        terms(slot, s, term)
        return carry

    lax.fori_loop(0, slots, expand_last, 0)
    lax.fori_loop(0, slots, own_terms, 0)
    for slot in range(slots):
        away(slot).wait_recv()

    sources = []
    for core, ref in ((s, term), (1 - s, term_in)):
        live = jnp.where(x == core, slot_count[0], counts[0])
        for slot in range(slots):
            sources.append((place_of(slot, x, core), slot < live, ref, slot))

    def sums_of(place):
        sums = jnp.zeros((rows, half), jnp.float32)
        for to, live, ref, slot in sources:
            chosen = jnp.logical_and(to == place, live)
            sums = sums + jnp.where(chosen, ref[slot].astype(jnp.float32), 0.0)
        return sums

    def far_copy(place):
        step, to = place // 2, place % 2
        other = jnp.where(x == to, 0, 1)
        chip = lax.rem(q + step, chips)
        return remote(
            far_out.at[place], far_in.at[2 * step + other], b_send.at[place],
            b_recv.at[2 * step + other], (2 * chip + to, s),
        )

    for place in reversed(range(2, REACH)):
        far_out[place] = sums_of(place).astype(jnp.bfloat16)
        far_copy(place).start()
    far_out[1 - x] = sums_of(1 - x).astype(jnp.bfloat16)
    for place in range(2):

        @pl.when(x != place)
        def _(place=place):
            far_copy(place).start()

    total = sums_of(x)

    def far_wait(at):
        block = far_in.at[at]
        pltpu.make_async_copy(block, block, b_recv.at[at]).wait()

    for at in (1, 2, 3):
        far_wait(at)
        total = total + far_in[at].astype(jnp.float32)
    final[...] = total

    @pl.when(x == 0)
    def _():
        for at in (4, 5):
            far_wait(at)
        final[...] = final[...] + far_in[4].astype(jnp.float32) + far_in[5].astype(jnp.float32)

    conf = jnp.maximum(final[:, 3 * pix :], 1.0)
    for comp in range(3):
        at = slice(comp * pix, (comp + 1) * pix)
        out[0, :, at] = (final[:, at] / conf).astype(jnp.bfloat16)

    for copy in (feature_across, near_one[0], far_zero[0]):
        copy.wait_send()

    @pl.when(even)
    def _():
        onto_next.wait_send()

    @pl.when(jnp.logical_not(even))
    def _():
        near_zero[0].wait_send()

    for place in range(REACH):
        relay(place).wait_send()

    @pl.when(at_home)
    def _():
        for copy in fc_home + gains_out + weights_out:
            copy.wait_send()

    @pl.when(jnp.logical_not(at_home))
    def _():
        for copy in fc_out:
            copy.wait_send()

    for copy in table_out:
        copy.wait_send()

    def drain(number, carry):
        step, kind = lax.div(number, kinds), lax.rem(number, kinds)
        block = ring_view(step, kind, s)

        @pl.when(step < chips - 1)
        def _():
            remote(
                block, block, r_send.at[step, kind], r_recv.at[step, kind], onward
            ).wait_send()

        remote(block, block, x_send.at[step, kind], x_recv.at[step, kind], sibling).wait_send()
        return carry

    lax.fori_loop(0, total_pieces, drain, 0)
    for slot in range(slots):
        away(slot).wait_send()
    for place in range(REACH):
        if place < 2:

            @pl.when(x != place)
            def _(place=place):
                far_copy(place).wait_send()

        else:
            far_copy(place).wait_send()


def on_device(
    features, image_slot, slot_images, slot_count, gain_self, gain_query, gain_memory, gain_mlp,
    gain_head, w_qkv, w_self_out, w_query, w_memory, w_cross_out, w_fc1, w_fc2, w_head,
):
    devices = lax.axis_size("pairs")
    chips = devices // 2
    blocks, rows, part = features.shape
    if blocks != 1 or chips % BLOCKS:
        raise ValueError("unsupported split")
    width = w_qkv.shape[1]
    slots = slot_images.shape[0]
    tall = padded(rows)
    shard = w_fc1.shape[1]
    kinds = 2 * (2 if shard % 32 == 0 else 1)
    half = w_head.shape[2] // 2
    bf16, f32 = jnp.bfloat16, jnp.float32
    dma = pltpu.SemaphoreType.DMA
    anywhere = pl.BlockSpec(memory_space=pl.ANY)
    return pl.pallas_call(
        decoder_kernel,
        out_shape=jax.ShapeDtypeStruct((1, rows, half * 3 // 4), bf16),
        in_specs=[pl.BlockSpec(memory_space=pltpu.SMEM)] * 3 + [anywhere] * 14,
        out_specs=pl.BlockSpec(memory_space=pltpu.VMEM),
        scratch_shapes=[
            pltpu.VMEM((REACH, 2, rows, part), bf16),
            pltpu.SMEM(slot_images.shape, jnp.int32),
            pltpu.SMEM(slot_count.shape, jnp.int32),
            pltpu.VMEM((5, 1, width), f32),
            pltpu.VMEM(w_qkv.shape[1:], bf16),
            pltpu.VMEM(w_self_out.shape[1:], bf16),
            pltpu.VMEM(w_query.shape[1:], bf16),
            pltpu.VMEM(w_memory.shape[1:], bf16),
            pltpu.VMEM(w_cross_out.shape[1:], bf16),
            pltpu.VMEM((2, width, half), bf16),
            pltpu.VMEM((2, devices, shard, width), bf16),
            pltpu.VMEM((rows, 3 * width), bf16),
            pltpu.VMEM((rows, 2 * width), bf16),
            pltpu.VMEM((rows, width), bf16),
            pltpu.VMEM((rows, width), bf16),
            pltpu.VMEM((slots, tall, width), f32),
            pltpu.VMEM((slots, tall, width), bf16),
            pltpu.VMEM((tall, half), f32),
            pltpu.VMEM((slots, rows, half), f32),
            pltpu.VMEM((slots, rows, half), bf16),
            pltpu.VMEM((slots, rows, half), bf16),
            pltpu.VMEM((REACH, rows, half), bf16),
            pltpu.VMEM((REACH + 1, rows, half), bf16),
            pltpu.VMEM((rows, half), f32),
            dma, dma((5,)), dma((REACH,)), dma((REACH,)), dma((REACH,)),
            dma((2,)), dma((2,)), dma((5,)), dma((5,)), dma((7,)), dma((7,)),
            dma((kinds,)), dma((chips, kinds)), dma((chips, kinds)), dma((chips, kinds)),
            dma((chips, kinds)), dma((slots,)), dma((slots,)), dma((REACH,)), dma((REACH + 1,)),
        ],
        compiler_params=pltpu.CompilerParams(
            collective_id=0, has_side_effects=True, vmem_limit_bytes=VMEM_LIMIT
        ),
    )(
        image_slot, slot_images, slot_count, features, gain_self, gain_query, gain_memory,
        gain_mlp, gain_head, w_qkv, w_self_out, w_query, w_memory, w_cross_out, w_fc1, w_fc2,
        w_head,
    )


def solution(mesh):
    placed = (
        P("pairs", None, "side"),
        P(),
        P("pairs", None),
        P("pairs"),
        P("side", None),
        P("side", None),
        P("side", None),
        P("side", None),
        P("side", None),
        P("side", None, None),
        P("side", None, None),
        P("side", None, None),
        P("side", None, None),
        P("side", None, None),
        P("side", "pairs", None),
        P("side", "pairs", None),
        P("side", None, None),
    )
    return jax.shard_map(
        on_device, mesh=mesh, in_specs=placed, out_specs=P("pairs", None, "side"), check_vma=False
    )
```

```python
import functools

import jax
import jax.numpy as jnp
from jax import lax
from jax.experimental import pallas as pl
from jax.experimental.pallas import tpu as pltpu
from jax.sharding import PartitionSpec as P

HEAD_DIM = 64
WINDOW = 4
PAIR = 2 * HEAD_DIM
BLOCKS = 4
REACH = WINDOW + 1
VMEM_LIMIT = 63 * 1024 * 1024
MESH = pl.DeviceIdType.MESH


def padded(rows):
    return -(-rows // 16) * 16


def layer_norm(values, gain):
    center = values - jnp.mean(values, axis=-1, keepdims=True)
    spread = jnp.mean(center * center, axis=-1, keepdims=True)
    return center * lax.rsqrt(spread + 1e-06) * gain


def matmul(left, right):
    return jnp.dot(left, right, preferred_element_type=jnp.float32)


def matmul_t(left, right):
    return lax.dot_general(
        left, right, (((1,), (1,)), ((), ())), preferred_element_type=jnp.float32
    )


def attend(q_ref, k_ref, v_ref, k_at, v_at, o_ref, width, comm):
    rows = q_ref.shape[0]
    low = lax.broadcasted_iota(jnp.int32, (rows, PAIR), 1) < HEAD_DIM
    for pair in range(width // PAIR):
        if pair * PAIR == width // 2:
            comm()
        q = q_ref[:, pair * PAIR : (pair + 1) * PAIR]
        k = k_ref[:, k_at + pair * PAIR : k_at + (pair + 1) * PAIR]
        v = v_ref[:, v_at + pair * PAIR : v_at + (pair + 1) * PAIR]
        mixed = None
        for keep in (low, jnp.logical_not(low)):
            q_head = jnp.where(keep, q, jnp.zeros_like(q))
            v_head = jnp.where(keep, v, jnp.zeros_like(v))
            scores = matmul_t(q_head, k) * HEAD_DIM ** (-0.5)
            expon = jnp.exp(scores)
            weights = (expon / jnp.sum(expon, axis=-1, keepdims=True)).astype(jnp.bfloat16)
            part = matmul(weights, v_head)
            mixed = part if mixed is None else mixed + part
        o_ref[:, pair * PAIR : (pair + 1) * PAIR] = mixed.astype(jnp.bfloat16)


def remote(src, dst, send, recv, device):
    return pltpu.make_async_remote_copy(
        src_ref=src, dst_ref=dst, send_sem=send, recv_sem=recv, device_id=device,
        device_id_type=MESH,
    )


def decoder_kernel(
    image_slot, slot_images, slot_count, features,
    g_self, g_query, g_memory, g_mlp, g_head,
    w_qkv, w_self_out, w_query, w_memory, w_cross_out, w_fc1, w_fc2, w_head,
    out,
    win, table, counts, gains, m_qkv, m_self_out, m_query, m_memory, m_cross_out, m_head, ring_w,
    triple, kv, queries, mixed, second, hidden, raw, term, term_away, term_in, far_out, far_in,
    final,
    f_local, f_send, f_recv, fr_send, fr_recv, t_send, t_recv, g_send, g_recv, w_send, w_recv,
    s_send, r_send, r_recv, x_send, x_recv, a_send, a_recv, b_send, b_recv,
):
    devices = lax.axis_size("pairs")
    chips = devices // 2
    here = lax.axis_index("pairs")
    s = lax.axis_index("side")
    x = lax.rem(here, 2)
    q = lax.div(here, 2)
    rows = features.shape[1]
    width = m_qkv.shape[0]
    slots = second.shape[0]
    tall = second.shape[1]
    per = chips // BLOCKS
    shard = ring_w.shape[2]
    split = 2 if shard % 32 == 0 else 1
    kinds = 2 * split
    rank = shard // split
    total_pieces = kinds * chips

    sibling = (here, 1 - s)
    partner = (2 * q + s, x)
    at_home = x == s

    def pair_of(step, flip):
        chip = lax.rem(q + (step + chips), chips)
        return 2 * chip + (1 - x if flip else x)

    up = jnp.where(
        lax.rem(q, 2) == 0,
        jnp.where(q + 2 < chips, q + 2, chips - 1),
        jnp.where(q >= 3, q - 2, 0),
    )
    down = jnp.where(
        lax.rem(q, 2) == 0,
        jnp.where(q == 0, 1, q - 2),
        jnp.where(q + 2 < chips, q + 2, chips - 2),
    )
    onward = (2 * jnp.where(s == 0, up, down) + x, s)

    mats = (
        (w_qkv, m_qkv), (w_self_out, m_self_out), (w_memory, m_memory), (w_query, m_query),
        (w_cross_out, m_cross_out),
    )
    half = w_head.shape[2] // 2
    weights = [(src.at[0], dst) for src, dst in mats]
    weights += [(w_head.at[0, :, h * half : (h + 1) * half], m_head.at[h]) for h in range(2)]
    gain_refs = (g_self, g_query, g_memory, g_mlp, g_head)
    fcs = (w_fc1, w_fc2)

    def slot_at(step, ring):
        return 2 * step + ring

    def ring_view(step, kind, ring):
        place = ring_w.at[lax.rem(kind, 2), slot_at(step, ring)]
        if split == 1:
            return place
        return place.at[pl.ds(pl.multiple_of(lax.div(kind, 2) * rank, rank), rank)]

    def own_fc(which, piece):
        if split == 1:
            return fcs[which].at[0]
        return fcs[which].at[0, pl.ds(pl.multiple_of(piece * rank, rank), rank)]

    own_win = pltpu.make_async_copy(features.at[0], win.at[x, s], f_local)
    own_win.start()

    @pl.when(at_home)
    def _():
        for at, ref in enumerate(gain_refs):
            pltpu.make_async_copy(ref, gains.at[at], g_recv.at[at]).start()
        for which in range(2):
            pltpu.make_async_copy(
                own_fc(which, s), ring_view(0, which, s), r_recv.at[0, which]
            ).start()
        for at, (src, dst) in enumerate(weights):
            pltpu.make_async_copy(src, dst, w_recv.at[at]).start()

    barrier = pltpu.get_barrier_semaphore()
    for step in range(-2, 3):
        for flip in range(2):
            if step or flip:
                pl.semaphore_signal(
                    barrier, inc=1, device_id=(pair_of(step, flip), s), device_id_type=MESH
                )
    pl.semaphore_signal(barrier, inc=1, device_id=sibling, device_id_type=MESH)

    @pl.when(jnp.logical_not(at_home))
    def _():
        pl.semaphore_signal(barrier, inc=1, device_id=partner, device_id_type=MESH)

    pl.semaphore_wait(barrier, 10 + (1 - at_home.astype(jnp.int32)))

    table_out = [
        remote(slot_images, table, t_send.at[0], t_recv.at[0], (pair_of(0, 1), s)),
        remote(slot_count, counts, t_send.at[1], t_recv.at[1], (pair_of(0, 1), s)),
    ]
    across = (2 * q + s, s)
    if split == 1:
        fc_home = []
        fc_out = [
            remote(own_fc(f, 0), ring_view(0, f, x), s_send.at[f], r_recv.at[0, f], partner)
            for f in range(2)
        ]
    else:
        fc_home = [
            remote(
                own_fc(f, 1 - s), ring_view(0, f, 1 - s), s_send.at[f], r_recv.at[0, f], sibling
            )
            for f in range(2)
        ]
        fc_out = [
            remote(
                own_fc(f, ring), ring_view(0, 2 + f, ring), s_send.at[2 * f + to],
                r_recv.at[0, 2 + f], device,
            )
            for f in range(2)
            for to, (ring, device) in enumerate(((x, partner), (s, across)))
        ]
    gains_out = [
        remote(ref, gains.at[at], g_send.at[at], g_recv.at[at], sibling)
        for at, ref in enumerate(gain_refs)
    ]
    weights_out = [
        remote(src, dst, w_send.at[at], w_recv.at[at], sibling)
        for at, (src, dst) in enumerate(weights)
    ]

    def feature_out(block, place, step, flip, at):
        return remote(
            block, win.at[place, s], f_send.at[at], f_recv.at[place], (pair_of(-step, flip), s)
        )

    own = features.at[0]
    passed = win.at[1 - x, s]
    even = lax.rem(q, 2) == 0
    near, far = 2 + x, WINDOW
    feature_across = feature_out(own, x, 0, 1, 0)
    feature_near = feature_out(own, near, 1, 0, 1)
    feature_far = feature_out(own, far, 2, 0, 2)
    feature_onto = feature_out(win.at[far, s], 2, -1, 0, 3)
    near_across = feature_out(win.at[near, s], near, 0, 1, 4)
    far_across = feature_out(win.at[far, s], far, 0, 1, 5)

    def relay(place, block=None):
        target = win.at[place, s]
        return remote(
            target if block is None else block, target, fr_send.at[place], fr_recv.at[place],
            sibling,
        )

    for copy in table_out:
        copy.start()
    feature_across.start()

    by_near = jnp.logical_or(x == 1, jnp.logical_not(even))

    @pl.when(x == 0)
    def _():
        feature_far.start()

    @pl.when(by_near)
    def _():
        feature_near.start()

    relay(x, own).start()

    @pl.when(at_home)
    def _():
        for copy in fc_home + gains_out:
            copy.start()
        weights_out[0].start()

    @pl.when(jnp.logical_not(at_home))
    def _():
        for copy in fc_out:
            copy.start()

    def piece(number):
        turn = lax.div(number, kinds // 2)
        last = turn == 2 * chips - 1
        ahead = jnp.logical_or(turn == 0, jnp.logical_and(lax.rem(turn, 2) == 1, turn < 2 * chips - 1))
        step = jnp.where(
            turn == 0,
            0,
            jnp.where(last, chips - 1, jnp.where(ahead, lax.div(turn + 1, 2), lax.div(turn, 2) - 1)),
        )
        kind = lax.rem(number, kinds // 2) + jnp.where(ahead, 0, kinds // 2)
        block = ring_view(step, kind, s)
        pltpu.make_async_copy(block, block, r_recv.at[step, kind]).wait()

        @pl.when(step < chips - 1)
        def _():
            remote(
                block, ring_view(step + 1, kind, s), r_send.at[step, kind],
                r_recv.at[step + 1, kind], onward,
            ).start()

        remote(block, block, x_send.at[step, kind], x_recv.at[step, kind], sibling).start()

    def pieces(low, high):
        def body(number, carry):
            piece(number)
            return carry

        lax.fori_loop(low, high, body, 0)

    def arrived(place):
        block = win.at[place, s]
        pltpu.make_async_copy(block, block, f_recv.at[place]).wait()
        relay(place).start()

    group = kinds // 2
    early = 4 * group
    pieces(0, group)
    arrived(1 - x)
    pieces(group, 2 * group)

    @pl.when(x == 0)
    def _():
        arrived(far)
        far_across.start()

        @pl.when(even)
        def _():
            feature_onto.start()

    arrived(near)
    near_across.start()
    pieces(2 * group, 3 * group)

    @pl.when(at_home)
    def _():
        for copy in weights_out[1:2]:
            copy.start()

    arrived(3 - x)

    @pl.when(x == 1)
    def _():
        arrived(far)

    pieces(3 * group, early)

    @pl.when(at_home)
    def _():
        for copy in weights_out[2:]:
            copy.start()

    own_win.wait()
    for place in range(REACH):
        block = win.at[place, 1 - s]
        pltpu.make_async_copy(block, block, fr_recv.at[place]).wait()
    for copy in table_out:
        copy.wait_recv()
    for at, ref in enumerate(gain_refs):
        pltpu.make_async_copy(ref, gains.at[at], g_recv.at[at]).wait()

    def weight_wait(at):
        src, dst = weights[at]
        pltpu.make_async_copy(src, dst, w_recv.at[at]).wait()

    def first_wait(slot, at):
        @pl.when(slot == 0)
        def _():
            weight_wait(at)

    def entry(slot, column, core):
        local = slot_images[slot, column]
        return jnp.where(x == core, local, table[slot, column])

    def place_of(slot, column, core=None):
        core = s if core is None else core
        stored = image_slot[entry(slot, column, core)]
        ahead = lax.rem(stored - (2 * q + core) + devices, devices)
        return jnp.minimum(ahead, WINDOW - 1) + core

    def tokens_of(place):
        return jnp.concatenate([win[place, 0], win[place, 1]], axis=-1).astype(jnp.float32)

    stops = 6 * slots
    each = max((total_pieces * 26 // 32 - early) // stops, 0)
    fronted = early + each * stops

    def front(slot, carry):
        told = [0]

        def comm():
            base = early + (6 * slot + told[0]) * each
            told[0] += 1
            for at in range(each):
                piece(base + at)

        first_wait(slot, 0)
        tokens = tokens_of(place_of(slot, x))
        state = layer_norm(tokens, gains[0]).astype(jnp.bfloat16)
        triple[...] = matmul(state, m_qkv[...]).astype(jnp.bfloat16)
        comm()
        attend(triple, triple, triple, width, 2 * width, mixed, width, comm)
        first_wait(slot, 1)
        first = tokens + matmul(mixed[...], m_self_out[...])
        second[slot, 0:rows, :] = first
        comm()
        first_wait(slot, 2)
        first_wait(slot, 3)
        query_in = layer_norm(first, gains[1]).astype(jnp.bfloat16)
        memory = tokens_of(place_of(slot, 1 - x))
        memory_in = layer_norm(memory, gains[2]).astype(jnp.bfloat16)
        queries[...] = matmul(query_in, m_query[...]).astype(jnp.bfloat16)
        kv[...] = matmul(memory_in, m_memory[...]).astype(jnp.bfloat16)
        comm()
        attend(queries, kv, kv, 0, width, mixed, width, comm)
        first_wait(slot, 4)
        result = second[slot, 0:rows, :] + matmul(mixed[...], m_cross_out[...])
        second[slot, 0:rows, :] = result
        hidden[slot, 0:rows, :] = layer_norm(result, gains[3]).astype(jnp.bfloat16)
        comm()
        return carry

    second[...] = jnp.zeros_like(second)
    hidden[...] = jnp.zeros_like(hidden)
    lax.fori_loop(0, slots, front, 0)

    def relayed(first, steps):
        def body(at, carry):
            step, kind = first + lax.div(at, kinds), lax.rem(at, kinds)
            view = ring_view(step, kind, 1 - s)
            pltpu.make_async_copy(view, view, x_recv.at[step, kind]).wait()
            return carry

        lax.fori_loop(0, steps * kinds, body, 0)

    def expand(first, steps, slot):
        count = 2 * steps
        if shard % 16 == 0:
            groups = [
                [ring_w[f, pl.ds(2 * first, count)].reshape(count * shard, width) for f in range(2)]
            ]
        else:
            groups = [[ring_w[f, 2 * first + at] for f in range(2)] for at in range(count)]
        total = second[slot]
        for fc1, fc2 in groups:
            pre = matmul_t(hidden[slot], fc1)
            act = (pre * (1.0 + lax.erf(pre * 0.5**0.5)) * 0.5).astype(jnp.bfloat16)
            total = total + matmul(act, fc2)
        second[slot] = total

    whole = total_pieces - group
    left = whole - fronted
    places = (BLOCKS - 1) * slots
    rate = -(-left // BLOCKS)

    def expand_early(turn, carry):
        block, slot = lax.div(turn, slots), lax.rem(turn, slots)

        @pl.when(slot == 0)
        def _():
            relayed(block * per, per)

        expand(block * per, per, slot)
        pieces(
            fronted + jnp.minimum(turn * rate, left), fronted + jnp.minimum((turn + 1) * rate, left)
        )
        return carry

    lax.fori_loop(0, places, expand_early, 0)
    relayed((BLOCKS - 1) * per, per - 1)

    def expand_late(slot, carry):
        expand((BLOCKS - 1) * per, per - 1, slot)
        pieces(
            whole + lax.div(slot * group, slots), whole + lax.div((slot + 1) * group, slots)
        )
        return carry

    lax.fori_loop(0, slots, expand_late, 0)
    weight_wait(5)
    weight_wait(6)
    relayed(chips - 1, 1)
    pix = half // 4

    def terms(slot, which, target):
        raw[...] = matmul(hidden[slot], m_head[which])
        conf = 1.0 + jnp.exp(raw[0:rows, 3 * pix :])
        for comp in range(4):
            at = slice(comp * pix, (comp + 1) * pix)
            value = conf if comp == 3 else conf * raw[0:rows, at]
            target[slot, :, at] = value.astype(target.dtype)

    def away(slot):
        return remote(
            term_away.at[slot], term_in.at[slot], a_send.at[slot], a_recv.at[slot], sibling
        )

    def expand_last(slot, carry):
        expand(chips - 1, 1, slot)
        hidden[slot] = layer_norm(second[slot], gains[4]).astype(jnp.bfloat16)
        terms(slot, 1 - s, term_away)
        away(slot).start()
        return carry

    def own_terms(slot, carry):
        terms(slot, s, term)
        return carry

    lax.fori_loop(0, slots, expand_last, 0)
    lax.fori_loop(0, slots, own_terms, 0)
    for slot in range(slots):
        away(slot).wait_recv()

    sources = []
    for core, ref in ((s, term), (1 - s, term_in)):
        live = jnp.where(x == core, slot_count[0], counts[0])
        for slot in range(slots):
            sources.append((place_of(slot, x, core), slot < live, ref, slot))

    def sums_of(place):
        sums = jnp.zeros((rows, half), jnp.float32)
        for to, live, ref, slot in sources:
            chosen = jnp.logical_and(to == place, live)
            sums = sums + jnp.where(chosen, ref[slot].astype(jnp.float32), 0.0)
        return sums

    def far_copy(place):
        step, to = place // 2, place % 2
        other = jnp.where(x == to, 0, 1)
        chip = lax.rem(q + step, chips)
        return remote(
            far_out.at[place], far_in.at[2 * step + other], b_send.at[place],
            b_recv.at[2 * step + other], (2 * chip + to, s),
        )

    for place in reversed(range(2, REACH)):
        far_out[place] = sums_of(place).astype(jnp.bfloat16)
        far_copy(place).start()
    far_out[1 - x] = sums_of(1 - x).astype(jnp.bfloat16)
    for place in range(2):

        @pl.when(x != place)
        def _(place=place):
            far_copy(place).start()

    total = sums_of(x)

    def far_wait(at):
        block = far_in.at[at]
        pltpu.make_async_copy(block, block, b_recv.at[at]).wait()

    for at in (1, 2, 3):
        far_wait(at)
        total = total + far_in[at].astype(jnp.float32)
    final[...] = total

    @pl.when(x == 0)
    def _():
        for at in (4, 5):
            far_wait(at)
        final[...] = final[...] + far_in[4].astype(jnp.float32) + far_in[5].astype(jnp.float32)

    conf = jnp.maximum(final[:, 3 * pix :], 1.0)
    for comp in range(3):
        at = slice(comp * pix, (comp + 1) * pix)
        out[0, :, at] = (final[:, at] / conf).astype(jnp.bfloat16)

    for copy in (feature_across, near_across):
        copy.wait_send()

    @pl.when(x == 0)
    def _():
        feature_far.wait_send()
        far_across.wait_send()

        @pl.when(even)
        def _():
            feature_onto.wait_send()

    @pl.when(by_near)
    def _():
        feature_near.wait_send()

    for place in range(REACH):
        relay(place).wait_send()

    @pl.when(at_home)
    def _():
        for copy in fc_home + gains_out + weights_out:
            copy.wait_send()

    @pl.when(jnp.logical_not(at_home))
    def _():
        for copy in fc_out:
            copy.wait_send()

    for copy in table_out:
        copy.wait_send()

    def drain(number, carry):
        step, kind = lax.div(number, kinds), lax.rem(number, kinds)
        block = ring_view(step, kind, s)

        @pl.when(step < chips - 1)
        def _():
            remote(
                block, block, r_send.at[step, kind], r_recv.at[step, kind], onward
            ).wait_send()

        remote(block, block, x_send.at[step, kind], x_recv.at[step, kind], sibling).wait_send()
        return carry

    lax.fori_loop(0, total_pieces, drain, 0)
    for slot in range(slots):
        away(slot).wait_send()
    for place in range(REACH):
        if place < 2:

            @pl.when(x != place)
            def _(place=place):
                far_copy(place).wait_send()

        else:
            far_copy(place).wait_send()


def on_device(
    features, image_slot, slot_images, slot_count, gain_self, gain_query, gain_memory, gain_mlp,
    gain_head, w_qkv, w_self_out, w_query, w_memory, w_cross_out, w_fc1, w_fc2, w_head,
):
    devices = lax.axis_size("pairs")
    chips = devices // 2
    blocks, rows, part = features.shape
    if blocks != 1 or chips % BLOCKS:
        raise ValueError("unsupported split")
    width = w_qkv.shape[1]
    slots = slot_images.shape[0]
    tall = padded(rows)
    shard = w_fc1.shape[1]
    kinds = 2 * (2 if shard % 32 == 0 else 1)
    half = w_head.shape[2] // 2
    bf16, f32 = jnp.bfloat16, jnp.float32
    dma = pltpu.SemaphoreType.DMA
    anywhere = pl.BlockSpec(memory_space=pl.ANY)
    return pl.pallas_call(
        decoder_kernel,
        out_shape=jax.ShapeDtypeStruct((1, rows, half * 3 // 4), bf16),
        in_specs=[pl.BlockSpec(memory_space=pltpu.SMEM)] * 3 + [anywhere] * 14,
        out_specs=pl.BlockSpec(memory_space=pltpu.VMEM),
        scratch_shapes=[
            pltpu.VMEM((REACH, 2, rows, part), bf16),
            pltpu.SMEM(slot_images.shape, jnp.int32),
            pltpu.SMEM(slot_count.shape, jnp.int32),
            pltpu.VMEM((5, 1, width), f32),
            pltpu.VMEM(w_qkv.shape[1:], bf16),
            pltpu.VMEM(w_self_out.shape[1:], bf16),
            pltpu.VMEM(w_query.shape[1:], bf16),
            pltpu.VMEM(w_memory.shape[1:], bf16),
            pltpu.VMEM(w_cross_out.shape[1:], bf16),
            pltpu.VMEM((2, width, half), bf16),
            pltpu.VMEM((2, devices, shard, width), bf16),
            pltpu.VMEM((rows, 3 * width), bf16),
            pltpu.VMEM((rows, 2 * width), bf16),
            pltpu.VMEM((rows, width), bf16),
            pltpu.VMEM((rows, width), bf16),
            pltpu.VMEM((slots, tall, width), f32),
            pltpu.VMEM((slots, tall, width), bf16),
            pltpu.VMEM((tall, half), f32),
            pltpu.VMEM((slots, rows, half), f32),
            pltpu.VMEM((slots, rows, half), bf16),
            pltpu.VMEM((slots, rows, half), bf16),
            pltpu.VMEM((REACH, rows, half), bf16),
            pltpu.VMEM((REACH + 1, rows, half), bf16),
            pltpu.VMEM((rows, half), f32),
            dma, dma((6,)), dma((REACH,)), dma((REACH,)), dma((REACH,)),
            dma((2,)), dma((2,)), dma((5,)), dma((5,)), dma((7,)), dma((7,)),
            dma((kinds,)), dma((chips, kinds)), dma((chips, kinds)), dma((chips, kinds)),
            dma((chips, kinds)), dma((slots,)), dma((slots,)), dma((REACH,)), dma((REACH + 1,)),
        ],
        compiler_params=pltpu.CompilerParams(
            collective_id=0, has_side_effects=True, vmem_limit_bytes=VMEM_LIMIT
        ),
    )(
        image_slot, slot_images, slot_count, features, gain_self, gain_query, gain_memory,
        gain_mlp, gain_head, w_qkv, w_self_out, w_query, w_memory, w_cross_out, w_fc1, w_fc2,
        w_head,
    )


def solution(mesh):
    placed = (
        P("pairs", None, "side"),
        P(),
        P("pairs", None),
        P("pairs"),
        P("side", None),
        P("side", None),
        P("side", None),
        P("side", None),
        P("side", None),
        P("side", None, None),
        P("side", None, None),
        P("side", None, None),
        P("side", None, None),
        P("side", None, None),
        P("side", "pairs", None),
        P("side", "pairs", None),
        P("side", None, None),
    )
    return jax.shard_map(
        on_device, mesh=mesh, in_specs=placed, out_specs=P("pairs", None, "side"), check_vma=False
    )
```

```python
import functools

import jax
import jax.numpy as jnp
from jax import lax
from jax.experimental import pallas as pl
from jax.experimental.pallas import tpu as pltpu
from jax.sharding import PartitionSpec as P

HEAD_DIM = 64
WINDOW = 4
PAIR = 2 * HEAD_DIM
BLOCKS = 4
REACH = WINDOW + 1
VMEM_LIMIT = 63 * 1024 * 1024
MESH = pl.DeviceIdType.MESH


def padded(rows):
    return -(-rows // 16) * 16


def layer_norm(values, gain):
    center = values - jnp.mean(values, axis=-1, keepdims=True)
    spread = jnp.mean(center * center, axis=-1, keepdims=True)
    return center * lax.rsqrt(spread + 1e-06) * gain


def matmul(left, right):
    return jnp.dot(left, right, preferred_element_type=jnp.float32)


def matmul_t(left, right):
    return lax.dot_general(
        left, right, (((1,), (1,)), ((), ())), preferred_element_type=jnp.float32
    )


def attend(q_ref, k_ref, v_ref, k_at, v_at, o_ref, width, comm):
    rows = q_ref.shape[0]
    low = lax.broadcasted_iota(jnp.int32, (rows, PAIR), 1) < HEAD_DIM
    for pair in range(width // PAIR):
        if pair * PAIR == width // 2:
            comm()
        q = q_ref[:, pair * PAIR : (pair + 1) * PAIR]
        k = k_ref[:, k_at + pair * PAIR : k_at + (pair + 1) * PAIR]
        v = v_ref[:, v_at + pair * PAIR : v_at + (pair + 1) * PAIR]
        mixed = None
        for keep in (low, jnp.logical_not(low)):
            q_head = jnp.where(keep, q, jnp.zeros_like(q))
            v_head = jnp.where(keep, v, jnp.zeros_like(v))
            scores = matmul_t(q_head, k) * HEAD_DIM ** (-0.5)
            expon = jnp.exp(scores)
            weights = (expon / jnp.sum(expon, axis=-1, keepdims=True)).astype(jnp.bfloat16)
            part = matmul(weights, v_head)
            mixed = part if mixed is None else mixed + part
        o_ref[:, pair * PAIR : (pair + 1) * PAIR] = mixed.astype(jnp.bfloat16)


def remote(src, dst, send, recv, device):
    return pltpu.make_async_remote_copy(
        src_ref=src, dst_ref=dst, send_sem=send, recv_sem=recv, device_id=device,
        device_id_type=MESH,
    )


def decoder_kernel(
    image_slot, slot_images, slot_count, features,
    g_self, g_query, g_memory, g_mlp, g_head,
    w_qkv, w_self_out, w_query, w_memory, w_cross_out, w_fc1, w_fc2, w_head,
    out,
    win, table, counts, gains, m_qkv, m_self_out, m_query, m_memory, m_cross_out, m_head, ring_w,
    triple, kv, queries, mixed, second, hidden, raw, term, term_away, term_in, far_out, far_in,
    final,
    f_local, f_send, f_recv, fr_send, fr_recv, t_send, t_recv, g_send, g_recv, w_send, w_recv,
    s_send, r_send, r_recv, x_send, x_recv, a_send, a_recv, b_send, b_recv,
):
    devices = lax.axis_size("pairs")
    chips = devices // 2
    here = lax.axis_index("pairs")
    s = lax.axis_index("side")
    x = lax.rem(here, 2)
    q = lax.div(here, 2)
    rows = features.shape[1]
    width = m_qkv.shape[0]
    slots = second.shape[0]
    tall = second.shape[1]
    per = chips // BLOCKS
    shard = ring_w.shape[2]
    split = 2 if shard % 32 == 0 else 1
    kinds = 2 * split
    rank = shard // split
    total_pieces = kinds * chips

    sibling = (here, 1 - s)
    partner = (2 * q + s, x)
    at_home = x == s

    def pair_of(step, flip):
        chip = lax.rem(q + (step + chips), chips)
        return 2 * chip + (1 - x if flip else x)

    up = jnp.where(
        lax.rem(q, 2) == 0,
        jnp.where(q + 2 < chips, q + 2, chips - 1),
        jnp.where(q >= 3, q - 2, 0),
    )
    down = jnp.where(
        lax.rem(q, 2) == 0,
        jnp.where(q == 0, 1, q - 2),
        jnp.where(q + 2 < chips, q + 2, chips - 2),
    )
    onward = (2 * jnp.where(s == 0, up, down) + x, s)

    mats = (
        (w_qkv, m_qkv), (w_self_out, m_self_out), (w_memory, m_memory), (w_query, m_query),
        (w_cross_out, m_cross_out),
    )
    half = w_head.shape[2] // 2
    weights = [(src.at[0], dst) for src, dst in mats]
    weights += [(w_head.at[0, :, h * half : (h + 1) * half], m_head.at[h]) for h in range(2)]
    gain_refs = (g_self, g_query, g_memory, g_mlp, g_head)
    fcs = (w_fc1, w_fc2)

    def slot_at(step, ring):
        return 2 * step + ring

    def ring_view(step, kind, ring):
        place = ring_w.at[lax.rem(kind, 2), slot_at(step, ring)]
        if split == 1:
            return place
        return place.at[pl.ds(pl.multiple_of(lax.div(kind, 2) * rank, rank), rank)]

    def own_fc(which, piece):
        if split == 1:
            return fcs[which].at[0]
        return fcs[which].at[0, pl.ds(pl.multiple_of(piece * rank, rank), rank)]

    own_win = pltpu.make_async_copy(features.at[0], win.at[x, s], f_local)
    own_win.start()

    @pl.when(at_home)
    def _():
        for at, ref in enumerate(gain_refs):
            pltpu.make_async_copy(ref, gains.at[at], g_recv.at[at]).start()
        for which in range(2):
            pltpu.make_async_copy(
                own_fc(which, s), ring_view(0, which, s), r_recv.at[0, which]
            ).start()
        for at, (src, dst) in enumerate(weights):
            pltpu.make_async_copy(src, dst, w_recv.at[at]).start()

    barrier = pltpu.get_barrier_semaphore()
    for step in range(-2, 3):
        for flip in range(2):
            if step or flip:
                pl.semaphore_signal(
                    barrier, inc=1, device_id=(pair_of(step, flip), s), device_id_type=MESH
                )
    pl.semaphore_signal(barrier, inc=1, device_id=sibling, device_id_type=MESH)

    @pl.when(jnp.logical_not(at_home))
    def _():
        pl.semaphore_signal(barrier, inc=1, device_id=partner, device_id_type=MESH)

    pl.semaphore_wait(barrier, 10 + (1 - at_home.astype(jnp.int32)))

    table_out = [
        remote(slot_images, table, t_send.at[0], t_recv.at[0], (pair_of(0, 1), s)),
        remote(slot_count, counts, t_send.at[1], t_recv.at[1], (pair_of(0, 1), s)),
    ]
    across = (2 * q + s, s)
    if split == 1:
        fc_home = []
        fc_out = [
            remote(own_fc(f, 0), ring_view(0, f, x), s_send.at[f], r_recv.at[0, f], partner)
            for f in range(2)
        ]
    else:
        fc_home = [
            remote(
                own_fc(f, 1 - s), ring_view(0, f, 1 - s), s_send.at[f], r_recv.at[0, f], sibling
            )
            for f in range(2)
        ]
        fc_out = [
            remote(
                own_fc(f, ring), ring_view(0, 2 + f, ring), s_send.at[2 * f + to],
                r_recv.at[0, 2 + f], device,
            )
            for f in range(2)
            for to, (ring, device) in enumerate(((x, partner), (s, across)))
        ]
    gains_out = [
        remote(ref, gains.at[at], g_send.at[at], g_recv.at[at], sibling)
        for at, ref in enumerate(gain_refs)
    ]
    weights_out = [
        remote(src, dst, w_send.at[at], w_recv.at[at], sibling)
        for at, (src, dst) in enumerate(weights)
    ]

    def feature_out(block, place, step, flip, at):
        return remote(
            block, win.at[place, s], f_send.at[at], f_recv.at[place], (pair_of(-step, flip), s)
        )

    own = features.at[0]
    passed = win.at[1 - x, s]
    even = lax.rem(q, 2) == 0
    feature_across = feature_out(own, x, 0, 1, 0)
    near_zero = [feature_out(block, 2, 1, 0, 1) for block in (own, passed)]
    near_one = [feature_out(block, 3, 1, 0, 2) for block in (passed, own)]
    far_zero = [feature_out(block, WINDOW, 2, 0, 3) for block in (own, passed)]
    onto_next = feature_out(win.at[WINDOW, s], 2, -1, 0, 4)

    def zero_start(at):
        far_zero[at].start()

        @pl.when(jnp.logical_not(even))
        def _():
            near_zero[at].start()

    def relay(place, block=None):
        target = win.at[place, s]
        return remote(
            target if block is None else block, target, fr_send.at[place], fr_recv.at[place],
            sibling,
        )

    for copy in table_out:
        copy.start()
    feature_across.start()

    @pl.when(x == 0)
    def _():
        zero_start(0)

    @pl.when(x == 1)
    def _():
        near_one[1].start()

    relay(x, own).start()

    @pl.when(at_home)
    def _():
        for copy in fc_home + gains_out:
            copy.start()
        weights_out[0].start()

    @pl.when(jnp.logical_not(at_home))
    def _():
        for copy in fc_out:
            copy.start()

    def piece(number):
        turn = lax.div(number, kinds // 2)
        last = turn == 2 * chips - 1
        ahead = jnp.logical_or(turn == 0, jnp.logical_and(lax.rem(turn, 2) == 1, turn < 2 * chips - 1))
        step = jnp.where(
            turn == 0,
            0,
            jnp.where(last, chips - 1, jnp.where(ahead, lax.div(turn + 1, 2), lax.div(turn, 2) - 1)),
        )
        kind = lax.rem(number, kinds // 2) + jnp.where(ahead, 0, kinds // 2)
        block = ring_view(step, kind, s)
        pltpu.make_async_copy(block, block, r_recv.at[step, kind]).wait()

        @pl.when(step < chips - 1)
        def _():
            remote(
                block, ring_view(step + 1, kind, s), r_send.at[step, kind],
                r_recv.at[step + 1, kind], onward,
            ).start()

        remote(block, block, x_send.at[step, kind], x_recv.at[step, kind], sibling).start()

    def pieces(low, high):
        def body(number, carry):
            piece(number)
            return carry

        lax.fori_loop(low, high, body, 0)

    def arrived(place):
        block = win.at[place, s]
        pltpu.make_async_copy(block, block, f_recv.at[place]).wait()
        relay(place).start()

    group = kinds // 2
    early = 3 * group
    pieces(0, group)
    arrived(1 - x)

    @pl.when(x == 0)
    def _():
        near_one[0].start()

    @pl.when(x == 1)
    def _():
        zero_start(1)

    arrived(WINDOW)

    @pl.when(even)
    def _():
        onto_next.start()

    pieces(group, 2 * group)
    arrived(3)
    arrived(2)

    @pl.when(at_home)
    def _():
        for copy in weights_out[1:]:
            copy.start()

    pieces(2 * group, early)
    own_win.wait()
    for place in range(REACH):
        block = win.at[place, 1 - s]
        pltpu.make_async_copy(block, block, fr_recv.at[place]).wait()
    for copy in table_out:
        copy.wait_recv()
    for at, ref in enumerate(gain_refs):
        pltpu.make_async_copy(ref, gains.at[at], g_recv.at[at]).wait()

    def weight_wait(at):
        src, dst = weights[at]
        pltpu.make_async_copy(src, dst, w_recv.at[at]).wait()

    def first_wait(slot, at):
        @pl.when(slot == 0)
        def _():
            weight_wait(at)

    def entry(slot, column, core):
        local = slot_images[slot, column]
        return jnp.where(x == core, local, table[slot, column])

    def place_of(slot, column, core=None):
        core = s if core is None else core
        stored = image_slot[entry(slot, column, core)]
        ahead = lax.rem(stored - (2 * q + core) + devices, devices)
        return jnp.minimum(ahead, WINDOW - 1) + core

    def tokens_of(place):
        return jnp.concatenate([win[place, 0], win[place, 1]], axis=-1).astype(jnp.float32)

    stops = 6 * slots
    each = max((total_pieces * 26 // 32 - early) // stops, 0)
    fronted = early + each * stops

    def front(slot, carry):
        told = [0]

        def comm():
            base = early + (6 * slot + told[0]) * each
            told[0] += 1
            for at in range(each):
                piece(base + at)

        first_wait(slot, 0)
        tokens = tokens_of(place_of(slot, x))
        state = layer_norm(tokens, gains[0]).astype(jnp.bfloat16)
        triple[...] = matmul(state, m_qkv[...]).astype(jnp.bfloat16)
        comm()
        attend(triple, triple, triple, width, 2 * width, mixed, width, comm)
        first_wait(slot, 1)
        first = tokens + matmul(mixed[...], m_self_out[...])
        second[slot, 0:rows, :] = first
        comm()
        first_wait(slot, 2)
        first_wait(slot, 3)
        query_in = layer_norm(first, gains[1]).astype(jnp.bfloat16)
        memory = tokens_of(place_of(slot, 1 - x))
        memory_in = layer_norm(memory, gains[2]).astype(jnp.bfloat16)
        queries[...] = matmul(query_in, m_query[...]).astype(jnp.bfloat16)
        kv[...] = matmul(memory_in, m_memory[...]).astype(jnp.bfloat16)
        comm()
        attend(queries, kv, kv, 0, width, mixed, width, comm)
        first_wait(slot, 4)
        result = second[slot, 0:rows, :] + matmul(mixed[...], m_cross_out[...])
        second[slot, 0:rows, :] = result
        hidden[slot, 0:rows, :] = layer_norm(result, gains[3]).astype(jnp.bfloat16)
        comm()
        return carry

    second[...] = jnp.zeros_like(second)
    hidden[...] = jnp.zeros_like(hidden)
    lax.fori_loop(0, slots, front, 0)

    def relayed(first, steps):
        def body(at, carry):
            step, kind = first + lax.div(at, kinds), lax.rem(at, kinds)
            view = ring_view(step, kind, 1 - s)
            pltpu.make_async_copy(view, view, x_recv.at[step, kind]).wait()
            return carry

        lax.fori_loop(0, steps * kinds, body, 0)

    def expand(first, steps, slot):
        count = 2 * steps
        if shard % 16 == 0:
            groups = [
                [ring_w[f, pl.ds(2 * first, count)].reshape(count * shard, width) for f in range(2)]
            ]
        else:
            groups = [[ring_w[f, 2 * first + at] for f in range(2)] for at in range(count)]
        total = second[slot]
        for fc1, fc2 in groups:
            pre = matmul_t(hidden[slot], fc1)
            act = (pre * (1.0 + lax.erf(pre * 0.5**0.5)) * 0.5).astype(jnp.bfloat16)
            total = total + matmul(act, fc2)
        second[slot] = total

    whole = total_pieces - group
    left = whole - fronted
    places = (BLOCKS - 1) * slots
    rate = -(-left // (2 * slots))

    def expand_early(turn, carry):
        block, slot = lax.div(turn, slots), lax.rem(turn, slots)

        @pl.when(slot == 0)
        def _():
            relayed(block * per, per)

        expand(block * per, per, slot)
        pieces(
            fronted + jnp.minimum(turn * rate, left), fronted + jnp.minimum((turn + 1) * rate, left)
        )
        return carry

    lax.fori_loop(0, places, expand_early, 0)
    relayed((BLOCKS - 1) * per, per - 1)

    def expand_late(slot, carry):
        expand((BLOCKS - 1) * per, per - 1, slot)
        pieces(
            whole + lax.div(slot * group, slots), whole + lax.div((slot + 1) * group, slots)
        )
        return carry

    lax.fori_loop(0, slots, expand_late, 0)
    weight_wait(5)
    weight_wait(6)
    relayed(chips - 1, 1)
    pix = half // 4

    def terms(slot, which, target):
        raw[...] = matmul(hidden[slot], m_head[which])
        conf = 1.0 + jnp.exp(raw[0:rows, 3 * pix :])
        for comp in range(4):
            at = slice(comp * pix, (comp + 1) * pix)
            value = conf if comp == 3 else conf * raw[0:rows, at]
            target[slot, :, at] = value.astype(target.dtype)

    def away(slot):
        return remote(
            term_away.at[slot], term_in.at[slot], a_send.at[slot], a_recv.at[slot], sibling
        )

    def expand_last(slot, carry):
        expand(chips - 1, 1, slot)
        hidden[slot] = layer_norm(second[slot], gains[4]).astype(jnp.bfloat16)
        terms(slot, 1 - s, term_away)
        away(slot).start()
        return carry

    def own_terms(slot, carry):
        terms(slot, s, term)
        return carry

    lax.fori_loop(0, slots, expand_last, 0)
    lax.fori_loop(0, slots, own_terms, 0)
    for slot in range(slots):
        away(slot).wait_recv()

    sources = []
    for core, ref in ((s, term), (1 - s, term_in)):
        live = jnp.where(x == core, slot_count[0], counts[0])
        for slot in range(slots):
            sources.append((place_of(slot, x, core), slot < live, ref, slot))

    def sums_of(place):
        sums = jnp.zeros((rows, half), jnp.float32)
        for to, live, ref, slot in sources:
            chosen = jnp.logical_and(to == place, live)
            sums = sums + jnp.where(chosen, ref[slot].astype(jnp.float32), 0.0)
        return sums

    def far_copy(at, step, flip):
        return remote(
            far_out.at[at], far_in.at[at], b_send.at[at], b_recv.at[at], (pair_of(step, flip), s)
        )

    def far_send(at, step, flip, sums):
        far_out[at] = sums.astype(jnp.bfloat16)
        far_copy(at, step, flip).start()

    def far_wait(at):
        block = far_in.at[at]
        pltpu.make_async_copy(block, block, b_recv.at[at]).wait()
        return block[...].astype(jnp.float32)

    far_send(0, 2, 0, sums_of(WINDOW))
    far_send(1, 0, 1, sums_of(3 - x))

    @pl.when(x == 0)
    def _():
        far_send(3, 0, 1, sums_of(1))

    final[...] = sums_of(2 + x)
    far_send(2, 1, 0, final[...] + far_wait(1))
    final[...] = sums_of(x)

    @pl.when(x == 1)
    def _():
        far_send(3, 0, 1, sums_of(0) + far_wait(0))

    @pl.when(x == 0)
    def _():
        final[...] = final[...] + far_wait(0)

    final[...] = final[...] + far_wait(2)
    final[...] = final[...] + far_wait(3)
    conf = jnp.maximum(final[:, 3 * pix :], 1.0)
    for comp in range(3):
        at = slice(comp * pix, (comp + 1) * pix)
        out[0, :, at] = (final[:, at] / conf).astype(jnp.bfloat16)

    for copy in (feature_across, near_one[0], far_zero[0]):
        copy.wait_send()

    @pl.when(even)
    def _():
        onto_next.wait_send()

    @pl.when(jnp.logical_not(even))
    def _():
        near_zero[0].wait_send()

    for place in range(REACH):
        relay(place).wait_send()

    @pl.when(at_home)
    def _():
        for copy in fc_home + gains_out + weights_out:
            copy.wait_send()

    @pl.when(jnp.logical_not(at_home))
    def _():
        for copy in fc_out:
            copy.wait_send()

    for copy in table_out:
        copy.wait_send()

    def drain(number, carry):
        step, kind = lax.div(number, kinds), lax.rem(number, kinds)
        block = ring_view(step, kind, s)

        @pl.when(step < chips - 1)
        def _():
            remote(
                block, block, r_send.at[step, kind], r_recv.at[step, kind], onward
            ).wait_send()

        remote(block, block, x_send.at[step, kind], x_recv.at[step, kind], sibling).wait_send()
        return carry

    lax.fori_loop(0, total_pieces, drain, 0)
    for slot in range(slots):
        away(slot).wait_send()
    for at, (step, flip) in enumerate(((2, 0), (0, 1), (1, 0), (0, 1))):
        far_copy(at, step, flip).wait_send()


def on_device(
    features, image_slot, slot_images, slot_count, gain_self, gain_query, gain_memory, gain_mlp,
    gain_head, w_qkv, w_self_out, w_query, w_memory, w_cross_out, w_fc1, w_fc2, w_head,
):
    devices = lax.axis_size("pairs")
    chips = devices // 2
    blocks, rows, part = features.shape
    if blocks != 1 or chips % BLOCKS:
        raise ValueError("unsupported split")
    width = w_qkv.shape[1]
    slots = slot_images.shape[0]
    tall = padded(rows)
    shard = w_fc1.shape[1]
    kinds = 2 * (2 if shard % 32 == 0 else 1)
    half = w_head.shape[2] // 2
    bf16, f32 = jnp.bfloat16, jnp.float32
    dma = pltpu.SemaphoreType.DMA
    anywhere = pl.BlockSpec(memory_space=pl.ANY)
    return pl.pallas_call(
        decoder_kernel,
        out_shape=jax.ShapeDtypeStruct((1, rows, half * 3 // 4), bf16),
        in_specs=[pl.BlockSpec(memory_space=pltpu.SMEM)] * 3 + [anywhere] * 14,
        out_specs=pl.BlockSpec(memory_space=pltpu.VMEM),
        scratch_shapes=[
            pltpu.VMEM((REACH, 2, rows, part), bf16),
            pltpu.SMEM(slot_images.shape, jnp.int32),
            pltpu.SMEM(slot_count.shape, jnp.int32),
            pltpu.VMEM((5, 1, width), f32),
            pltpu.VMEM(w_qkv.shape[1:], bf16),
            pltpu.VMEM(w_self_out.shape[1:], bf16),
            pltpu.VMEM(w_query.shape[1:], bf16),
            pltpu.VMEM(w_memory.shape[1:], bf16),
            pltpu.VMEM(w_cross_out.shape[1:], bf16),
            pltpu.VMEM((2, width, half), bf16),
            pltpu.VMEM((2, devices, shard, width), bf16),
            pltpu.VMEM((rows, 3 * width), bf16),
            pltpu.VMEM((rows, 2 * width), bf16),
            pltpu.VMEM((rows, width), bf16),
            pltpu.VMEM((rows, width), bf16),
            pltpu.VMEM((slots, tall, width), f32),
            pltpu.VMEM((slots, tall, width), bf16),
            pltpu.VMEM((tall, half), f32),
            pltpu.VMEM((slots, rows, half), f32),
            pltpu.VMEM((slots, rows, half), bf16),
            pltpu.VMEM((slots, rows, half), bf16),
            pltpu.VMEM((4, rows, half), bf16),
            pltpu.VMEM((4, rows, half), bf16),
            pltpu.VMEM((rows, half), f32),
            dma, dma((5,)), dma((REACH,)), dma((REACH,)), dma((REACH,)),
            dma((2,)), dma((2,)), dma((5,)), dma((5,)), dma((7,)), dma((7,)),
            dma((kinds,)), dma((chips, kinds)), dma((chips, kinds)), dma((chips, kinds)),
            dma((chips, kinds)), dma((slots,)), dma((slots,)), dma((4,)), dma((4,)),
        ],
        compiler_params=pltpu.CompilerParams(
            collective_id=0, has_side_effects=True, vmem_limit_bytes=VMEM_LIMIT
        ),
    )(
        image_slot, slot_images, slot_count, features, gain_self, gain_query, gain_memory,
        gain_mlp, gain_head, w_qkv, w_self_out, w_query, w_memory, w_cross_out, w_fc1, w_fc2,
        w_head,
    )


def solution(mesh):
    placed = (
        P("pairs", None, "side"),
        P(),
        P("pairs", None),
        P("pairs"),
        P("side", None),
        P("side", None),
        P("side", None),
        P("side", None),
        P("side", None),
        P("side", None, None),
        P("side", None, None),
        P("side", None, None),
        P("side", None, None),
        P("side", None, None),
        P("side", "pairs", None),
        P("side", "pairs", None),
        P("side", None, None),
    )
    return jax.shard_map(
        on_device, mesh=mesh, in_specs=placed, out_specs=P("pairs", None, "side"), check_vma=False
    )
```

```python
import functools

import jax
import jax.numpy as jnp
from jax import lax
from jax.experimental import pallas as pl
from jax.experimental.pallas import tpu as pltpu
from jax.sharding import PartitionSpec as P

HEAD_DIM = 64
WINDOW = 4
PAIR = 2 * HEAD_DIM
BLOCKS = 4
REACH = WINDOW + 1
VMEM_LIMIT = 63 * 1024 * 1024
MESH = pl.DeviceIdType.MESH


def padded(rows):
    return -(-rows // 16) * 16


def layer_norm(values, gain):
    center = values - jnp.mean(values, axis=-1, keepdims=True)
    spread = jnp.mean(center * center, axis=-1, keepdims=True)
    return center * lax.rsqrt(spread + 1e-06) * gain


def matmul(left, right):
    return jnp.dot(left, right, preferred_element_type=jnp.float32)


def matmul_t(left, right):
    return lax.dot_general(
        left, right, (((1,), (1,)), ((), ())), preferred_element_type=jnp.float32
    )


def attend(q_ref, k_ref, v_ref, k_at, v_at, o_ref, width, comm):
    rows = q_ref.shape[0]
    low = lax.broadcasted_iota(jnp.int32, (rows, PAIR), 1) < HEAD_DIM
    for pair in range(width // PAIR):
        if comm is not None and pair * PAIR == width // 2:
            comm()
        q = q_ref[:, pair * PAIR : (pair + 1) * PAIR]
        k = k_ref[:, k_at + pair * PAIR : k_at + (pair + 1) * PAIR]
        v = v_ref[:, v_at + pair * PAIR : v_at + (pair + 1) * PAIR]
        mixed = None
        for keep in (low, jnp.logical_not(low)):
            q_head = jnp.where(keep, q, jnp.zeros_like(q))
            v_head = jnp.where(keep, v, jnp.zeros_like(v))
            scores = matmul_t(q_head, k) * HEAD_DIM ** (-0.5)
            expon = jnp.exp(scores)
            weights = (expon / jnp.sum(expon, axis=-1, keepdims=True)).astype(jnp.bfloat16)
            part = matmul(weights, v_head)
            mixed = part if mixed is None else mixed + part
        o_ref[:, pair * PAIR : (pair + 1) * PAIR] = mixed.astype(jnp.bfloat16)


def remote(src, dst, send, recv, device):
    return pltpu.make_async_remote_copy(
        src_ref=src, dst_ref=dst, send_sem=send, recv_sem=recv, device_id=device,
        device_id_type=MESH,
    )


def decoder_kernel(
    image_slot, slot_images, slot_count, features,
    g_self, g_query, g_memory, g_mlp, g_head,
    w_qkv, w_self_out, w_query, w_memory, w_cross_out, w_fc1, w_fc2, w_head,
    out,
    win, table, counts, gains, m_qkv, m_self_out, m_query, m_memory, m_cross_out, m_head, ring_w,
    triple, kv, queries, mixed, second, hidden, raw, term, term_away, term_in, far_out, far_in,
    final,
    f_local, f_send, f_recv, fr_send, fr_recv, t_send, t_recv, g_send, g_recv, w_send, w_recv,
    s_send, r_send, r_recv, x_send, x_recv, a_send, a_recv, b_send, b_recv,
):
    devices = lax.axis_size("pairs")
    chips = devices // 2
    here = lax.axis_index("pairs")
    s = lax.axis_index("side")
    x = lax.rem(here, 2)
    q = lax.div(here, 2)
    rows = features.shape[1]
    width = m_qkv.shape[0]
    slots = second.shape[0]
    tall = second.shape[1]
    per = chips // BLOCKS
    shard = ring_w.shape[2]
    split = 2 if shard % 32 == 0 else 1
    kinds = 2 * split
    rank = shard // split
    total_pieces = kinds * chips

    sibling = (here, 1 - s)
    partner = (2 * q + s, x)
    at_home = x == s

    def pair_of(step, flip):
        chip = lax.rem(q + (step + chips), chips)
        return 2 * chip + (1 - x if flip else x)

    up = jnp.where(
        lax.rem(q, 2) == 0,
        jnp.where(q + 2 < chips, q + 2, chips - 1),
        jnp.where(q >= 3, q - 2, 0),
    )
    down = jnp.where(
        lax.rem(q, 2) == 0,
        jnp.where(q == 0, 1, q - 2),
        jnp.where(q + 2 < chips, q + 2, chips - 2),
    )
    onward = (2 * jnp.where(s == 0, up, down) + x, s)

    mats = (
        (w_qkv, m_qkv), (w_self_out, m_self_out), (w_memory, m_memory), (w_query, m_query),
        (w_cross_out, m_cross_out),
    )
    half = w_head.shape[2] // 2
    weights = [(src.at[0], dst) for src, dst in mats]
    weights += [(w_head.at[0, :, h * half : (h + 1) * half], m_head.at[h]) for h in range(2)]
    gain_refs = (g_self, g_query, g_memory, g_mlp, g_head)
    fcs = (w_fc1, w_fc2)

    def slot_at(step, ring):
        return 2 * step + ring

    def ring_view(step, kind, ring):
        place = ring_w.at[lax.rem(kind, 2), slot_at(step, ring)]
        if split == 1:
            return place
        return place.at[pl.ds(pl.multiple_of(lax.div(kind, 2) * rank, rank), rank)]

    def own_fc(which, piece):
        if split == 1:
            return fcs[which].at[0]
        return fcs[which].at[0, pl.ds(pl.multiple_of(piece * rank, rank), rank)]

    own_win = pltpu.make_async_copy(features.at[0], win.at[x, s], f_local)
    own_win.start()

    @pl.when(at_home)
    def _():
        for at, ref in enumerate(gain_refs):
            pltpu.make_async_copy(ref, gains.at[at], g_recv.at[at]).start()
        for which in range(2):
            pltpu.make_async_copy(
                own_fc(which, s), ring_view(0, which, s), r_recv.at[0, which]
            ).start()
        for at, (src, dst) in enumerate(weights):
            pltpu.make_async_copy(src, dst, w_recv.at[at]).start()

    barrier = pltpu.get_barrier_semaphore()
    for step in range(-2, 3):
        for flip in range(2):
            if step or flip:
                pl.semaphore_signal(
                    barrier, inc=1, device_id=(pair_of(step, flip), s), device_id_type=MESH
                )
    pl.semaphore_signal(barrier, inc=1, device_id=sibling, device_id_type=MESH)

    @pl.when(jnp.logical_not(at_home))
    def _():
        pl.semaphore_signal(barrier, inc=1, device_id=partner, device_id_type=MESH)

    pl.semaphore_wait(barrier, 10 + (1 - at_home.astype(jnp.int32)))

    table_out = [
        remote(slot_images, table, t_send.at[0], t_recv.at[0], (pair_of(0, 1), s)),
        remote(slot_count, counts, t_send.at[1], t_recv.at[1], (pair_of(0, 1), s)),
    ]
    across = (2 * q + s, s)
    if split == 1:
        fc_home = []
        fc_out = [
            remote(own_fc(f, 0), ring_view(0, f, x), s_send.at[f], r_recv.at[0, f], partner)
            for f in range(2)
        ]
    else:
        fc_home = [
            remote(
                own_fc(f, 1 - s), ring_view(0, f, 1 - s), s_send.at[f], r_recv.at[0, f], sibling
            )
            for f in range(2)
        ]
        fc_out = [
            remote(
                own_fc(f, ring), ring_view(0, 2 + f, ring), s_send.at[2 * f + to],
                r_recv.at[0, 2 + f], device,
            )
            for f in range(2)
            for to, (ring, device) in enumerate(((x, partner), (s, across)))
        ]
    gains_out = [
        remote(ref, gains.at[at], g_send.at[at], g_recv.at[at], sibling)
        for at, ref in enumerate(gain_refs)
    ]
    weights_out = [
        remote(src, dst, w_send.at[at], w_recv.at[at], sibling)
        for at, (src, dst) in enumerate(weights)
    ]

    def feature_out(block, place, step, flip, at):
        return remote(
            block, win.at[place, s], f_send.at[at], f_recv.at[place], (pair_of(-step, flip), s)
        )

    own = features.at[0]
    passed = win.at[1 - x, s]
    even = lax.rem(q, 2) == 0
    feature_across = feature_out(own, x, 0, 1, 0)
    near_zero = [feature_out(block, 2, 1, 0, 1) for block in (own, passed)]
    near_one = [feature_out(block, 3, 1, 0, 2) for block in (passed, own)]
    far_zero = feature_out(own, WINDOW, 2, 0, 3)
    onto_next = feature_out(win.at[WINDOW, s], 2, -1, 0, 4)
    far_across = feature_out(win.at[WINDOW, s], WINDOW, 0, 1, 5)

    def relay(place, block=None):
        target = win.at[place, s]
        return remote(
            target if block is None else block, target, fr_send.at[place], fr_recv.at[place],
            sibling,
        )

    for copy in table_out:
        copy.start()
    feature_across.start()

    @pl.when(x == 0)
    def _():
        far_zero.start()

        @pl.when(jnp.logical_not(even))
        def _():
            near_zero[0].start()

    @pl.when(x == 1)
    def _():
        near_one[1].start()

    relay(x, own).start()

    @pl.when(at_home)
    def _():
        for copy in fc_home + gains_out:
            copy.start()
        weights_out[0].start()

    @pl.when(jnp.logical_not(at_home))
    def _():
        for copy in fc_out:
            copy.start()

    def piece(number):
        turn = lax.div(number, kinds // 2)
        last = turn == 2 * chips - 1
        ahead = jnp.logical_or(turn == 0, jnp.logical_and(lax.rem(turn, 2) == 1, turn < 2 * chips - 1))
        step = jnp.where(
            turn == 0,
            0,
            jnp.where(last, chips - 1, jnp.where(ahead, lax.div(turn + 1, 2), lax.div(turn, 2) - 1)),
        )
        kind = lax.rem(number, kinds // 2) + jnp.where(ahead, 0, kinds // 2)
        block = ring_view(step, kind, s)
        pltpu.make_async_copy(block, block, r_recv.at[step, kind]).wait()

        @pl.when(step < chips - 1)
        def _():
            remote(
                block, ring_view(step + 1, kind, s), r_send.at[step, kind],
                r_recv.at[step + 1, kind], onward,
            ).start()

        remote(block, block, x_send.at[step, kind], x_recv.at[step, kind], sibling).start()

    def pieces(low, high):
        def body(number, carry):
            piece(number)
            return carry

        lax.fori_loop(low, high, body, 0)

    def arrived(place):
        block = win.at[place, s]
        pltpu.make_async_copy(block, block, f_recv.at[place]).wait()
        relay(place).start()

    group = kinds // 2
    early = 5 * group
    pieces(0, group)
    arrived(1 - x)

    @pl.when(x == 0)
    def _():
        near_one[0].start()
        arrived(WINDOW)

        @pl.when(even)
        def _():
            onto_next.start()

        far_across.start()

    @pl.when(x == 1)
    def _():
        near_zero[1].start()

    @pl.when(at_home)
    def _():
        weights_out[1].start()

    pieces(group, 2 * group)
    arrived(3)

    @pl.when(x == 1)
    def _():
        arrived(WINDOW)

    pieces(2 * group, 4 * group)
    arrived(2)

    @pl.when(at_home)
    def _():
        for copy in weights_out[2:]:
            copy.start()

    pieces(4 * group, early)
    own_win.wait()
    for place in range(REACH):
        block = win.at[place, 1 - s]
        pltpu.make_async_copy(block, block, fr_recv.at[place]).wait()
    for copy in table_out:
        copy.wait_recv()
    for at, ref in enumerate(gain_refs):
        pltpu.make_async_copy(ref, gains.at[at], g_recv.at[at]).wait()

    def weight_wait(at):
        src, dst = weights[at]
        pltpu.make_async_copy(src, dst, w_recv.at[at]).wait()

    def first_wait(slot, at):
        @pl.when(slot == 0)
        def _():
            weight_wait(at)

    def entry(slot, column, core):
        local = slot_images[slot, column]
        return jnp.where(x == core, local, table[slot, column])

    def place_of(slot, column, core=None):
        core = s if core is None else core
        stored = image_slot[entry(slot, column, core)]
        ahead = lax.rem(stored - (2 * q + core) + devices, devices)
        return jnp.minimum(ahead, WINDOW - 1) + core

    def tokens_of(place):
        return jnp.concatenate([win[place, 0], win[place, 1]], axis=-1).astype(jnp.float32)

    stops = 5 * slots
    each = max((total_pieces * 26 // 32 - early) // stops, 0)
    fronted = early + each * stops

    def front(slot, carry):
        told = [0]

        def comm():
            base = early + (5 * slot + told[0]) * each
            told[0] += 1
            for at in range(each):
                piece(base + at)

        first_wait(slot, 0)
        tokens = tokens_of(place_of(slot, x))
        state = layer_norm(tokens, gains[0]).astype(jnp.bfloat16)
        triple[...] = matmul(state, m_qkv[...]).astype(jnp.bfloat16)
        comm()
        attend(triple, triple, triple, width, 2 * width, mixed, width, comm)
        first_wait(slot, 1)
        first = tokens + matmul(mixed[...], m_self_out[...])
        second[slot, 0:rows, :] = first
        comm()
        first_wait(slot, 2)
        first_wait(slot, 3)
        query_in = layer_norm(first, gains[1]).astype(jnp.bfloat16)
        memory = tokens_of(place_of(slot, 1 - x))
        memory_in = layer_norm(memory, gains[2]).astype(jnp.bfloat16)
        queries[...] = matmul(query_in, m_query[...]).astype(jnp.bfloat16)
        kv[...] = matmul(memory_in, m_memory[...]).astype(jnp.bfloat16)
        comm()
        attend(queries, kv, kv, 0, width, mixed, width, None)
        first_wait(slot, 4)
        result = second[slot, 0:rows, :] + matmul(mixed[...], m_cross_out[...])
        second[slot, 0:rows, :] = result
        hidden[slot, 0:rows, :] = layer_norm(result, gains[3]).astype(jnp.bfloat16)
        comm()
        return carry

    second[...] = jnp.zeros_like(second)
    hidden[...] = jnp.zeros_like(hidden)
    lax.fori_loop(0, slots, front, 0)

    def relayed(first, steps):
        def body(at, carry):
            step, kind = first + lax.div(at, kinds), lax.rem(at, kinds)
            view = ring_view(step, kind, 1 - s)
            pltpu.make_async_copy(view, view, x_recv.at[step, kind]).wait()
            return carry

        lax.fori_loop(0, steps * kinds, body, 0)

    def expand(first, steps, slot):
        count = 2 * steps
        if shard % 16 == 0:
            groups = [
                [ring_w[f, pl.ds(2 * first, count)].reshape(count * shard, width) for f in range(2)]
            ]
        else:
            groups = [[ring_w[f, 2 * first + at] for f in range(2)] for at in range(count)]
        total = second[slot]
        for fc1, fc2 in groups:
            pre = matmul_t(hidden[slot], fc1)
            act = (pre * (1.0 + lax.erf(pre * 0.5**0.5)) * 0.5).astype(jnp.bfloat16)
            total = total + matmul(act, fc2)
        second[slot] = total

    whole = total_pieces - group
    left = whole - fronted
    places = (BLOCKS - 1) * slots
    rate = -(-left // (2 * slots))

    def expand_early(turn, carry):
        block, slot = lax.div(turn, slots), lax.rem(turn, slots)

        @pl.when(slot == 0)
        def _():
            relayed(block * per, per)

        expand(block * per, per, slot)
        pieces(
            fronted + jnp.minimum(turn * rate, left), fronted + jnp.minimum((turn + 1) * rate, left)
        )
        return carry

    lax.fori_loop(0, places, expand_early, 0)
    relayed((BLOCKS - 1) * per, per - 1)

    def expand_late(slot, carry):
        expand((BLOCKS - 1) * per, per - 1, slot)
        pieces(
            whole + lax.div(slot * group, slots), whole + lax.div((slot + 1) * group, slots)
        )
        return carry

    lax.fori_loop(0, slots, expand_late, 0)
    weight_wait(5)
    weight_wait(6)
    relayed(chips - 1, 1)
    pix = half // 4

    def terms(slot, which, target):
        raw[...] = matmul(hidden[slot], m_head[which])
        conf = 1.0 + jnp.exp(raw[0:rows, 3 * pix :])
        for comp in range(4):
            at = slice(comp * pix, (comp + 1) * pix)
            value = conf if comp == 3 else conf * raw[0:rows, at]
            target[slot, :, at] = value.astype(target.dtype)

    def away(slot):
        return remote(
            term_away.at[slot], term_in.at[slot], a_send.at[slot], a_recv.at[slot], sibling
        )

    def expand_last(slot, carry):
        expand(chips - 1, 1, slot)
        hidden[slot] = layer_norm(second[slot], gains[4]).astype(jnp.bfloat16)
        terms(slot, 1 - s, term_away)
        away(slot).start()
        return carry

    def own_terms(slot, carry):
        terms(slot, s, term)
        return carry

    lax.fori_loop(0, slots, expand_last, 0)
    lax.fori_loop(0, slots, own_terms, 0)
    for slot in range(slots):
        away(slot).wait_recv()

    sources = []
    for core, ref in ((s, term), (1 - s, term_in)):
        live = jnp.where(x == core, slot_count[0], counts[0])
        for slot in range(slots):
            sources.append((place_of(slot, x, core), slot < live, ref, slot))

    def sums_of(place):
        sums = jnp.zeros((rows, half), jnp.float32)
        for to, live, ref, slot in sources:
            chosen = jnp.logical_and(to == place, live)
            sums = sums + jnp.where(chosen, ref[slot].astype(jnp.float32), 0.0)
        return sums

    def far_copy(at, step, flip):
        return remote(
            far_out.at[at], far_in.at[at], b_send.at[at], b_recv.at[at], (pair_of(step, flip), s)
        )

    def far_send(at, step, flip, sums):
        far_out[at] = sums.astype(jnp.bfloat16)
        far_copy(at, step, flip).start()

    def far_wait(at):
        block = far_in.at[at]
        pltpu.make_async_copy(block, block, b_recv.at[at]).wait()
        return block[...].astype(jnp.float32)

    far_send(0, 2, 0, sums_of(WINDOW))
    far_send(1, 0, 1, sums_of(3 - x))

    @pl.when(x == 0)
    def _():
        far_send(3, 0, 1, sums_of(1))

    final[...] = sums_of(2 + x)
    far_send(2, 1, 0, final[...] + far_wait(1))
    final[...] = sums_of(x)

    @pl.when(x == 1)
    def _():
        far_send(3, 0, 1, sums_of(0) + far_wait(0))

    @pl.when(x == 0)
    def _():
        final[...] = final[...] + far_wait(0)

    final[...] = final[...] + far_wait(2)
    final[...] = final[...] + far_wait(3)
    conf = jnp.maximum(final[:, 3 * pix :], 1.0)
    for comp in range(3):
        at = slice(comp * pix, (comp + 1) * pix)
        out[0, :, at] = (final[:, at] / conf).astype(jnp.bfloat16)

    for copy in (feature_across, near_one[0]):
        copy.wait_send()

    @pl.when(x == 0)
    def _():
        far_zero.wait_send()
        far_across.wait_send()

        @pl.when(even)
        def _():
            onto_next.wait_send()

    @pl.when(jnp.logical_or(x == 1, jnp.logical_not(even)))
    def _():
        near_zero[0].wait_send()

    for place in range(REACH):
        relay(place).wait_send()

    @pl.when(at_home)
    def _():
        for copy in fc_home + gains_out + weights_out:
            copy.wait_send()

    @pl.when(jnp.logical_not(at_home))
    def _():
        for copy in fc_out:
            copy.wait_send()

    for copy in table_out:
        copy.wait_send()

    def drain(number, carry):
        step, kind = lax.div(number, kinds), lax.rem(number, kinds)
        block = ring_view(step, kind, s)

        @pl.when(step < chips - 1)
        def _():
            remote(
                block, block, r_send.at[step, kind], r_recv.at[step, kind], onward
            ).wait_send()

        remote(block, block, x_send.at[step, kind], x_recv.at[step, kind], sibling).wait_send()
        return carry

    lax.fori_loop(0, total_pieces, drain, 0)
    for slot in range(slots):
        away(slot).wait_send()
    for at, (step, flip) in enumerate(((2, 0), (0, 1), (1, 0), (0, 1))):
        far_copy(at, step, flip).wait_send()


def on_device(
    features, image_slot, slot_images, slot_count, gain_self, gain_query, gain_memory, gain_mlp,
    gain_head, w_qkv, w_self_out, w_query, w_memory, w_cross_out, w_fc1, w_fc2, w_head,
):
    devices = lax.axis_size("pairs")
    chips = devices // 2
    blocks, rows, part = features.shape
    if blocks != 1 or chips % BLOCKS:
        raise ValueError("unsupported split")
    width = w_qkv.shape[1]
    slots = slot_images.shape[0]
    tall = padded(rows)
    shard = w_fc1.shape[1]
    kinds = 2 * (2 if shard % 32 == 0 else 1)
    half = w_head.shape[2] // 2
    bf16, f32 = jnp.bfloat16, jnp.float32
    dma = pltpu.SemaphoreType.DMA
    anywhere = pl.BlockSpec(memory_space=pl.ANY)
    return pl.pallas_call(
        decoder_kernel,
        out_shape=jax.ShapeDtypeStruct((1, rows, half * 3 // 4), bf16),
        in_specs=[pl.BlockSpec(memory_space=pltpu.SMEM)] * 3 + [anywhere] * 14,
        out_specs=pl.BlockSpec(memory_space=pltpu.VMEM),
        scratch_shapes=[
            pltpu.VMEM((REACH, 2, rows, part), bf16),
            pltpu.SMEM(slot_images.shape, jnp.int32),
            pltpu.SMEM(slot_count.shape, jnp.int32),
            pltpu.VMEM((5, 1, width), f32),
            pltpu.VMEM(w_qkv.shape[1:], bf16),
            pltpu.VMEM(w_self_out.shape[1:], bf16),
            pltpu.VMEM(w_query.shape[1:], bf16),
            pltpu.VMEM(w_memory.shape[1:], bf16),
            pltpu.VMEM(w_cross_out.shape[1:], bf16),
            pltpu.VMEM((2, width, half), bf16),
            pltpu.VMEM((2, devices, shard, width), bf16),
            pltpu.VMEM((rows, 3 * width), bf16),
            pltpu.VMEM((rows, 2 * width), bf16),
            pltpu.VMEM((rows, width), bf16),
            pltpu.VMEM((rows, width), bf16),
            pltpu.VMEM((slots, tall, width), f32),
            pltpu.VMEM((slots, tall, width), bf16),
            pltpu.VMEM((tall, half), f32),
            pltpu.VMEM((slots, rows, half), f32),
            pltpu.VMEM((slots, rows, half), bf16),
            pltpu.VMEM((slots, rows, half), bf16),
            pltpu.VMEM((4, rows, half), bf16),
            pltpu.VMEM((4, rows, half), bf16),
            pltpu.VMEM((rows, half), f32),
            dma, dma((6,)), dma((REACH,)), dma((REACH,)), dma((REACH,)),
            dma((2,)), dma((2,)), dma((5,)), dma((5,)), dma((7,)), dma((7,)),
            dma((kinds,)), dma((chips, kinds)), dma((chips, kinds)), dma((chips, kinds)),
            dma((chips, kinds)), dma((slots,)), dma((slots,)), dma((4,)), dma((4,)),
        ],
        compiler_params=pltpu.CompilerParams(
            collective_id=0, has_side_effects=True, vmem_limit_bytes=VMEM_LIMIT
        ),
    )(
        image_slot, slot_images, slot_count, features, gain_self, gain_query, gain_memory,
        gain_mlp, gain_head, w_qkv, w_self_out, w_query, w_memory, w_cross_out, w_fc1, w_fc2,
        w_head,
    )


def solution(mesh):
    placed = (
        P("pairs", None, "side"),
        P(),
        P("pairs", None),
        P("pairs"),
        P("side", None),
        P("side", None),
        P("side", None),
        P("side", None),
        P("side", None),
        P("side", None, None),
        P("side", None, None),
        P("side", None, None),
        P("side", None, None),
        P("side", None, None),
        P("side", "pairs", None),
        P("side", "pairs", None),
        P("side", None, None),
    )
    return jax.shard_map(
        on_device, mesh=mesh, in_specs=placed, out_specs=P("pairs", None, "side"), check_vma=False
    )
```

```python
import functools

import jax
import jax.numpy as jnp
from jax import lax
from jax.experimental import pallas as pl
from jax.experimental.pallas import tpu as pltpu
from jax.sharding import PartitionSpec as P

HEAD_DIM = 64
WINDOW = 4
PAIR = 2 * HEAD_DIM
BLOCKS = 4
REACH = WINDOW + 1
VMEM_LIMIT = 63 * 1024 * 1024
MESH = pl.DeviceIdType.MESH


def padded(rows):
    return -(-rows // 16) * 16


def layer_norm(values, gain):
    center = values - jnp.mean(values, axis=-1, keepdims=True)
    spread = jnp.mean(center * center, axis=-1, keepdims=True)
    return center * lax.rsqrt(spread + 1e-06) * gain


def matmul(left, right):
    return jnp.dot(left, right, preferred_element_type=jnp.float32)


def matmul_t(left, right):
    return lax.dot_general(
        left, right, (((1,), (1,)), ((), ())), preferred_element_type=jnp.float32
    )


def attend(q_ref, k_ref, v_ref, k_at, v_at, o_ref, width, comm):
    rows = q_ref.shape[0]
    low = lax.broadcasted_iota(jnp.int32, (rows, PAIR), 1) < HEAD_DIM
    for pair in range(width // PAIR):
        if comm is not None and pair * PAIR == width // 2:
            comm()
        q = q_ref[:, pair * PAIR : (pair + 1) * PAIR]
        k = k_ref[:, k_at + pair * PAIR : k_at + (pair + 1) * PAIR]
        v = v_ref[:, v_at + pair * PAIR : v_at + (pair + 1) * PAIR]
        mixed = None
        for keep in (low, jnp.logical_not(low)):
            q_head = jnp.where(keep, q, jnp.zeros_like(q))
            v_head = jnp.where(keep, v, jnp.zeros_like(v))
            scores = matmul_t(q_head, k) * HEAD_DIM ** (-0.5)
            expon = jnp.exp(scores)
            weights = (expon / jnp.sum(expon, axis=-1, keepdims=True)).astype(jnp.bfloat16)
            part = matmul(weights, v_head)
            mixed = part if mixed is None else mixed + part
        o_ref[:, pair * PAIR : (pair + 1) * PAIR] = mixed.astype(jnp.bfloat16)


def remote(src, dst, send, recv, device):
    return pltpu.make_async_remote_copy(
        src_ref=src, dst_ref=dst, send_sem=send, recv_sem=recv, device_id=device,
        device_id_type=MESH,
    )


def decoder_kernel(
    image_slot, slot_images, slot_count, features,
    g_self, g_query, g_memory, g_mlp, g_head,
    w_qkv, w_self_out, w_query, w_memory, w_cross_out, w_fc1, w_fc2, w_head,
    out,
    win, table, counts, gains, m_qkv, m_self_out, m_query, m_memory, m_cross_out, m_head, ring_w,
    triple, kv, queries, mixed, second, hidden, raw, term, term_away, term_in, far_out, far_in,
    final,
    f_local, f_send, f_recv, fr_send, fr_recv, t_send, t_recv, g_send, g_recv, w_send, w_recv,
    s_send, r_send, r_recv, x_send, x_recv, a_send, a_recv, b_send, b_recv,
):
    devices = lax.axis_size("pairs")
    chips = devices // 2
    here = lax.axis_index("pairs")
    s = lax.axis_index("side")
    x = lax.rem(here, 2)
    q = lax.div(here, 2)
    rows = features.shape[1]
    width = m_qkv.shape[0]
    slots = second.shape[0]
    tall = second.shape[1]
    shard = w_fc1.shape[1]
    rank = ring_w.shape[2]
    split = shard // rank
    kinds = 2 * split
    total_pieces = kinds * chips

    sibling = (here, 1 - s)
    partner = (2 * q + s, x)
    at_home = x == s

    def pair_of(step, flip):
        chip = lax.rem(q + (step + chips), chips)
        return 2 * chip + (1 - x if flip else x)

    up = jnp.where(
        lax.rem(q, 2) == 0,
        jnp.where(q + 2 < chips, q + 2, chips - 1),
        jnp.where(q >= 3, q - 2, 0),
    )
    down = jnp.where(
        lax.rem(q, 2) == 0,
        jnp.where(q == 0, 1, q - 2),
        jnp.where(q + 2 < chips, q + 2, chips - 2),
    )
    onward = (2 * jnp.where(s == 0, up, down) + x, s)

    mats = (
        (w_qkv, m_qkv), (w_self_out, m_self_out), (w_memory, m_memory), (w_query, m_query),
        (w_cross_out, m_cross_out),
    )
    half = w_head.shape[2] // 2
    weights = [(src.at[0], dst) for src, dst in mats]
    weights += [(w_head.at[0, :, h * half : (h + 1) * half], m_head.at[h]) for h in range(2)]
    gain_refs = (g_self, g_query, g_memory, g_mlp, g_head)
    fcs = (w_fc1, w_fc2)

    def ring_view(step, kind, ring):
        return ring_w.at[lax.rem(kind, 2), 2 * (split * step + lax.div(kind, 2)) + ring]

    def own_fc(which, piece):
        if split == 1:
            return fcs[which].at[0]
        return fcs[which].at[0, pl.ds(pl.multiple_of(piece * rank, rank), rank)]

    own_win = pltpu.make_async_copy(features.at[0], win.at[x, s], f_local)
    own_win.start()

    @pl.when(at_home)
    def _():
        for at, ref in enumerate(gain_refs):
            pltpu.make_async_copy(ref, gains.at[at], g_recv.at[at]).start()
        for which in range(2):
            pltpu.make_async_copy(
                own_fc(which, s), ring_view(0, which, s), r_recv.at[0, which]
            ).start()
        for at, (src, dst) in enumerate(weights):
            pltpu.make_async_copy(src, dst, w_recv.at[at]).start()

    barrier = pltpu.get_barrier_semaphore()
    for step in range(-2, 3):
        for flip in range(2):
            if step or flip:
                pl.semaphore_signal(
                    barrier, inc=1, device_id=(pair_of(step, flip), s), device_id_type=MESH
                )
    pl.semaphore_signal(barrier, inc=1, device_id=sibling, device_id_type=MESH)

    @pl.when(jnp.logical_not(at_home))
    def _():
        pl.semaphore_signal(barrier, inc=1, device_id=partner, device_id_type=MESH)

    pl.semaphore_wait(barrier, 10 + (1 - at_home.astype(jnp.int32)))

    table_out = [
        remote(slot_images, table, t_send.at[0], t_recv.at[0], (pair_of(0, 1), s)),
        remote(slot_count, counts, t_send.at[1], t_recv.at[1], (pair_of(0, 1), s)),
    ]
    across = (2 * q + s, s)
    if split == 1:
        fc_home = []
        fc_out = [
            remote(own_fc(f, 0), ring_view(0, f, x), s_send.at[f], r_recv.at[0, f], partner)
            for f in range(2)
        ]
    else:
        fc_home = [
            remote(
                own_fc(f, 1 - s), ring_view(0, f, 1 - s), s_send.at[f], r_recv.at[0, f], sibling
            )
            for f in range(2)
        ]
        fc_out = [
            remote(
                own_fc(f, ring), ring_view(0, 2 + f, ring), s_send.at[2 * f + to],
                r_recv.at[0, 2 + f], device,
            )
            for f in range(2)
            for to, (ring, device) in enumerate(((x, partner), (s, across)))
        ]
    gains_out = [
        remote(ref, gains.at[at], g_send.at[at], g_recv.at[at], sibling)
        for at, ref in enumerate(gain_refs)
    ]
    weights_out = [
        remote(src, dst, w_send.at[at], w_recv.at[at], sibling)
        for at, (src, dst) in enumerate(weights)
    ]

    def feature_out(block, place, step, flip, at):
        return remote(
            block, win.at[place, s], f_send.at[at], f_recv.at[place], (pair_of(-step, flip), s)
        )

    own = features.at[0]
    passed = win.at[1 - x, s]
    even = lax.rem(q, 2) == 0
    feature_across = feature_out(own, x, 0, 1, 0)
    near_zero = [feature_out(block, 2, 1, 0, 1) for block in (own, passed)]
    near_one = [feature_out(block, 3, 1, 0, 2) for block in (passed, own)]
    far_zero = feature_out(own, WINDOW, 2, 0, 3)
    onto_next = feature_out(win.at[WINDOW, s], 2, -1, 0, 4)
    far_across = feature_out(win.at[WINDOW, s], WINDOW, 0, 1, 5)

    def relay(place, block=None):
        target = win.at[place, s]
        return remote(
            target if block is None else block, target, fr_send.at[place], fr_recv.at[place],
            sibling,
        )

    for copy in table_out:
        copy.start()
    feature_across.start()

    @pl.when(x == 0)
    def _():
        far_zero.start()

        @pl.when(jnp.logical_not(even))
        def _():
            near_zero[0].start()

    @pl.when(x == 1)
    def _():
        near_one[1].start()

    relay(x, own).start()

    @pl.when(at_home)
    def _():
        for copy in fc_home + gains_out:
            copy.start()
        weights_out[0].start()

    swapped = len(fc_out) // 2

    @pl.when(jnp.logical_not(at_home))
    def _():
        for copy in fc_out[:swapped]:
            copy.start()

        @pl.when(x == 1)
        def _():
            for copy in fc_out[swapped:]:
                copy.start()

    def piece(number):
        turn = lax.div(number, kinds // 2)
        last = turn == 2 * chips - 1
        ahead = jnp.logical_or(turn == 0, jnp.logical_and(lax.rem(turn, 2) == 1, turn < 2 * chips - 1))
        step = jnp.where(
            turn == 0,
            0,
            jnp.where(last, chips - 1, jnp.where(ahead, lax.div(turn + 1, 2), lax.div(turn, 2) - 1)),
        )
        kind = lax.rem(number, kinds // 2) + jnp.where(ahead, 0, kinds // 2)
        block = ring_view(step, kind, s)
        pltpu.make_async_copy(block, block, r_recv.at[step, kind]).wait()

        @pl.when(step < chips - 1)
        def _():
            remote(
                block, ring_view(step + 1, kind, s), r_send.at[step, kind],
                r_recv.at[step + 1, kind], onward,
            ).start()

        remote(block, block, x_send.at[step, kind], x_recv.at[step, kind], sibling).start()

    def pieces(low, high):
        def body(number, carry):
            piece(number)
            return carry

        lax.fori_loop(low, high, body, 0)

    def arrived(place):
        block = win.at[place, s]
        pltpu.make_async_copy(block, block, f_recv.at[place]).wait()
        relay(place).start()

    group = kinds // 2
    early = 5 * group
    pieces(0, group)
    arrived(1 - x)

    @pl.when(x == 0)
    def _():
        near_one[0].start()
        arrived(WINDOW)

        @pl.when(even)
        def _():
            onto_next.start()

        far_across.start()

        @pl.when(jnp.logical_not(at_home))
        def _():
            for copy in fc_out[swapped:]:
                copy.start()

    @pl.when(x == 1)
    def _():
        near_zero[1].start()

    @pl.when(at_home)
    def _():
        weights_out[1].start()

    pieces(group, 2 * group)
    arrived(3)

    @pl.when(x == 1)
    def _():
        arrived(WINDOW)

    pieces(2 * group, 4 * group)
    arrived(2)

    @pl.when(at_home)
    def _():
        for copy in weights_out[2:]:
            copy.start()

    pieces(4 * group, early)
    own_win.wait()
    for place in range(REACH):
        block = win.at[place, 1 - s]
        pltpu.make_async_copy(block, block, fr_recv.at[place]).wait()
    for copy in table_out:
        copy.wait_recv()
    for at, ref in enumerate(gain_refs):
        pltpu.make_async_copy(ref, gains.at[at], g_recv.at[at]).wait()

    def weight_wait(at):
        src, dst = weights[at]
        pltpu.make_async_copy(src, dst, w_recv.at[at]).wait()

    def first_wait(slot, at):
        @pl.when(slot == 0)
        def _():
            weight_wait(at)

    def entry(slot, column, core):
        local = slot_images[slot, column]
        return jnp.where(x == core, local, table[slot, column])

    def place_of(slot, column, core=None):
        core = s if core is None else core
        stored = image_slot[entry(slot, column, core)]
        ahead = lax.rem(stored - (2 * q + core) + devices, devices)
        return jnp.minimum(ahead, WINDOW - 1) + core

    def tokens_of(place):
        return jnp.concatenate([win[place, 0], win[place, 1]], axis=-1).astype(jnp.float32)

    stops = 5 * slots
    each = max((total_pieces * 26 // 32 - early) // stops, 0)
    fronted = early + each * stops

    def front(slot, carry):
        told = [0]

        def comm():
            base = early + (5 * slot + told[0]) * each
            told[0] += 1
            for at in range(each):
                piece(base + at)

        first_wait(slot, 0)
        tokens = tokens_of(place_of(slot, x))
        state = layer_norm(tokens, gains[0]).astype(jnp.bfloat16)
        triple[...] = matmul(state, m_qkv[...]).astype(jnp.bfloat16)
        comm()
        attend(triple, triple, triple, width, 2 * width, mixed, width, comm)
        first_wait(slot, 1)
        first = tokens + matmul(mixed[...], m_self_out[...])
        second[slot, 0:rows, :] = first
        comm()
        first_wait(slot, 2)
        first_wait(slot, 3)
        query_in = layer_norm(first, gains[1]).astype(jnp.bfloat16)
        memory = tokens_of(place_of(slot, 1 - x))
        memory_in = layer_norm(memory, gains[2]).astype(jnp.bfloat16)
        queries[...] = matmul(query_in, m_query[...]).astype(jnp.bfloat16)
        kv[...] = matmul(memory_in, m_memory[...]).astype(jnp.bfloat16)
        comm()
        attend(queries, kv, kv, 0, width, mixed, width, None)
        first_wait(slot, 4)
        result = second[slot, 0:rows, :] + matmul(mixed[...], m_cross_out[...])
        second[slot, 0:rows, :] = result
        hidden[slot, 0:rows, :] = layer_norm(result, gains[3]).astype(jnp.bfloat16)
        comm()
        return carry

    second[...] = jnp.zeros_like(second)
    hidden[...] = jnp.zeros_like(hidden)
    lax.fori_loop(0, slots, front, 0)

    def relayed(first, count):
        def body(at, carry):
            turn, which = first + lax.div(at, 2), lax.rem(at, 2)
            step, kind = lax.div(turn, split), 2 * lax.rem(turn, split) + which
            view = ring_view(step, kind, 1 - s)
            pltpu.make_async_copy(view, view, x_recv.at[step, kind]).wait()
            return carry

        lax.fori_loop(0, 2 * count, body, 0)

    def expand(first, turns, slot):
        count = 2 * turns
        if rank % 16 == 0:
            groups = [
                [ring_w[f, pl.ds(2 * first, count)].reshape(count * rank, width) for f in range(2)]
            ]
        else:
            groups = [[ring_w[f, 2 * first + at] for f in range(2)] for at in range(count)]
        total = second[slot]
        for fc1, fc2 in groups:
            pre = matmul_t(hidden[slot], fc1)
            act = (pre * (1.0 + lax.erf(pre * 0.5**0.5)) * 0.5).astype(jnp.bfloat16)
            total = total + matmul(act, fc2)
        second[slot] = total

    turns = split * chips
    span = turns // BLOCKS
    whole = total_pieces - group
    left = whole - fronted
    places = (BLOCKS - 1) * slots
    rate = -(-left // (2 * slots))

    def expand_early(turn, carry):
        block, slot = lax.div(turn, slots), lax.rem(turn, slots)

        @pl.when(slot == 0)
        def _():
            relayed(block * span, span)

        expand(block * span, span, slot)
        pieces(
            fronted + jnp.minimum(turn * rate, left), fronted + jnp.minimum((turn + 1) * rate, left)
        )
        return carry

    lax.fori_loop(0, places, expand_early, 0)
    relayed((BLOCKS - 1) * span, span - 1)

    def expand_late(slot, carry):
        expand((BLOCKS - 1) * span, span - 1, slot)
        pieces(
            whole + lax.div(slot * group, slots), whole + lax.div((slot + 1) * group, slots)
        )
        return carry

    lax.fori_loop(0, slots, expand_late, 0)
    weight_wait(5)
    weight_wait(6)
    relayed(turns - 1, 1)
    pix = half // 4

    def terms(slot, which, target):
        raw[...] = matmul(hidden[slot], m_head[which])
        conf = 1.0 + jnp.exp(raw[0:rows, 3 * pix :])
        for comp in range(4):
            at = slice(comp * pix, (comp + 1) * pix)
            value = conf if comp == 3 else conf * raw[0:rows, at]
            target[slot, :, at] = value.astype(target.dtype)

    def away(slot):
        return remote(
            term_away.at[slot], term_in.at[slot], a_send.at[slot], a_recv.at[slot], sibling
        )

    def expand_last(slot, carry):
        expand(turns - 1, 1, slot)
        hidden[slot] = layer_norm(second[slot], gains[4]).astype(jnp.bfloat16)
        terms(slot, 1 - s, term_away)
        away(slot).start()
        return carry

    def own_terms(slot, carry):
        terms(slot, s, term)
        return carry

    lax.fori_loop(0, slots, expand_last, 0)
    lax.fori_loop(0, slots, own_terms, 0)
    for slot in range(slots):
        away(slot).wait_recv()

    sources = []
    for core, ref in ((s, term), (1 - s, term_in)):
        live = jnp.where(x == core, slot_count[0], counts[0])
        for slot in range(slots):
            sources.append((place_of(slot, x, core), slot < live, ref, slot))

    quarter = half // 2

    def sums_of(place, part):
        sums = jnp.zeros((rows, quarter), jnp.float32)
        for to, live, ref, slot in sources:
            chosen = jnp.logical_and(to == place, live)
            value = ref[slot, :, part * quarter : (part + 1) * quarter].astype(jnp.float32)
            sums = sums + jnp.where(chosen, value, 0.0)
        return sums

    def far_copy(at, part, step, flip):
        return remote(
            far_out.at[at, part], far_in.at[at, part], b_send.at[at, part], b_recv.at[at, part],
            (pair_of(step, flip), s),
        )

    def far_send(at, part, step, flip, sums):
        far_out[at, part] = sums.astype(jnp.bfloat16)
        far_copy(at, part, step, flip).start()

    def far_wait(at, part):
        block = far_in.at[at, part]
        pltpu.make_async_copy(block, block, b_recv.at[at, part]).wait()
        return block[...].astype(jnp.float32)

    for part in range(2):
        far_send(1, part, 0, 1, sums_of(3 - x, part))
    for part in range(2):
        far_send(0, part, 2, 0, sums_of(WINDOW, part))

    @pl.when(x == 0)
    def _():
        for part in range(2):
            far_send(3, part, 0, 1, sums_of(1, part))

    for part in range(2):
        final[part] = sums_of(2 + x, part)
    for part in range(2):
        far_send(2, part, 1, 0, final[part] + far_wait(1, part))
    for part in range(2):
        final[part] = sums_of(x, part)

    @pl.when(x == 1)
    def _():
        for part in range(2):
            far_send(3, part, 0, 1, sums_of(0, part) + far_wait(0, part))

    @pl.when(x == 0)
    def _():
        for part in range(2):
            final[part] = final[part] + far_wait(0, part)

    for part in range(2):
        final[part] = final[part] + far_wait(2, part)
    for part in range(2):
        final[part] = final[part] + far_wait(3, part)
    conf = jnp.maximum(final[1, :, pix:], 1.0)
    for comp in range(3):
        value = final[comp // 2, :, comp % 2 * pix : (comp % 2 + 1) * pix]
        out[0, :, comp * pix : (comp + 1) * pix] = (value / conf).astype(jnp.bfloat16)

    for copy in (feature_across, near_one[0]):
        copy.wait_send()

    @pl.when(x == 0)
    def _():
        far_zero.wait_send()
        far_across.wait_send()

        @pl.when(even)
        def _():
            onto_next.wait_send()

    @pl.when(jnp.logical_or(x == 1, jnp.logical_not(even)))
    def _():
        near_zero[0].wait_send()

    for place in range(REACH):
        relay(place).wait_send()

    @pl.when(at_home)
    def _():
        for copy in fc_home + gains_out + weights_out:
            copy.wait_send()

    @pl.when(jnp.logical_not(at_home))
    def _():
        for copy in fc_out:
            copy.wait_send()

    for copy in table_out:
        copy.wait_send()

    def drain(number, carry):
        step, kind = lax.div(number, kinds), lax.rem(number, kinds)
        block = ring_view(step, kind, s)

        @pl.when(step < chips - 1)
        def _():
            remote(
                block, block, r_send.at[step, kind], r_recv.at[step, kind], onward
            ).wait_send()

        remote(block, block, x_send.at[step, kind], x_recv.at[step, kind], sibling).wait_send()
        return carry

    lax.fori_loop(0, total_pieces, drain, 0)
    for slot in range(slots):
        away(slot).wait_send()
    for at, (step, flip) in enumerate(((2, 0), (0, 1), (1, 0), (0, 1))):
        for part in range(2):
            far_copy(at, part, step, flip).wait_send()


def on_device(
    features, image_slot, slot_images, slot_count, gain_self, gain_query, gain_memory, gain_mlp,
    gain_head, w_qkv, w_self_out, w_query, w_memory, w_cross_out, w_fc1, w_fc2, w_head,
):
    devices = lax.axis_size("pairs")
    chips = devices // 2
    blocks, rows, part = features.shape
    if blocks != 1 or chips % BLOCKS:
        raise ValueError("unsupported split")
    width = w_qkv.shape[1]
    slots = slot_images.shape[0]
    tall = padded(rows)
    shard = w_fc1.shape[1]
    split = 2 if shard % 32 == 0 else 1
    kinds = 2 * split
    half = w_head.shape[2] // 2
    bf16, f32 = jnp.bfloat16, jnp.float32
    dma = pltpu.SemaphoreType.DMA
    anywhere = pl.BlockSpec(memory_space=pl.ANY)
    return pl.pallas_call(
        decoder_kernel,
        out_shape=jax.ShapeDtypeStruct((1, rows, half * 3 // 4), bf16),
        in_specs=[pl.BlockSpec(memory_space=pltpu.SMEM)] * 3 + [anywhere] * 14,
        out_specs=pl.BlockSpec(memory_space=pltpu.VMEM),
        scratch_shapes=[
            pltpu.VMEM((REACH, 2, rows, part), bf16),
            pltpu.SMEM(slot_images.shape, jnp.int32),
            pltpu.SMEM(slot_count.shape, jnp.int32),
            pltpu.VMEM((5, 1, width), f32),
            pltpu.VMEM(w_qkv.shape[1:], bf16),
            pltpu.VMEM(w_self_out.shape[1:], bf16),
            pltpu.VMEM(w_query.shape[1:], bf16),
            pltpu.VMEM(w_memory.shape[1:], bf16),
            pltpu.VMEM(w_cross_out.shape[1:], bf16),
            pltpu.VMEM((2, width, half), bf16),
            pltpu.VMEM((2, devices * split, shard // split, width), bf16),
            pltpu.VMEM((rows, 3 * width), bf16),
            pltpu.VMEM((rows, 2 * width), bf16),
            pltpu.VMEM((rows, width), bf16),
            pltpu.VMEM((rows, width), bf16),
            pltpu.VMEM((slots, tall, width), f32),
            pltpu.VMEM((slots, tall, width), bf16),
            pltpu.VMEM((tall, half), f32),
            pltpu.VMEM((slots, rows, half), f32),
            pltpu.VMEM((slots, rows, half), bf16),
            pltpu.VMEM((slots, rows, half), bf16),
            pltpu.VMEM((4, 2, rows, half // 2), bf16),
            pltpu.VMEM((4, 2, rows, half // 2), bf16),
            pltpu.VMEM((2, rows, half // 2), f32),
            dma, dma((6,)), dma((REACH,)), dma((REACH,)), dma((REACH,)),
            dma((2,)), dma((2,)), dma((5,)), dma((5,)), dma((7,)), dma((7,)),
            dma((kinds,)), dma((chips, kinds)), dma((chips, kinds)), dma((chips, kinds)),
            dma((chips, kinds)), dma((slots,)), dma((slots,)), dma((4, 2)), dma((4, 2)),
        ],
        compiler_params=pltpu.CompilerParams(
            collective_id=0, has_side_effects=True, vmem_limit_bytes=VMEM_LIMIT
        ),
    )(
        image_slot, slot_images, slot_count, features, gain_self, gain_query, gain_memory,
        gain_mlp, gain_head, w_qkv, w_self_out, w_query, w_memory, w_cross_out, w_fc1, w_fc2,
        w_head,
    )


def solution(mesh):
    placed = (
        P("pairs", None, "side"),
        P(),
        P("pairs", None),
        P("pairs"),
        P("side", None),
        P("side", None),
        P("side", None),
        P("side", None),
        P("side", None),
        P("side", None, None),
        P("side", None, None),
        P("side", None, None),
        P("side", None, None),
        P("side", None, None),
        P("side", "pairs", None),
        P("side", "pairs", None),
        P("side", None, None),
    )
    return jax.shard_map(
        on_device, mesh=mesh, in_specs=placed, out_specs=P("pairs", None, "side"), check_vma=False
    )
```

```python
import functools

import jax
import jax.numpy as jnp
from jax import lax
from jax.experimental import pallas as pl
from jax.experimental.pallas import tpu as pltpu
from jax.sharding import PartitionSpec as P

HEAD_DIM = 64
WINDOW = 4
PAIR = 2 * HEAD_DIM
BLOCKS = 4
REACH = WINDOW + 1
VMEM_LIMIT = 63 * 1024 * 1024
MESH = pl.DeviceIdType.MESH


def padded(rows):
    return -(-rows // 16) * 16


def layer_norm(values, gain):
    center = values - jnp.mean(values, axis=-1, keepdims=True)
    spread = jnp.mean(center * center, axis=-1, keepdims=True)
    return center * lax.rsqrt(spread + 1e-06) * gain


def matmul(left, right):
    return jnp.dot(left, right, preferred_element_type=jnp.float32)


def matmul_t(left, right):
    return lax.dot_general(
        left, right, (((1,), (1,)), ((), ())), preferred_element_type=jnp.float32
    )


def attend(q_ref, k_ref, v_ref, k_at, v_at, o_ref, width, comm):
    rows = q_ref.shape[0]
    low = lax.broadcasted_iota(jnp.int32, (rows, PAIR), 1) < HEAD_DIM
    for pair in range(width // PAIR):
        if comm is not None and pair * PAIR == width // 2:
            comm()
        q = q_ref[:, pair * PAIR : (pair + 1) * PAIR]
        k = k_ref[:, k_at + pair * PAIR : k_at + (pair + 1) * PAIR]
        v = v_ref[:, v_at + pair * PAIR : v_at + (pair + 1) * PAIR]
        mixed = None
        for keep in (low, jnp.logical_not(low)):
            q_head = jnp.where(keep, q, jnp.zeros_like(q))
            v_head = jnp.where(keep, v, jnp.zeros_like(v))
            scores = matmul_t(q_head, k) * HEAD_DIM ** (-0.5)
            expon = jnp.exp(scores)
            weights = (expon / jnp.sum(expon, axis=-1, keepdims=True)).astype(jnp.bfloat16)
            part = matmul(weights, v_head)
            mixed = part if mixed is None else mixed + part
        o_ref[:, pair * PAIR : (pair + 1) * PAIR] = mixed.astype(jnp.bfloat16)


def remote(src, dst, send, recv, device):
    return pltpu.make_async_remote_copy(
        src_ref=src, dst_ref=dst, send_sem=send, recv_sem=recv, device_id=device,
        device_id_type=MESH,
    )


def decoder_kernel(
    image_slot, slot_images, slot_count, features,
    g_self, g_query, g_memory, g_mlp, g_head,
    w_qkv, w_self_out, w_query, w_memory, w_cross_out, w_fc1, w_fc2, w_head,
    out,
    win, table, counts, gains, m_qkv, m_self_out, m_query, m_memory, m_cross_out, m_head, ring_w,
    triple, kv, queries, mixed, second, hidden, raw, term, term_away, term_in, far_out, far_in,
    final,
    f_local, f_send, f_recv, fr_send, fr_recv, t_send, t_recv, g_send, g_recv, w_send, w_recv,
    s_send, r_send, r_recv, x_send, x_recv, a_send, a_recv, b_send, b_recv,
):
    devices = lax.axis_size("pairs")
    chips = devices // 2
    here = lax.axis_index("pairs")
    s = lax.axis_index("side")
    x = lax.rem(here, 2)
    q = lax.div(here, 2)
    rows = features.shape[1]
    width = m_qkv.shape[0]
    slots = second.shape[0]
    tall = second.shape[1]
    shard = w_fc1.shape[1]
    rank = ring_w.shape[2]
    split = shard // rank
    kinds = 2 * split
    total_pieces = kinds * chips

    sibling = (here, 1 - s)
    partner = (2 * q + s, x)
    at_home = x == s

    def pair_of(step, flip):
        chip = lax.rem(q + (step + chips), chips)
        return 2 * chip + (1 - x if flip else x)

    up = jnp.where(
        lax.rem(q, 2) == 0,
        jnp.where(q + 2 < chips, q + 2, chips - 1),
        jnp.where(q >= 3, q - 2, 0),
    )
    down = jnp.where(
        lax.rem(q, 2) == 0,
        jnp.where(q == 0, 1, q - 2),
        jnp.where(q + 2 < chips, q + 2, chips - 2),
    )
    onward = (2 * jnp.where(s == 0, up, down) + x, s)

    mats = (
        (w_qkv, m_qkv), (w_self_out, m_self_out), (w_memory, m_memory), (w_query, m_query),
        (w_cross_out, m_cross_out),
    )
    half = w_head.shape[2] // 2
    weights = [(src.at[0], dst) for src, dst in mats]
    weights += [(w_head.at[0, :, h * half : (h + 1) * half], m_head.at[h]) for h in range(2)]
    gain_refs = (g_self, g_query, g_memory, g_mlp, g_head)
    fcs = (w_fc1, w_fc2)

    def ring_view(step, kind, ring):
        return ring_w.at[lax.rem(kind, 2), 2 * (split * step + lax.div(kind, 2)) + ring]

    def own_fc(which, piece):
        if split == 1:
            return fcs[which].at[0]
        return fcs[which].at[0, pl.ds(pl.multiple_of(piece * rank, rank), rank)]

    own_win = pltpu.make_async_copy(features.at[0], win.at[x, s], f_local)
    own_win.start()

    @pl.when(at_home)
    def _():
        for at, ref in enumerate(gain_refs):
            pltpu.make_async_copy(ref, gains.at[at], g_recv.at[at]).start()
        for which in range(2):
            pltpu.make_async_copy(
                own_fc(which, s), ring_view(0, which, s), r_recv.at[0, which]
            ).start()
        for at, (src, dst) in enumerate(weights):
            pltpu.make_async_copy(src, dst, w_recv.at[at]).start()

    barrier = pltpu.get_barrier_semaphore()
    for step in range(-2, 3):
        for flip in range(2):
            if step or flip:
                pl.semaphore_signal(
                    barrier, inc=1, device_id=(pair_of(step, flip), s), device_id_type=MESH
                )
    pl.semaphore_signal(barrier, inc=1, device_id=sibling, device_id_type=MESH)

    @pl.when(jnp.logical_not(at_home))
    def _():
        pl.semaphore_signal(barrier, inc=1, device_id=partner, device_id_type=MESH)

    pl.semaphore_wait(barrier, 10 + (1 - at_home.astype(jnp.int32)))

    table_out = [
        remote(slot_images, table, t_send.at[0], t_recv.at[0], (pair_of(0, 1), s)),
        remote(slot_count, counts, t_send.at[1], t_recv.at[1], (pair_of(0, 1), s)),
    ]
    across = (2 * q + s, s)
    if split == 1:
        fc_home = []
        fc_out = [
            remote(own_fc(f, 0), ring_view(0, f, x), s_send.at[f], r_recv.at[0, f], partner)
            for f in range(2)
        ]
    else:
        fc_home = [
            remote(
                own_fc(f, 1 - s), ring_view(0, f, 1 - s), s_send.at[f], r_recv.at[0, f], sibling
            )
            for f in range(2)
        ]
        fc_out = [
            remote(
                own_fc(f, ring), ring_view(0, 2 + f, ring), s_send.at[2 * f + to],
                r_recv.at[0, 2 + f], device,
            )
            for f in range(2)
            for to, (ring, device) in enumerate(((x, partner), (s, across)))
        ]
    gains_out = [
        remote(ref, gains.at[at], g_send.at[at], g_recv.at[at], sibling)
        for at, ref in enumerate(gain_refs)
    ]
    weights_out = [
        remote(src, dst, w_send.at[at], w_recv.at[at], sibling)
        for at, (src, dst) in enumerate(weights)
    ]

    def feature_out(block, place, step, flip, at):
        return remote(
            block, win.at[place, s], f_send.at[at], f_recv.at[place], (pair_of(-step, flip), s)
        )

    own = features.at[0]
    passed = win.at[1 - x, s]
    even = lax.rem(q, 2) == 0
    feature_across = feature_out(own, x, 0, 1, 0)
    near_zero = [feature_out(block, 2, 1, 0, 1) for block in (own, passed)]
    near_one = [feature_out(block, 3, 1, 0, 2) for block in (passed, own)]
    far_zero = feature_out(own, WINDOW, 2, 0, 3)
    onto_next = feature_out(win.at[WINDOW, s], 2, -1, 0, 4)
    far_across = feature_out(win.at[WINDOW, s], WINDOW, 0, 1, 5)

    def relay(place, block=None):
        target = win.at[place, s]
        return remote(
            target if block is None else block, target, fr_send.at[place], fr_recv.at[place],
            sibling,
        )

    for copy in table_out:
        copy.start()
    feature_across.start()

    @pl.when(x == 0)
    def _():
        far_zero.start()

        @pl.when(jnp.logical_not(even))
        def _():
            near_zero[0].start()

    @pl.when(x == 1)
    def _():
        near_one[1].start()

    relay(x, own).start()

    @pl.when(at_home)
    def _():
        for copy in fc_home + gains_out:
            copy.start()
        weights_out[0].start()

    swapped = len(fc_out) // 2

    @pl.when(jnp.logical_not(at_home))
    def _():
        for copy in fc_out[:swapped]:
            copy.start()

        @pl.when(x == 1)
        def _():
            for copy in fc_out[swapped:]:
                copy.start()

    def piece(number):
        turn = lax.div(number, kinds // 2)
        last = turn == 2 * chips - 1
        ahead = jnp.logical_or(turn == 0, jnp.logical_and(lax.rem(turn, 2) == 1, turn < 2 * chips - 1))
        step = jnp.where(
            turn == 0,
            0,
            jnp.where(last, chips - 1, jnp.where(ahead, lax.div(turn + 1, 2), lax.div(turn, 2) - 1)),
        )
        kind = lax.rem(number, kinds // 2) + jnp.where(ahead, 0, kinds // 2)
        block = ring_view(step, kind, s)
        pltpu.make_async_copy(block, block, r_recv.at[step, kind]).wait()

        @pl.when(step < chips - 1)
        def _():
            remote(
                block, ring_view(step + 1, kind, s), r_send.at[step, kind],
                r_recv.at[step + 1, kind], onward,
            ).start()

        remote(block, block, x_send.at[step, kind], x_recv.at[step, kind], sibling).start()

    def pieces(low, high):
        def body(number, carry):
            piece(number)
            return carry

        lax.fori_loop(low, high, body, 0)

    def arrived(place):
        block = win.at[place, s]
        pltpu.make_async_copy(block, block, f_recv.at[place]).wait()
        relay(place).start()

    group = kinds // 2
    early = 5 * group
    pieces(0, group)
    arrived(1 - x)

    @pl.when(x == 0)
    def _():
        near_one[0].start()
        arrived(WINDOW)

        @pl.when(even)
        def _():
            onto_next.start()

        far_across.start()

        @pl.when(jnp.logical_not(at_home))
        def _():
            for copy in fc_out[swapped:]:
                copy.start()

    @pl.when(x == 1)
    def _():
        near_zero[1].start()

    @pl.when(at_home)
    def _():
        weights_out[1].start()

    pieces(group, 2 * group)
    arrived(3)

    @pl.when(x == 1)
    def _():
        arrived(WINDOW)

    pieces(2 * group, 4 * group)
    arrived(2)

    @pl.when(at_home)
    def _():
        for copy in weights_out[2:]:
            copy.start()

    pieces(4 * group, early)
    own_win.wait()
    for place in range(REACH):
        block = win.at[place, 1 - s]
        pltpu.make_async_copy(block, block, fr_recv.at[place]).wait()
    for copy in table_out:
        copy.wait_recv()
    for at, ref in enumerate(gain_refs):
        pltpu.make_async_copy(ref, gains.at[at], g_recv.at[at]).wait()

    def weight_wait(at):
        src, dst = weights[at]
        pltpu.make_async_copy(src, dst, w_recv.at[at]).wait()

    def first_wait(slot, at):
        @pl.when(slot == 0)
        def _():
            weight_wait(at)

    def entry(slot, column, core):
        local = slot_images[column, slot]
        return jnp.where(x == core, local, table[column, slot])

    def place_of(slot, column, core=None):
        core = s if core is None else core
        stored = image_slot[entry(slot, column, core)]
        ahead = lax.rem(stored - (2 * q + core) + devices, devices)
        return jnp.minimum(ahead, WINDOW - 1) + core

    def tokens_of(place):
        return jnp.concatenate([win[place, 0], win[place, 1]], axis=-1).astype(jnp.float32)

    stops = 5 * slots
    each = max((total_pieces * 26 // 32 - early) // stops, 0)
    fronted = early + each * stops

    def front(slot, carry):
        told = [0]

        def comm():
            base = early + (5 * slot + told[0]) * each
            told[0] += 1
            for at in range(each):
                piece(base + at)

        first_wait(slot, 0)
        tokens = tokens_of(place_of(slot, x))
        state = layer_norm(tokens, gains[0]).astype(jnp.bfloat16)
        triple[...] = matmul(state, m_qkv[...]).astype(jnp.bfloat16)
        comm()
        attend(triple, triple, triple, width, 2 * width, mixed, width, comm)
        first_wait(slot, 1)
        first = tokens + matmul(mixed[...], m_self_out[...])
        second[slot, 0:rows, :] = first
        comm()
        first_wait(slot, 2)
        first_wait(slot, 3)
        query_in = layer_norm(first, gains[1]).astype(jnp.bfloat16)
        memory = tokens_of(place_of(slot, 1 - x))
        memory_in = layer_norm(memory, gains[2]).astype(jnp.bfloat16)
        queries[...] = matmul(query_in, m_query[...]).astype(jnp.bfloat16)
        kv[...] = matmul(memory_in, m_memory[...]).astype(jnp.bfloat16)
        comm()
        attend(queries, kv, kv, 0, width, mixed, width, None)
        first_wait(slot, 4)
        result = second[slot, 0:rows, :] + matmul(mixed[...], m_cross_out[...])
        second[slot, 0:rows, :] = result
        hidden[slot, 0:rows, :] = layer_norm(result, gains[3]).astype(jnp.bfloat16)
        comm()
        return carry

    second[...] = jnp.zeros_like(second)
    hidden[...] = jnp.zeros_like(hidden)
    lax.fori_loop(0, slots, front, 0)

    def relayed(first, count):
        def body(at, carry):
            turn, which = first + lax.div(at, 2), lax.rem(at, 2)
            step, kind = lax.div(turn, split), 2 * lax.rem(turn, split) + which
            view = ring_view(step, kind, 1 - s)
            pltpu.make_async_copy(view, view, x_recv.at[step, kind]).wait()
            return carry

        lax.fori_loop(0, 2 * count, body, 0)

    def expand(first, turns, slot):
        count = 2 * turns
        if rank % 16 == 0:
            groups = [
                [ring_w[f, pl.ds(2 * first, count)].reshape(count * rank, width) for f in range(2)]
            ]
        else:
            groups = [[ring_w[f, 2 * first + at] for f in range(2)] for at in range(count)]
        total = second[slot]
        for fc1, fc2 in groups:
            pre = matmul_t(hidden[slot], fc1)
            act = (pre * (1.0 + lax.erf(pre * 0.5**0.5)) * 0.5).astype(jnp.bfloat16)
            total = total + matmul(act, fc2)
        second[slot] = total

    turns = split * chips
    span = turns // BLOCKS
    whole = total_pieces - group
    left = whole - fronted
    places = (BLOCKS - 1) * slots
    rate = -(-left // (2 * slots))

    def expand_early(turn, carry):
        block, slot = lax.div(turn, slots), lax.rem(turn, slots)

        @pl.when(slot == 0)
        def _():
            relayed(block * span, span)

        expand(block * span, span, slot)
        pieces(
            fronted + jnp.minimum(turn * rate, left), fronted + jnp.minimum((turn + 1) * rate, left)
        )
        return carry

    lax.fori_loop(0, places, expand_early, 0)
    relayed((BLOCKS - 1) * span, span - 1)

    def expand_late(slot, carry):
        expand((BLOCKS - 1) * span, span - 1, slot)
        pieces(
            whole + lax.div(slot * group, slots), whole + lax.div((slot + 1) * group, slots)
        )
        return carry

    lax.fori_loop(0, slots, expand_late, 0)
    weight_wait(5)
    weight_wait(6)
    relayed(turns - 1, 1)
    pix = half // 4

    def terms(slot, which, target):
        raw[...] = matmul(hidden[slot], m_head[which])
        conf = 1.0 + jnp.exp(raw[0:rows, 3 * pix :])
        for comp in range(4):
            at = slice(comp * pix, (comp + 1) * pix)
            value = conf if comp == 3 else conf * raw[0:rows, at]
            target[slot, :, at] = value.astype(target.dtype)

    def away(slot):
        return remote(
            term_away.at[slot], term_in.at[slot], a_send.at[slot], a_recv.at[slot], sibling
        )

    def expand_last(slot, carry):
        expand(turns - 1, 1, slot)
        hidden[slot] = layer_norm(second[slot], gains[4]).astype(jnp.bfloat16)
        terms(slot, 1 - s, term_away)
        away(slot).start()
        return carry

    def own_terms(slot, carry):
        terms(slot, s, term)
        return carry

    lax.fori_loop(0, slots, expand_last, 0)
    lax.fori_loop(0, slots, own_terms, 0)
    for slot in range(slots):
        away(slot).wait_recv()

    sources = []
    for core, ref in ((s, term), (1 - s, term_in)):
        live = jnp.where(x == core, slot_count[0], counts[0])
        for slot in range(slots):
            sources.append((place_of(slot, x, core), slot < live, ref, slot))

    quarter = half // 2

    def sums_of(place, part):
        sums = jnp.zeros((rows, quarter), jnp.float32)
        for to, live, ref, slot in sources:
            chosen = jnp.logical_and(to == place, live)
            value = ref[slot, :, part * quarter : (part + 1) * quarter].astype(jnp.float32)
            sums = sums + jnp.where(chosen, value, 0.0)
        return sums

    def far_copy(at, part, step, flip):
        return remote(
            far_out.at[at, part], far_in.at[at, part], b_send.at[at, part], b_recv.at[at, part],
            (pair_of(step, flip), s),
        )

    def far_send(at, part, step, flip, sums):
        far_out[at, part] = sums.astype(jnp.bfloat16)
        far_copy(at, part, step, flip).start()

    def far_wait(at, part):
        block = far_in.at[at, part]
        pltpu.make_async_copy(block, block, b_recv.at[at, part]).wait()
        return block[...].astype(jnp.float32)

    for part in range(2):
        far_send(1, part, 0, 1, sums_of(3 - x, part))
    for part in range(2):
        far_send(0, part, 2, 0, sums_of(WINDOW, part))

    @pl.when(x == 0)
    def _():
        for part in range(2):
            far_send(3, part, 0, 1, sums_of(1, part))

    for part in range(2):
        final[part] = sums_of(2 + x, part)
    for part in range(2):
        far_send(2, part, 1, 0, final[part] + far_wait(1, part))
    for part in range(2):
        final[part] = sums_of(x, part)

    @pl.when(x == 1)
    def _():
        for part in range(2):
            far_send(3, part, 0, 1, sums_of(0, part) + far_wait(0, part))

    @pl.when(x == 0)
    def _():
        for part in range(2):
            final[part] = final[part] + far_wait(0, part)

    for part in range(2):
        final[part] = final[part] + far_wait(2, part)
    for part in range(2):
        final[part] = final[part] + far_wait(3, part)
    conf = jnp.maximum(final[1, :, pix:], 1.0)
    for comp in range(3):
        value = final[comp // 2, :, comp % 2 * pix : (comp % 2 + 1) * pix]
        out[0, :, comp * pix : (comp + 1) * pix] = (value / conf).astype(jnp.bfloat16)

    for copy in (feature_across, near_one[0]):
        copy.wait_send()

    @pl.when(x == 0)
    def _():
        far_zero.wait_send()
        far_across.wait_send()

        @pl.when(even)
        def _():
            onto_next.wait_send()

    @pl.when(jnp.logical_or(x == 1, jnp.logical_not(even)))
    def _():
        near_zero[0].wait_send()

    for place in range(REACH):
        relay(place).wait_send()

    @pl.when(at_home)
    def _():
        for copy in fc_home + gains_out + weights_out:
            copy.wait_send()

    @pl.when(jnp.logical_not(at_home))
    def _():
        for copy in fc_out:
            copy.wait_send()

    for copy in table_out:
        copy.wait_send()

    def drain(number, carry):
        step, kind = lax.div(number, kinds), lax.rem(number, kinds)
        block = ring_view(step, kind, s)

        @pl.when(step < chips - 1)
        def _():
            remote(
                block, block, r_send.at[step, kind], r_recv.at[step, kind], onward
            ).wait_send()

        remote(block, block, x_send.at[step, kind], x_recv.at[step, kind], sibling).wait_send()
        return carry

    lax.fori_loop(0, total_pieces, drain, 0)
    for slot in range(slots):
        away(slot).wait_send()
    for at, (step, flip) in enumerate(((2, 0), (0, 1), (1, 0), (0, 1))):
        for part in range(2):
            far_copy(at, part, step, flip).wait_send()


def on_device(
    features, image_slot, slot_images, slot_count, gain_self, gain_query, gain_memory, gain_mlp,
    gain_head, w_qkv, w_self_out, w_query, w_memory, w_cross_out, w_fc1, w_fc2, w_head,
):
    devices = lax.axis_size("pairs")
    chips = devices // 2
    blocks, rows, part = features.shape
    if blocks != 1 or chips % BLOCKS:
        raise ValueError("unsupported split")
    width = w_qkv.shape[1]
    slots = slot_images.shape[0]
    tall = padded(rows)
    shard = w_fc1.shape[1]
    split = 2 if shard % 32 == 0 else 1
    kinds = 2 * split
    half = w_head.shape[2] // 2
    bf16, f32 = jnp.bfloat16, jnp.float32
    dma = pltpu.SemaphoreType.DMA
    anywhere = pl.BlockSpec(memory_space=pl.ANY)
    return pl.pallas_call(
        decoder_kernel,
        out_shape=pltpu.VMEM((1, rows, half * 3 // 4), bf16),
        in_specs=[pl.BlockSpec(memory_space=pltpu.SMEM)] * 3 + [anywhere] * 14,
        out_specs=pl.BlockSpec(memory_space=pltpu.VMEM),
        scratch_shapes=[
            pltpu.VMEM((REACH, 2, rows, part), bf16),
            pltpu.SMEM(slot_images.shape[::-1], jnp.int32),
            pltpu.SMEM(slot_count.shape, jnp.int32),
            pltpu.VMEM((5, 1, width), f32),
            pltpu.VMEM(w_qkv.shape[1:], bf16),
            pltpu.VMEM(w_self_out.shape[1:], bf16),
            pltpu.VMEM(w_query.shape[1:], bf16),
            pltpu.VMEM(w_memory.shape[1:], bf16),
            pltpu.VMEM(w_cross_out.shape[1:], bf16),
            pltpu.VMEM((2, width, half), bf16),
            pltpu.VMEM((2, devices * split, shard // split, width), bf16),
            pltpu.VMEM((rows, 3 * width), bf16),
            pltpu.VMEM((rows, 2 * width), bf16),
            pltpu.VMEM((rows, width), bf16),
            pltpu.VMEM((rows, width), bf16),
            pltpu.VMEM((slots, tall, width), f32),
            pltpu.VMEM((slots, tall, width), bf16),
            pltpu.VMEM((tall, half), f32),
            pltpu.VMEM((slots, rows, half), f32),
            pltpu.VMEM((slots, rows, half), bf16),
            pltpu.VMEM((slots, rows, half), bf16),
            pltpu.VMEM((4, 2, rows, half // 2), bf16),
            pltpu.VMEM((4, 2, rows, half // 2), bf16),
            pltpu.VMEM((2, rows, half // 2), f32),
            dma, dma((6,)), dma((REACH,)), dma((REACH,)), dma((REACH,)),
            dma((2,)), dma((2,)), dma((5,)), dma((5,)), dma((7,)), dma((7,)),
            dma((kinds,)), dma((chips, kinds)), dma((chips, kinds)), dma((chips, kinds)),
            dma((chips, kinds)), dma((slots,)), dma((slots,)), dma((4, 2)), dma((4, 2)),
        ],
        compiler_params=pltpu.CompilerParams(
            collective_id=0, has_side_effects=True, vmem_limit_bytes=VMEM_LIMIT
        ),
    )(
        image_slot, slot_images.T, slot_count, features, gain_self, gain_query, gain_memory,
        gain_mlp, gain_head, w_qkv, w_self_out, w_query, w_memory, w_cross_out, w_fc1, w_fc2,
        w_head,
    )


def solution(mesh):
    placed = (
        P("pairs", None, "side"),
        P(),
        P("pairs", None),
        P("pairs"),
        P("side", None),
        P("side", None),
        P("side", None),
        P("side", None),
        P("side", None),
        P("side", None, None),
        P("side", None, None),
        P("side", None, None),
        P("side", None, None),
        P("side", None, None),
        P("side", "pairs", None),
        P("side", "pairs", None),
        P("side", None, None),
    )
    return jax.shard_map(
        on_device, mesh=mesh, in_specs=placed, out_specs=P("pairs", None, "side"), check_vma=False
    )
```

```python
import functools

import jax
import jax.numpy as jnp
from jax import lax
from jax.experimental import pallas as pl
from jax.experimental.pallas import tpu as pltpu
from jax.sharding import PartitionSpec as P

HEAD_DIM = 64
WINDOW = 4
PAIR = 2 * HEAD_DIM
BLOCKS = 4
REACH = WINDOW + 1
VMEM_LIMIT = 63 * 1024 * 1024
MESH = pl.DeviceIdType.MESH


def padded(rows):
    return -(-rows // 16) * 16


def layer_norm(values, gain):
    center = values - jnp.mean(values, axis=-1, keepdims=True)
    spread = jnp.mean(center * center, axis=-1, keepdims=True)
    return center * lax.rsqrt(spread + 1e-06) * gain


def matmul(left, right):
    return jnp.dot(left, right, preferred_element_type=jnp.float32)


def matmul_t(left, right):
    return lax.dot_general(
        left, right, (((1,), (1,)), ((), ())), preferred_element_type=jnp.float32
    )


def attend(q_ref, k_ref, v_ref, k_at, v_at, o_ref, width, comm):
    rows = q_ref.shape[0]
    low = lax.broadcasted_iota(jnp.int32, (rows, PAIR), 1) < HEAD_DIM
    for pair in range(width // PAIR):
        if comm is not None and pair * PAIR == width // 2:
            comm()
        q = q_ref[:, pair * PAIR : (pair + 1) * PAIR]
        k = k_ref[:, k_at + pair * PAIR : k_at + (pair + 1) * PAIR]
        v = v_ref[:, v_at + pair * PAIR : v_at + (pair + 1) * PAIR]
        mixed = None
        for keep in (low, jnp.logical_not(low)):
            q_head = jnp.where(keep, q, jnp.zeros_like(q))
            v_head = jnp.where(keep, v, jnp.zeros_like(v))
            scores = matmul_t(q_head, k) * HEAD_DIM ** (-0.5)
            expon = jnp.exp(scores)
            weights = (expon / jnp.sum(expon, axis=-1, keepdims=True)).astype(jnp.bfloat16)
            part = matmul(weights, v_head)
            mixed = part if mixed is None else mixed + part
        o_ref[:, pair * PAIR : (pair + 1) * PAIR] = mixed.astype(jnp.bfloat16)


def remote(src, dst, send, recv, device):
    return pltpu.make_async_remote_copy(
        src_ref=src, dst_ref=dst, send_sem=send, recv_sem=recv, device_id=device,
        device_id_type=MESH,
    )


def decoder_kernel(
    image_slot, slot_images, slot_count, features,
    g_self, g_query, g_memory, g_mlp, g_head,
    w_qkv, w_self_out, w_query, w_memory, w_cross_out, w_fc1, w_fc2, w_head,
    out,
    win, table, counts, gains, m_qkv, m_self_out, m_query, m_memory, m_cross_out, m_head, ring_w,
    triple, kv, queries, mixed, second, hidden, raw, term, term_away, term_in, far_out, far_in,
    final,
    f_local, f_send, f_recv, fr_send, fr_recv, t_send, t_recv, g_send, g_recv, w_send, w_recv,
    s_send, r_send, r_recv, x_send, x_recv, a_send, a_recv, b_send, b_recv,
):
    devices = lax.axis_size("pairs")
    chips = devices // 2
    here = lax.axis_index("pairs")
    s = lax.axis_index("side")
    x = lax.rem(here, 2)
    q = lax.div(here, 2)
    rows = features.shape[1]
    width = m_qkv.shape[0]
    slots = second.shape[0]
    tall = second.shape[1]
    shard = w_fc1.shape[1]
    rank = ring_w.shape[2]
    split = shard // rank
    kinds = 2 * split
    total_pieces = kinds * chips

    sibling = (here, 1 - s)
    partner = (2 * q + s, x)
    at_home = x == s

    def pair_of(step, flip):
        chip = lax.rem(q + (step + chips), chips)
        return 2 * chip + (1 - x if flip else x)

    up = jnp.where(
        lax.rem(q, 2) == 0,
        jnp.where(q + 2 < chips, q + 2, chips - 1),
        jnp.where(q >= 3, q - 2, 0),
    )
    down = jnp.where(
        lax.rem(q, 2) == 0,
        jnp.where(q == 0, 1, q - 2),
        jnp.where(q + 2 < chips, q + 2, chips - 2),
    )
    onward = (2 * jnp.where(s == 0, up, down) + x, s)

    mats = (
        (w_qkv, m_qkv), (w_self_out, m_self_out), (w_memory, m_memory), (w_query, m_query),
        (w_cross_out, m_cross_out),
    )
    half = w_head.shape[2] // 2
    weights = [(src.at[0], dst) for src, dst in mats]
    weights += [(w_head.at[0, :, h * half : (h + 1) * half], m_head.at[h]) for h in range(2)]
    gain_refs = (g_self, g_query, g_memory, g_mlp, g_head)
    fcs = (w_fc1, w_fc2)

    def ring_view(step, kind, ring):
        return ring_w.at[lax.rem(kind, 2), 2 * (split * step + lax.div(kind, 2)) + ring]

    def own_fc(which, piece):
        if split == 1:
            return fcs[which].at[0]
        return fcs[which].at[0, pl.ds(pl.multiple_of(piece * rank, rank), rank)]

    own_win = pltpu.make_async_copy(features.at[0], win.at[x, s], f_local)
    own_win.start()

    @pl.when(at_home)
    def _():
        for at, ref in enumerate(gain_refs):
            pltpu.make_async_copy(ref, gains.at[at], g_recv.at[at]).start()
        for which in range(2):
            pltpu.make_async_copy(
                own_fc(which, s), ring_view(0, which, s), r_recv.at[0, which]
            ).start()
        for at, (src, dst) in enumerate(weights):
            pltpu.make_async_copy(src, dst, w_recv.at[at]).start()

    barrier = pltpu.get_barrier_semaphore()
    for step in range(-2, 3):
        for flip in range(2):
            if step or flip:
                pl.semaphore_signal(
                    barrier, inc=1, device_id=(pair_of(step, flip), s), device_id_type=MESH
                )
    pl.semaphore_signal(barrier, inc=1, device_id=sibling, device_id_type=MESH)

    @pl.when(jnp.logical_not(at_home))
    def _():
        pl.semaphore_signal(barrier, inc=1, device_id=partner, device_id_type=MESH)

    pl.semaphore_wait(barrier, 10 + (1 - at_home.astype(jnp.int32)))

    table_out = [
        remote(slot_images, table, t_send.at[0], t_recv.at[0], (pair_of(0, 1), s)),
        remote(slot_count, counts, t_send.at[1], t_recv.at[1], (pair_of(0, 1), s)),
    ]
    across = (2 * q + s, s)
    if split == 1:
        fc_home = []
        fc_out = [
            remote(own_fc(f, 0), ring_view(0, f, x), s_send.at[f], r_recv.at[0, f], partner)
            for f in range(2)
        ]
    else:
        fc_home = [
            remote(
                own_fc(f, 1 - s), ring_view(0, f, 1 - s), s_send.at[f], r_recv.at[0, f], sibling
            )
            for f in range(2)
        ]
        fc_out = [
            remote(
                own_fc(f, ring), ring_view(0, 2 + f, ring), s_send.at[2 * f + to],
                r_recv.at[0, 2 + f], device,
            )
            for f in range(2)
            for to, (ring, device) in enumerate(((x, partner), (s, across)))
        ]
    gains_out = [
        remote(ref, gains.at[at], g_send.at[at], g_recv.at[at], sibling)
        for at, ref in enumerate(gain_refs)
    ]
    weights_out = [
        remote(src, dst, w_send.at[at], w_recv.at[at], sibling)
        for at, (src, dst) in enumerate(weights)
    ]

    def feature_out(block, place, step, flip, at):
        return remote(
            block, win.at[place, s], f_send.at[at], f_recv.at[place], (pair_of(-step, flip), s)
        )

    own = features.at[0]
    passed = win.at[1 - x, s]
    even = lax.rem(q, 2) == 0
    feature_across = feature_out(own, x, 0, 1, 0)
    near_zero = [feature_out(block, 2, 1, 0, 1) for block in (own, passed)]
    near_one = [feature_out(block, 3, 1, 0, 2) for block in (passed, own)]
    far_zero = feature_out(own, WINDOW, 2, 0, 3)
    onto_next = feature_out(win.at[WINDOW, s], 2, -1, 0, 4)
    far_across = feature_out(win.at[WINDOW, s], WINDOW, 0, 1, 5)

    def relay(place, block=None):
        target = win.at[place, s]
        return remote(
            target if block is None else block, target, fr_send.at[place], fr_recv.at[place],
            sibling,
        )

    for copy in table_out:
        copy.start()
    feature_across.start()

    @pl.when(x == 0)
    def _():
        far_zero.start()

        @pl.when(jnp.logical_not(even))
        def _():
            near_zero[0].start()

    @pl.when(x == 1)
    def _():
        near_one[1].start()

    relay(x, own).start()

    @pl.when(at_home)
    def _():
        for copy in fc_home + gains_out:
            copy.start()
        weights_out[0].start()

    swapped = len(fc_out) // 2

    @pl.when(jnp.logical_not(at_home))
    def _():
        for copy in fc_out[:swapped]:
            copy.start()

        @pl.when(x == 1)
        def _():
            for copy in fc_out[swapped:]:
                copy.start()

    def piece(number):
        turn = lax.div(number, kinds // 2)
        last = turn == 2 * chips - 1
        ahead = jnp.logical_or(turn == 0, jnp.logical_and(lax.rem(turn, 2) == 1, turn < 2 * chips - 1))
        step = jnp.where(
            turn == 0,
            0,
            jnp.where(last, chips - 1, jnp.where(ahead, lax.div(turn + 1, 2), lax.div(turn, 2) - 1)),
        )
        kind = lax.rem(number, kinds // 2) + jnp.where(ahead, 0, kinds // 2)
        block = ring_view(step, kind, s)
        pltpu.make_async_copy(block, block, r_recv.at[step, kind]).wait()

        @pl.when(step < chips - 1)
        def _():
            remote(
                block, ring_view(step + 1, kind, s), r_send.at[step, kind],
                r_recv.at[step + 1, kind], onward,
            ).start()

        remote(block, block, x_send.at[step, kind], x_recv.at[step, kind], sibling).start()

    def pieces(low, high):
        def body(number, carry):
            piece(number)
            return carry

        lax.fori_loop(low, high, body, 0)

    def arrived(place):
        block = win.at[place, s]
        pltpu.make_async_copy(block, block, f_recv.at[place]).wait()
        relay(place).start()

    group = kinds // 2
    early = 5 * group
    pieces(0, group)
    arrived(1 - x)

    @pl.when(x == 0)
    def _():
        near_one[0].start()
        arrived(WINDOW)

        @pl.when(even)
        def _():
            onto_next.start()

        far_across.start()

        @pl.when(jnp.logical_not(at_home))
        def _():
            for copy in fc_out[swapped:]:
                copy.start()

    @pl.when(x == 1)
    def _():
        near_zero[1].start()

    @pl.when(at_home)
    def _():
        weights_out[1].start()

    pieces(group, 2 * group)
    arrived(3)

    @pl.when(x == 1)
    def _():
        arrived(WINDOW)

    pieces(2 * group, 4 * group)
    arrived(2)

    @pl.when(at_home)
    def _():
        for copy in weights_out[2:]:
            copy.start()

    pieces(4 * group, early)
    own_win.wait()
    for place in range(REACH):
        block = win.at[place, 1 - s]
        pltpu.make_async_copy(block, block, fr_recv.at[place]).wait()
    for copy in table_out:
        copy.wait_recv()
    for at, ref in enumerate(gain_refs):
        pltpu.make_async_copy(ref, gains.at[at], g_recv.at[at]).wait()

    def weight_wait(at):
        src, dst = weights[at]
        pltpu.make_async_copy(src, dst, w_recv.at[at]).wait()

    def first_wait(slot, at):
        @pl.when(slot == 0)
        def _():
            weight_wait(at)

    def entry(slot, column, core):
        local = slot_images[column, slot]
        return jnp.where(x == core, local, table[column, slot])

    def place_of(slot, column, core=None):
        core = s if core is None else core
        stored = image_slot[entry(slot, column, core)]
        ahead = lax.rem(stored - (2 * q + core) + devices, devices)
        return jnp.minimum(ahead, WINDOW - 1) + core

    def tokens_of(place):
        return jnp.concatenate([win[place, 0], win[place, 1]], axis=-1).astype(jnp.float32)

    stops = 4 * slots
    each = max((total_pieces * 26 // 32 - early) // stops, 0)
    fronted = early + each * stops

    def front(slot, carry):
        told = [0]

        def comm():
            base = early + (4 * slot + told[0]) * each
            told[0] += 1
            for at in range(each):
                piece(base + at)

        first_wait(slot, 0)
        tokens = tokens_of(place_of(slot, x))
        state = layer_norm(tokens, gains[0]).astype(jnp.bfloat16)
        triple[...] = matmul(state, m_qkv[...]).astype(jnp.bfloat16)
        comm()
        attend(triple, triple, triple, width, 2 * width, mixed, width, None)
        first_wait(slot, 1)
        first = tokens + matmul(mixed[...], m_self_out[...])
        second[slot, 0:rows, :] = first
        comm()
        first_wait(slot, 2)
        first_wait(slot, 3)
        query_in = layer_norm(first, gains[1]).astype(jnp.bfloat16)
        memory = tokens_of(place_of(slot, 1 - x))
        memory_in = layer_norm(memory, gains[2]).astype(jnp.bfloat16)
        queries[...] = matmul(query_in, m_query[...]).astype(jnp.bfloat16)
        kv[...] = matmul(memory_in, m_memory[...]).astype(jnp.bfloat16)
        attend(queries, kv, kv, 0, width, mixed, width, comm)
        first_wait(slot, 4)
        result = second[slot, 0:rows, :] + matmul(mixed[...], m_cross_out[...])
        second[slot, 0:rows, :] = result
        hidden[slot, 0:rows, :] = layer_norm(result, gains[3]).astype(jnp.bfloat16)
        comm()
        return carry

    second[...] = jnp.zeros_like(second)
    hidden[...] = jnp.zeros_like(hidden)
    lax.fori_loop(0, slots, front, 0)

    def relayed(first, count):
        def body(at, carry):
            turn, which = first + lax.div(at, 2), lax.rem(at, 2)
            step, kind = lax.div(turn, split), 2 * lax.rem(turn, split) + which
            view = ring_view(step, kind, 1 - s)
            pltpu.make_async_copy(view, view, x_recv.at[step, kind]).wait()
            return carry

        lax.fori_loop(0, 2 * count, body, 0)

    def expand(first, turns, slot):
        count = 2 * turns
        if rank % 16 == 0:
            groups = [
                [ring_w[f, pl.ds(2 * first, count)].reshape(count * rank, width) for f in range(2)]
            ]
        else:
            groups = [[ring_w[f, 2 * first + at] for f in range(2)] for at in range(count)]
        total = second[slot]
        for fc1, fc2 in groups:
            pre = matmul_t(hidden[slot], fc1)
            act = (pre * (1.0 + lax.erf(pre * 0.5**0.5)) * 0.5).astype(jnp.bfloat16)
            total = total + matmul(act, fc2)
        second[slot] = total

    turns = split * chips
    span = turns // BLOCKS
    whole = total_pieces - group
    left = whole - fronted
    places = (BLOCKS - 1) * slots
    pace = BLOCKS * slots

    def expand_early(turn, carry):
        block, slot = lax.div(turn, slots), lax.rem(turn, slots)

        @pl.when(slot == 0)
        def _():
            relayed(block * span, span)

        expand(block * span, span, slot)
        pieces(
            fronted + lax.div(turn * left, pace), fronted + lax.div((turn + 1) * left, pace)
        )
        return carry

    lax.fori_loop(0, places, expand_early, 0)
    pieces(fronted + places * left // pace, whole)
    relayed((BLOCKS - 1) * span, span - 1)

    def expand_late(slot, carry):
        expand((BLOCKS - 1) * span, span - 1, slot)
        pieces(
            whole + lax.div(slot * group, slots), whole + lax.div((slot + 1) * group, slots)
        )
        return carry

    lax.fori_loop(0, slots, expand_late, 0)
    weight_wait(5)
    weight_wait(6)
    relayed(turns - 1, 1)
    pix = half // 4

    def terms(slot, which, target):
        raw[...] = matmul(hidden[slot], m_head[which])
        conf = 1.0 + jnp.exp(raw[0:rows, 3 * pix :])
        for comp in range(4):
            at = slice(comp * pix, (comp + 1) * pix)
            value = conf if comp == 3 else conf * raw[0:rows, at]
            target[slot, :, at] = value.astype(target.dtype)

    def away(slot):
        return remote(
            term_away.at[slot], term_in.at[slot], a_send.at[slot], a_recv.at[slot], sibling
        )

    def expand_last(slot, carry):
        expand(turns - 1, 1, slot)
        hidden[slot] = layer_norm(second[slot], gains[4]).astype(jnp.bfloat16)
        terms(slot, 1 - s, term_away)
        away(slot).start()
        return carry

    def own_terms(slot, carry):
        terms(slot, s, term)
        return carry

    lax.fori_loop(0, slots, expand_last, 0)
    lax.fori_loop(0, slots, own_terms, 0)
    for slot in range(slots):
        away(slot).wait_recv()

    sources = []
    for core, ref in ((s, term), (1 - s, term_in)):
        live = jnp.where(x == core, slot_count[0], counts[0])
        for slot in range(slots):
            sources.append((place_of(slot, x, core), slot < live, ref, slot))

    quarter = half // 2

    def sums_of(place, part):
        sums = jnp.zeros((rows, quarter), jnp.float32)
        for to, live, ref, slot in sources:
            chosen = jnp.logical_and(to == place, live)
            value = ref[slot, :, part * quarter : (part + 1) * quarter].astype(jnp.float32)
            sums = sums + jnp.where(chosen, value, 0.0)
        return sums

    def far_copy(at, part, step, flip):
        return remote(
            far_out.at[at, part], far_in.at[at, part], b_send.at[at, part], b_recv.at[at, part],
            (pair_of(step, flip), s),
        )

    def far_send(at, part, step, flip, sums):
        far_out[at, part] = sums.astype(jnp.bfloat16)
        far_copy(at, part, step, flip).start()

    def far_wait(at, part):
        block = far_in.at[at, part]
        pltpu.make_async_copy(block, block, b_recv.at[at, part]).wait()
        return block[...].astype(jnp.float32)

    for part in range(2):
        far_send(1, part, 0, 1, sums_of(3 - x, part))
    for part in range(2):
        far_send(0, part, 2, 0, sums_of(WINDOW, part))

    @pl.when(x == 0)
    def _():
        for part in range(2):
            far_send(3, part, 0, 1, sums_of(1, part))

    for part in range(2):
        final[part] = sums_of(2 + x, part)
    for part in range(2):
        far_send(2, part, 1, 0, final[part] + far_wait(1, part))
    for part in range(2):
        final[part] = sums_of(x, part)

    @pl.when(x == 1)
    def _():
        for part in range(2):
            far_send(3, part, 0, 1, sums_of(0, part) + far_wait(0, part))

    @pl.when(x == 0)
    def _():
        for part in range(2):
            final[part] = final[part] + far_wait(0, part)

    for part in range(2):
        final[part] = final[part] + far_wait(2, part)
    for part in range(2):
        final[part] = final[part] + far_wait(3, part)
    conf = jnp.maximum(final[1, :, pix:], 1.0)
    for comp in range(3):
        value = final[comp // 2, :, comp % 2 * pix : (comp % 2 + 1) * pix]
        out[0, :, comp * pix : (comp + 1) * pix] = (value / conf).astype(jnp.bfloat16)

    for copy in (feature_across, near_one[0]):
        copy.wait_send()

    @pl.when(x == 0)
    def _():
        far_zero.wait_send()
        far_across.wait_send()

        @pl.when(even)
        def _():
            onto_next.wait_send()

    @pl.when(jnp.logical_or(x == 1, jnp.logical_not(even)))
    def _():
        near_zero[0].wait_send()

    for place in range(REACH):
        relay(place).wait_send()

    @pl.when(at_home)
    def _():
        for copy in fc_home + gains_out + weights_out:
            copy.wait_send()

    @pl.when(jnp.logical_not(at_home))
    def _():
        for copy in fc_out:
            copy.wait_send()

    for copy in table_out:
        copy.wait_send()

    def drain(number, carry):
        step, kind = lax.div(number, kinds), lax.rem(number, kinds)
        block = ring_view(step, kind, s)

        @pl.when(step < chips - 1)
        def _():
            remote(
                block, block, r_send.at[step, kind], r_recv.at[step, kind], onward
            ).wait_send()

        remote(block, block, x_send.at[step, kind], x_recv.at[step, kind], sibling).wait_send()
        return carry

    lax.fori_loop(0, total_pieces, drain, 0)
    for slot in range(slots):
        away(slot).wait_send()
    for at, (step, flip) in enumerate(((2, 0), (0, 1), (1, 0), (0, 1))):
        for part in range(2):
            far_copy(at, part, step, flip).wait_send()


def on_device(
    features, image_slot, slot_images, slot_count, gain_self, gain_query, gain_memory, gain_mlp,
    gain_head, w_qkv, w_self_out, w_query, w_memory, w_cross_out, w_fc1, w_fc2, w_head,
):
    devices = lax.axis_size("pairs")
    chips = devices // 2
    blocks, rows, part = features.shape
    if blocks != 1 or chips % BLOCKS:
        raise ValueError("unsupported split")
    width = w_qkv.shape[1]
    slots = slot_images.shape[0]
    tall = padded(rows)
    shard = w_fc1.shape[1]
    split = 2 if shard % 32 == 0 else 1
    kinds = 2 * split
    half = w_head.shape[2] // 2
    bf16, f32 = jnp.bfloat16, jnp.float32
    dma = pltpu.SemaphoreType.DMA
    anywhere = pl.BlockSpec(memory_space=pl.ANY)
    return pl.pallas_call(
        decoder_kernel,
        out_shape=pltpu.VMEM((1, rows, half * 3 // 4), bf16),
        in_specs=[pl.BlockSpec(memory_space=pltpu.SMEM)] * 3 + [anywhere] * 14,
        out_specs=pl.BlockSpec(memory_space=pltpu.VMEM),
        scratch_shapes=[
            pltpu.VMEM((REACH, 2, rows, part), bf16),
            pltpu.SMEM(slot_images.shape[::-1], jnp.int32),
            pltpu.SMEM(slot_count.shape, jnp.int32),
            pltpu.VMEM((5, 1, width), f32),
            pltpu.VMEM(w_qkv.shape[1:], bf16),
            pltpu.VMEM(w_self_out.shape[1:], bf16),
            pltpu.VMEM(w_query.shape[1:], bf16),
            pltpu.VMEM(w_memory.shape[1:], bf16),
            pltpu.VMEM(w_cross_out.shape[1:], bf16),
            pltpu.VMEM((2, width, half), bf16),
            pltpu.VMEM((2, devices * split, shard // split, width), bf16),
            pltpu.VMEM((rows, 3 * width), bf16),
            pltpu.VMEM((rows, 2 * width), bf16),
            pltpu.VMEM((rows, width), bf16),
            pltpu.VMEM((rows, width), bf16),
            pltpu.VMEM((slots, tall, width), f32),
            pltpu.VMEM((slots, tall, width), bf16),
            pltpu.VMEM((tall, half), f32),
            pltpu.VMEM((slots, rows, half), f32),
            pltpu.VMEM((slots, rows, half), bf16),
            pltpu.VMEM((slots, rows, half), bf16),
            pltpu.VMEM((4, 2, rows, half // 2), bf16),
            pltpu.VMEM((4, 2, rows, half // 2), bf16),
            pltpu.VMEM((2, rows, half // 2), f32),
            dma, dma((6,)), dma((REACH,)), dma((REACH,)), dma((REACH,)),
            dma((2,)), dma((2,)), dma((5,)), dma((5,)), dma((7,)), dma((7,)),
            dma((kinds,)), dma((chips, kinds)), dma((chips, kinds)), dma((chips, kinds)),
            dma((chips, kinds)), dma((slots,)), dma((slots,)), dma((4, 2)), dma((4, 2)),
        ],
        compiler_params=pltpu.CompilerParams(
            collective_id=0, has_side_effects=True, vmem_limit_bytes=VMEM_LIMIT
        ),
    )(
        image_slot, slot_images.T, slot_count, features, gain_self, gain_query, gain_memory,
        gain_mlp, gain_head, w_qkv, w_self_out, w_query, w_memory, w_cross_out, w_fc1, w_fc2,
        w_head,
    )


def solution(mesh):
    placed = (
        P("pairs", None, "side"),
        P(),
        P("pairs", None),
        P("pairs"),
        P("side", None),
        P("side", None),
        P("side", None),
        P("side", None),
        P("side", None),
        P("side", None, None),
        P("side", None, None),
        P("side", None, None),
        P("side", None, None),
        P("side", None, None),
        P("side", "pairs", None),
        P("side", "pairs", None),
        P("side", None, None),
    )
    return jax.shard_map(
        on_device, mesh=mesh, in_specs=placed, out_specs=P("pairs", None, "side"), check_vma=False
    )
```

```python
import functools

import jax
import jax.numpy as jnp
from jax import lax
from jax.experimental import pallas as pl
from jax.experimental.pallas import tpu as pltpu
from jax.sharding import PartitionSpec as P

HEAD_DIM = 64
WINDOW = 4
PAIR = 2 * HEAD_DIM
BLOCKS = 4
REACH = WINDOW + 1
VMEM_LIMIT = 63 * 1024 * 1024
MESH = pl.DeviceIdType.MESH


def padded(rows):
    return -(-rows // 16) * 16


def layer_norm(values, gain):
    center = values - jnp.mean(values, axis=-1, keepdims=True)
    spread = jnp.mean(center * center, axis=-1, keepdims=True)
    return center * lax.rsqrt(spread + 1e-06) * gain


def matmul(left, right):
    return jnp.dot(left, right, preferred_element_type=jnp.float32)


def matmul_t(left, right):
    return lax.dot_general(
        left, right, (((1,), (1,)), ((), ())), preferred_element_type=jnp.float32
    )


def attend(q_ref, k_ref, v_ref, k_at, v_at, o_ref, width, comm):
    rows = q_ref.shape[0]
    low = lax.broadcasted_iota(jnp.int32, (rows, PAIR), 1) < HEAD_DIM
    for pair in range(width // PAIR):
        if comm is not None and pair * PAIR == width // 2:
            comm()
        q = q_ref[:, pair * PAIR : (pair + 1) * PAIR]
        k = k_ref[:, k_at + pair * PAIR : k_at + (pair + 1) * PAIR]
        v = v_ref[:, v_at + pair * PAIR : v_at + (pair + 1) * PAIR]
        mixed = None
        for keep in (low, jnp.logical_not(low)):
            q_head = jnp.where(keep, q, jnp.zeros_like(q))
            v_head = jnp.where(keep, v, jnp.zeros_like(v))
            scores = matmul_t(q_head, k) * HEAD_DIM ** (-0.5)
            expon = jnp.exp(scores)
            weights = (expon / jnp.sum(expon, axis=-1, keepdims=True)).astype(jnp.bfloat16)
            part = matmul(weights, v_head)
            mixed = part if mixed is None else mixed + part
        o_ref[:, pair * PAIR : (pair + 1) * PAIR] = mixed.astype(jnp.bfloat16)


def remote(src, dst, send, recv, device):
    return pltpu.make_async_remote_copy(
        src_ref=src, dst_ref=dst, send_sem=send, recv_sem=recv, device_id=device,
        device_id_type=MESH,
    )


def decoder_kernel(
    image_slot, slot_images, slot_count, features,
    g_self, g_query, g_memory, g_mlp, g_head,
    w_qkv, w_self_out, w_query, w_memory, w_cross_out, w_fc1, w_fc2, w_head,
    out,
    win, table, counts, gains, m_qkv, m_self_out, m_query, m_memory, m_cross_out, m_head, ring_w,
    triple, kv, queries, mixed, second, hidden, raw, term, term_away, term_in, far_out, far_in,
    final,
    f_local, f_send, f_recv, fr_send, fr_recv, t_send, t_recv, g_send, g_recv, w_send, w_recv,
    s_send, r_send, r_recv, x_send, x_recv, a_send, a_recv, b_send, b_recv,
):
    devices = lax.axis_size("pairs")
    chips = devices // 2
    here = lax.axis_index("pairs")
    s = lax.axis_index("side")
    x = lax.rem(here, 2)
    q = lax.div(here, 2)
    rows = features.shape[1]
    width = m_qkv.shape[0]
    slots = second.shape[0]
    tall = second.shape[1]
    shard = w_fc1.shape[1]
    rank = ring_w.shape[2]
    split = shard // rank
    kinds = 2 * split
    total_pieces = kinds * chips

    sibling = (here, 1 - s)
    partner = (2 * q + s, x)
    at_home = x == s

    def pair_of(step, flip):
        chip = lax.rem(q + (step + chips), chips)
        return 2 * chip + (1 - x if flip else x)

    up = jnp.where(
        lax.rem(q, 2) == 0,
        jnp.where(q + 2 < chips, q + 2, chips - 1),
        jnp.where(q >= 3, q - 2, 0),
    )
    down = jnp.where(
        lax.rem(q, 2) == 0,
        jnp.where(q == 0, 1, q - 2),
        jnp.where(q + 2 < chips, q + 2, chips - 2),
    )
    onward = (2 * jnp.where(s == 0, up, down) + x, s)

    mats = (
        (w_qkv, m_qkv), (w_self_out, m_self_out), (w_memory, m_memory), (w_query, m_query),
        (w_cross_out, m_cross_out),
    )
    half = w_head.shape[2] // 2
    weights = [(src.at[0], dst) for src, dst in mats]
    weights += [(w_head.at[0, :, h * half : (h + 1) * half], m_head.at[h]) for h in range(2)]
    gain_refs = (g_self, g_query, g_memory, g_mlp, g_head)
    fcs = (w_fc1, w_fc2)

    def ring_view(step, kind, ring):
        return ring_w.at[lax.rem(kind, 2), 2 * (split * step + lax.div(kind, 2)) + ring]

    def own_fc(which, piece):
        if split == 1:
            return fcs[which].at[0]
        return fcs[which].at[0, pl.ds(pl.multiple_of(piece * rank, rank), rank)]

    own_win = pltpu.make_async_copy(features.at[0], win.at[x, s], f_local)
    own_win.start()

    @pl.when(at_home)
    def _():
        for at, ref in enumerate(gain_refs):
            pltpu.make_async_copy(ref, gains.at[at], g_recv.at[at]).start()
        for which in range(2):
            pltpu.make_async_copy(
                own_fc(which, s), ring_view(0, which, s), r_recv.at[0, which]
            ).start()
        for at, (src, dst) in enumerate(weights):
            pltpu.make_async_copy(src, dst, w_recv.at[at]).start()

    barrier = pltpu.get_barrier_semaphore()
    for step in range(-2, 3):
        for flip in range(2):
            if step or flip:
                pl.semaphore_signal(
                    barrier, inc=1, device_id=(pair_of(step, flip), s), device_id_type=MESH
                )
    pl.semaphore_signal(barrier, inc=1, device_id=sibling, device_id_type=MESH)

    @pl.when(jnp.logical_not(at_home))
    def _():
        pl.semaphore_signal(barrier, inc=1, device_id=partner, device_id_type=MESH)

    pl.semaphore_wait(barrier, 10 + (1 - at_home.astype(jnp.int32)))

    table_out = [
        remote(slot_images, table, t_send.at[0], t_recv.at[0], (pair_of(0, 1), s)),
        remote(slot_count, counts, t_send.at[1], t_recv.at[1], (pair_of(0, 1), s)),
    ]
    across = (2 * q + s, s)
    if split == 1:
        fc_home = []
        fc_out = [
            remote(own_fc(f, 0), ring_view(0, f, x), s_send.at[f], r_recv.at[0, f], partner)
            for f in range(2)
        ]
    else:
        fc_home = [
            remote(
                own_fc(f, 1 - s), ring_view(0, f, 1 - s), s_send.at[f], r_recv.at[0, f], sibling
            )
            for f in range(2)
        ]
        fc_out = [
            remote(
                own_fc(f, ring), ring_view(0, 2 + f, ring), s_send.at[2 * f + to],
                r_recv.at[0, 2 + f], device,
            )
            for f in range(2)
            for to, (ring, device) in enumerate(((x, partner), (s, across)))
        ]
    gains_out = [
        remote(ref, gains.at[at], g_send.at[at], g_recv.at[at], sibling)
        for at, ref in enumerate(gain_refs)
    ]
    weights_out = [
        remote(src, dst, w_send.at[at], w_recv.at[at], sibling)
        for at, (src, dst) in enumerate(weights)
    ]

    def feature_out(block, place, step, flip, at):
        return remote(
            block, win.at[place, s], f_send.at[at], f_recv.at[place], (pair_of(-step, flip), s)
        )

    own = features.at[0]
    passed = win.at[1 - x, s]
    even = lax.rem(q, 2) == 0
    feature_across = feature_out(own, x, 0, 1, 0)
    near_zero = [feature_out(block, 2, 1, 0, 1) for block in (own, passed)]
    near_one = [feature_out(block, 3, 1, 0, 2) for block in (passed, own)]
    far_zero = feature_out(own, WINDOW, 2, 0, 3)
    onto_next = feature_out(win.at[WINDOW, s], 2, -1, 0, 4)
    far_across = feature_out(win.at[WINDOW, s], WINDOW, 0, 1, 5)

    def relay(place, block=None):
        target = win.at[place, s]
        return remote(
            target if block is None else block, target, fr_send.at[place], fr_recv.at[place],
            sibling,
        )

    @pl.when(at_home)
    def _():
        for copy in fc_home:
            copy.start()

    for copy in table_out:
        copy.start()
    feature_across.start()

    @pl.when(x == 0)
    def _():
        far_zero.start()

        @pl.when(jnp.logical_not(even))
        def _():
            near_zero[0].start()

    @pl.when(x == 1)
    def _():
        near_one[1].start()

    relay(x, own).start()

    @pl.when(at_home)
    def _():
        for copy in gains_out:
            copy.start()
        weights_out[0].start()

    swapped = len(fc_out) // 2

    @pl.when(jnp.logical_not(at_home))
    def _():
        for copy in fc_out[:swapped]:
            copy.start()

        @pl.when(x == 1)
        def _():
            for copy in fc_out[swapped:]:
                copy.start()

    def piece(number):
        turn = lax.div(number, kinds // 2)
        last = turn == 2 * chips - 1
        ahead = jnp.logical_or(turn == 0, jnp.logical_and(lax.rem(turn, 2) == 1, turn < 2 * chips - 1))
        step = jnp.where(
            turn == 0,
            0,
            jnp.where(last, chips - 1, jnp.where(ahead, lax.div(turn + 1, 2), lax.div(turn, 2) - 1)),
        )
        kind = lax.rem(number, kinds // 2) + jnp.where(ahead, 0, kinds // 2)
        block = ring_view(step, kind, s)
        pltpu.make_async_copy(block, block, r_recv.at[step, kind]).wait()

        @pl.when(step < chips - 1)
        def _():
            remote(
                block, ring_view(step + 1, kind, s), r_send.at[step, kind],
                r_recv.at[step + 1, kind], onward,
            ).start()

        remote(block, block, x_send.at[step, kind], x_recv.at[step, kind], sibling).start()

    def pieces(low, high):
        def body(number, carry):
            piece(number)
            return carry

        lax.fori_loop(low, high, body, 0)

    def arrived(place):
        block = win.at[place, s]
        pltpu.make_async_copy(block, block, f_recv.at[place]).wait()
        relay(place).start()

    group = kinds // 2
    early = 5 * group
    pieces(0, group)
    arrived(1 - x)

    @pl.when(x == 0)
    def _():
        near_one[0].start()
        arrived(WINDOW)

        @pl.when(even)
        def _():
            onto_next.start()

        far_across.start()

        @pl.when(jnp.logical_not(at_home))
        def _():
            for copy in fc_out[swapped:]:
                copy.start()

    @pl.when(x == 1)
    def _():
        near_zero[1].start()

    @pl.when(at_home)
    def _():
        weights_out[1].start()

    pieces(group, 2 * group)
    arrived(3)

    @pl.when(x == 1)
    def _():
        arrived(WINDOW)

    pieces(2 * group, 4 * group)
    arrived(2)

    @pl.when(at_home)
    def _():
        for copy in weights_out[2:]:
            copy.start()

    pieces(4 * group, early)
    own_win.wait()
    for place in range(REACH):
        block = win.at[place, 1 - s]
        pltpu.make_async_copy(block, block, fr_recv.at[place]).wait()
    for copy in table_out:
        copy.wait_recv()
    for at, ref in enumerate(gain_refs):
        pltpu.make_async_copy(ref, gains.at[at], g_recv.at[at]).wait()

    def weight_wait(at):
        src, dst = weights[at]
        pltpu.make_async_copy(src, dst, w_recv.at[at]).wait()

    def first_wait(slot, at):
        @pl.when(slot == 0)
        def _():
            weight_wait(at)

    def entry(slot, column, core):
        local = slot_images[column, slot]
        return jnp.where(x == core, local, table[column, slot])

    def place_of(slot, column, core=None):
        core = s if core is None else core
        stored = image_slot[entry(slot, column, core)]
        ahead = lax.rem(stored - (2 * q + core) + devices, devices)
        return jnp.minimum(ahead, WINDOW - 1) + core

    def tokens_of(place):
        return jnp.concatenate([win[place, 0], win[place, 1]], axis=-1).astype(jnp.float32)

    stops = 4 * slots
    each = max((total_pieces * 26 // 32 - early) // stops, 0)
    fronted = early + each * stops

    def front(slot, carry):
        told = [0]

        def comm():
            base = early + (4 * slot + told[0]) * each
            told[0] += 1
            for at in range(each):
                piece(base + at)

        first_wait(slot, 0)
        tokens = tokens_of(place_of(slot, x))
        state = layer_norm(tokens, gains[0]).astype(jnp.bfloat16)
        triple[...] = matmul(state, m_qkv[...]).astype(jnp.bfloat16)
        comm()
        attend(triple, triple, triple, width, 2 * width, mixed, width, None)
        first_wait(slot, 1)
        first = tokens + matmul(mixed[...], m_self_out[...])
        second[slot, 0:rows, :] = first
        comm()
        first_wait(slot, 2)
        first_wait(slot, 3)
        query_in = layer_norm(first, gains[1]).astype(jnp.bfloat16)
        memory = tokens_of(place_of(slot, 1 - x))
        memory_in = layer_norm(memory, gains[2]).astype(jnp.bfloat16)
        queries[...] = matmul(query_in, m_query[...]).astype(jnp.bfloat16)
        kv[...] = matmul(memory_in, m_memory[...]).astype(jnp.bfloat16)
        attend(queries, kv, kv, 0, width, mixed, width, comm)
        first_wait(slot, 4)
        result = second[slot, 0:rows, :] + matmul(mixed[...], m_cross_out[...])
        second[slot, 0:rows, :] = result
        hidden[slot, 0:rows, :] = layer_norm(result, gains[3]).astype(jnp.bfloat16)
        comm()
        return carry

    second[...] = jnp.zeros_like(second)
    hidden[...] = jnp.zeros_like(hidden)
    lax.fori_loop(0, slots, front, 0)

    def relayed(first, count):
        def body(at, carry):
            turn, which = first + lax.div(at, 2), lax.rem(at, 2)
            step, kind = lax.div(turn, split), 2 * lax.rem(turn, split) + which
            view = ring_view(step, kind, 1 - s)
            pltpu.make_async_copy(view, view, x_recv.at[step, kind]).wait()
            return carry

        lax.fori_loop(0, 2 * count, body, 0)

    def expand(first, turns, slot):
        count = 2 * turns
        if rank % 16 == 0:
            groups = [
                [ring_w[f, pl.ds(2 * first, count)].reshape(count * rank, width) for f in range(2)]
            ]
        else:
            groups = [[ring_w[f, 2 * first + at] for f in range(2)] for at in range(count)]
        total = second[slot]
        for fc1, fc2 in groups:
            pre = matmul_t(hidden[slot], fc1)
            act = (pre * (1.0 + lax.erf(pre * 0.5**0.5)) * 0.5).astype(jnp.bfloat16)
            total = total + matmul(act, fc2)
        second[slot] = total

    turns = split * chips
    span = turns // BLOCKS
    whole = total_pieces - group
    left = whole - fronted
    places = (BLOCKS - 1) * slots
    pace = BLOCKS * slots

    def expand_early(turn, carry):
        block, slot = lax.div(turn, slots), lax.rem(turn, slots)

        @pl.when(slot == 0)
        def _():
            relayed(block * span, span)

        expand(block * span, span, slot)
        pieces(
            fronted + lax.div(turn * left, pace), fronted + lax.div((turn + 1) * left, pace)
        )
        return carry

    lax.fori_loop(0, places, expand_early, 0)
    pieces(fronted + places * left // pace, whole)
    relayed((BLOCKS - 1) * span, span - 1)

    early_rate = -(-group // (slots - 1))

    def expand_late(slot, carry):
        expand((BLOCKS - 1) * span, span - 1, slot)
        pieces(
            whole + jnp.minimum(slot * early_rate, group),
            whole + jnp.minimum((slot + 1) * early_rate, group),
        )
        return carry

    lax.fori_loop(0, slots, expand_late, 0)
    weight_wait(5)
    weight_wait(6)
    relayed(turns - 1, 1)
    pix = half // 4

    def terms(slot, which, target):
        raw[...] = matmul(hidden[slot], m_head[which])
        conf = 1.0 + jnp.exp(raw[0:rows, 3 * pix :])
        for comp in range(4):
            at = slice(comp * pix, (comp + 1) * pix)
            value = conf if comp == 3 else conf * raw[0:rows, at]
            target[slot, :, at] = value.astype(target.dtype)

    def away(slot):
        return remote(
            term_away.at[slot], term_in.at[slot], a_send.at[slot], a_recv.at[slot], sibling
        )

    def expand_last(slot, carry):
        expand(turns - 1, 1, slot)
        hidden[slot] = layer_norm(second[slot], gains[4]).astype(jnp.bfloat16)
        terms(slot, 1 - s, term_away)
        away(slot).start()
        return carry

    def own_terms(slot, carry):
        terms(slot, s, term)
        return carry

    for slot in range(slots):
        expand_last(slot, 0)
    for slot in range(slots):
        own_terms(slot, 0)
    for slot in range(slots):
        away(slot).wait_recv()

    sources = []
    for core, ref in ((s, term), (1 - s, term_in)):
        live = jnp.where(x == core, slot_count[0], counts[0])
        for slot in range(slots):
            sources.append((place_of(slot, x, core), slot < live, ref, slot))

    quarter = half // 2

    def sums_of(place, part):
        sums = jnp.zeros((rows, quarter), jnp.float32)
        for to, live, ref, slot in sources:
            chosen = jnp.logical_and(to == place, live)
            value = ref[slot, :, part * quarter : (part + 1) * quarter].astype(jnp.float32)
            sums = sums + jnp.where(chosen, value, 0.0)
        return sums

    def far_copy(at, part, step, flip):
        return remote(
            far_out.at[at, part], far_in.at[at, part], b_send.at[at, part], b_recv.at[at, part],
            (pair_of(step, flip), s),
        )

    def far_send(at, part, step, flip, sums):
        far_out[at, part] = sums.astype(jnp.bfloat16)
        far_copy(at, part, step, flip).start()

    def far_wait(at, part):
        block = far_in.at[at, part]
        pltpu.make_async_copy(block, block, b_recv.at[at, part]).wait()
        return block[...].astype(jnp.float32)

    for part in range(2):
        far_send(1, part, 0, 1, sums_of(3 - x, part))
    for part in range(2):
        far_send(0, part, 2, 0, sums_of(WINDOW, part))

    @pl.when(x == 0)
    def _():
        for part in range(2):
            far_send(3, part, 0, 1, sums_of(1, part))

    for copy in (feature_across, near_one[0]):
        copy.wait_send()

    @pl.when(x == 0)
    def _():
        far_zero.wait_send()
        far_across.wait_send()

        @pl.when(even)
        def _():
            onto_next.wait_send()

    @pl.when(jnp.logical_or(x == 1, jnp.logical_not(even)))
    def _():
        near_zero[0].wait_send()

    for place in range(REACH):
        relay(place).wait_send()

    @pl.when(at_home)
    def _():
        for copy in fc_home + gains_out + weights_out:
            copy.wait_send()

    @pl.when(jnp.logical_not(at_home))
    def _():
        for copy in fc_out:
            copy.wait_send()

    for copy in table_out:
        copy.wait_send()

    def drain(number, carry):
        step, kind = lax.div(number, kinds), lax.rem(number, kinds)
        block = ring_view(step, kind, s)

        @pl.when(step < chips - 1)
        def _():
            remote(
                block, block, r_send.at[step, kind], r_recv.at[step, kind], onward
            ).wait_send()

        remote(block, block, x_send.at[step, kind], x_recv.at[step, kind], sibling).wait_send()
        return carry

    lax.fori_loop(0, total_pieces, drain, 0)
    for part in range(2):
        final[part] = sums_of(2 + x, part)
    for part in range(2):
        far_send(2, part, 1, 0, final[part] + far_wait(1, part))
    for part in range(2):
        final[part] = sums_of(x, part)

    @pl.when(x == 1)
    def _():
        for part in range(2):
            far_send(3, part, 0, 1, sums_of(0, part) + far_wait(0, part))

    @pl.when(x == 0)
    def _():
        for part in range(2):
            final[part] = final[part] + far_wait(0, part)

    for part in range(2):
        final[part] = final[part] + far_wait(2, part)
    for part in range(2):
        final[part] = final[part] + far_wait(3, part)
    conf = jnp.maximum(final[1, :, pix:], 1.0)
    for comp in range(3):
        value = final[comp // 2, :, comp % 2 * pix : (comp % 2 + 1) * pix]
        out[0, :, comp * pix : (comp + 1) * pix] = (value / conf).astype(jnp.bfloat16)

    for slot in range(slots):
        away(slot).wait_send()
    for at, (step, flip) in enumerate(((2, 0), (0, 1), (1, 0), (0, 1))):
        for part in range(2):
            far_copy(at, part, step, flip).wait_send()


def on_device(
    features, image_slot, slot_images, slot_count, gain_self, gain_query, gain_memory, gain_mlp,
    gain_head, w_qkv, w_self_out, w_query, w_memory, w_cross_out, w_fc1, w_fc2, w_head,
):
    devices = lax.axis_size("pairs")
    chips = devices // 2
    blocks, rows, part = features.shape
    if blocks != 1 or chips % BLOCKS:
        raise ValueError("unsupported split")
    width = w_qkv.shape[1]
    slots = slot_images.shape[0]
    tall = padded(rows)
    shard = w_fc1.shape[1]
    split = 2 if shard % 32 == 0 else 1
    kinds = 2 * split
    half = w_head.shape[2] // 2
    bf16, f32 = jnp.bfloat16, jnp.float32
    dma = pltpu.SemaphoreType.DMA
    anywhere = pl.BlockSpec(memory_space=pl.ANY)
    return pl.pallas_call(
        decoder_kernel,
        out_shape=pltpu.VMEM((1, rows, half * 3 // 4), bf16),
        in_specs=[pl.BlockSpec(memory_space=pltpu.SMEM)] * 3 + [anywhere] * 14,
        out_specs=pl.BlockSpec(memory_space=pltpu.VMEM),
        scratch_shapes=[
            pltpu.VMEM((REACH, 2, rows, part), bf16),
            pltpu.SMEM(slot_images.shape[::-1], jnp.int32),
            pltpu.SMEM(slot_count.shape, jnp.int32),
            pltpu.VMEM((5, 1, width), f32),
            pltpu.VMEM(w_qkv.shape[1:], bf16),
            pltpu.VMEM(w_self_out.shape[1:], bf16),
            pltpu.VMEM(w_query.shape[1:], bf16),
            pltpu.VMEM(w_memory.shape[1:], bf16),
            pltpu.VMEM(w_cross_out.shape[1:], bf16),
            pltpu.VMEM((2, width, half), bf16),
            pltpu.VMEM((2, devices * split, shard // split, width), bf16),
            pltpu.VMEM((rows, 3 * width), bf16),
            pltpu.VMEM((rows, 2 * width), bf16),
            pltpu.VMEM((rows, width), bf16),
            pltpu.VMEM((rows, width), bf16),
            pltpu.VMEM((slots, tall, width), f32),
            pltpu.VMEM((slots, tall, width), bf16),
            pltpu.VMEM((tall, half), f32),
            pltpu.VMEM((slots, rows, half), f32),
            pltpu.VMEM((slots, rows, half), bf16),
            pltpu.VMEM((slots, rows, half), bf16),
            pltpu.VMEM((4, 2, rows, half // 2), bf16),
            pltpu.VMEM((4, 2, rows, half // 2), bf16),
            pltpu.VMEM((2, rows, half // 2), f32),
            dma, dma((6,)), dma((REACH,)), dma((REACH,)), dma((REACH,)),
            dma((2,)), dma((2,)), dma((5,)), dma((5,)), dma((7,)), dma((7,)),
            dma((kinds,)), dma((chips, kinds)), dma((chips, kinds)), dma((chips, kinds)),
            dma((chips, kinds)), dma((slots,)), dma((slots,)), dma((4, 2)), dma((4, 2)),
        ],
        compiler_params=pltpu.CompilerParams(
            collective_id=0, has_side_effects=True, vmem_limit_bytes=VMEM_LIMIT
        ),
    )(
        image_slot, slot_images.T, slot_count, features, gain_self, gain_query, gain_memory,
        gain_mlp, gain_head, w_qkv, w_self_out, w_query, w_memory, w_cross_out, w_fc1, w_fc2,
        w_head,
    )


def solution(mesh):
    placed = (
        P("pairs", None, "side"),
        P(),
        P("pairs", None),
        P("pairs"),
        P("side", None),
        P("side", None),
        P("side", None),
        P("side", None),
        P("side", None),
        P("side", None, None),
        P("side", None, None),
        P("side", None, None),
        P("side", None, None),
        P("side", None, None),
        P("side", "pairs", None),
        P("side", "pairs", None),
        P("side", None, None),
    )
    return jax.shard_map(
        on_device, mesh=mesh, in_specs=placed, out_specs=P("pairs", None, "side"), check_vma=False
    )
```

```python
import functools

import jax
import jax.numpy as jnp
from jax import lax
from jax.experimental import pallas as pl
from jax.experimental.pallas import tpu as pltpu
from jax.sharding import PartitionSpec as P

HEAD_DIM = 64
WINDOW = 4
PAIR = 2 * HEAD_DIM
BLOCKS = 4
REACH = WINDOW + 1
VMEM_LIMIT = 63 * 1024 * 1024
MESH = pl.DeviceIdType.MESH


def padded(rows):
    return -(-rows // 16) * 16


def layer_norm(values, gain):
    center = values - jnp.mean(values, axis=-1, keepdims=True)
    spread = jnp.mean(center * center, axis=-1, keepdims=True)
    return center * lax.rsqrt(spread + 1e-06) * gain


def matmul(left, right):
    return jnp.dot(left, right, preferred_element_type=jnp.float32)


def matmul_t(left, right):
    return lax.dot_general(
        left, right, (((1,), (1,)), ((), ())), preferred_element_type=jnp.float32
    )


def attend(q_ref, k_ref, v_ref, k_at, v_at, o_ref, width, comm):
    rows = q_ref.shape[0]
    low = lax.broadcasted_iota(jnp.int32, (rows, PAIR), 1) < HEAD_DIM
    for pair in range(width // PAIR):
        if comm is not None and pair * PAIR == width // 2:
            comm()
        q = q_ref[:, pair * PAIR : (pair + 1) * PAIR]
        k = k_ref[:, k_at + pair * PAIR : k_at + (pair + 1) * PAIR]
        v = v_ref[:, v_at + pair * PAIR : v_at + (pair + 1) * PAIR]
        mixed = None
        for keep in (low, jnp.logical_not(low)):
            q_head = jnp.where(keep, q, jnp.zeros_like(q))
            v_head = jnp.where(keep, v, jnp.zeros_like(v))
            scores = matmul_t(q_head, k) * HEAD_DIM ** (-0.5)
            expon = jnp.exp(scores)
            weights = (expon / jnp.sum(expon, axis=-1, keepdims=True)).astype(jnp.bfloat16)
            part = matmul(weights, v_head)
            mixed = part if mixed is None else mixed + part
        o_ref[:, pair * PAIR : (pair + 1) * PAIR] = mixed.astype(jnp.bfloat16)


def remote(src, dst, send, recv, device):
    return pltpu.make_async_remote_copy(
        src_ref=src, dst_ref=dst, send_sem=send, recv_sem=recv, device_id=device,
        device_id_type=MESH,
    )


def decoder_kernel(
    image_slot, slot_images, slot_count, features,
    g_self, g_query, g_memory, g_mlp, g_head,
    w_qkv, w_self_out, w_query, w_memory, w_cross_out, w_fc1, w_fc2, w_head,
    out,
    win, table, counts, gains, m_qkv, m_self_out, m_query, m_memory, m_cross_out, m_head, ring_w,
    triple, kv, queries, mixed, second, hidden, raw, term, term_away, term_in, far_out, far_in,
    final,
    f_local, f_send, f_recv, fr_send, fr_recv, t_send, t_recv, g_send, g_recv, w_send, w_recv,
    s_send, r_send, r_recv, x_send, x_recv, a_send, a_recv, b_send, b_recv,
):
    devices = lax.axis_size("pairs")
    chips = devices // 2
    here = lax.axis_index("pairs")
    s = lax.axis_index("side")
    x = lax.rem(here, 2)
    q = lax.div(here, 2)
    rows = features.shape[1]
    width = m_qkv.shape[0]
    slots = second.shape[0]
    tall = second.shape[1]
    shard = w_fc1.shape[1]
    rank = ring_w.shape[2]
    split = shard // rank
    kinds = 2 * split
    total_pieces = kinds * chips

    sibling = (here, 1 - s)
    partner = (2 * q + s, x)
    at_home = x == s

    def pair_of(step, flip):
        chip = lax.rem(q + (step + chips), chips)
        return 2 * chip + (1 - x if flip else x)

    up = jnp.where(
        lax.rem(q, 2) == 0,
        jnp.where(q + 2 < chips, q + 2, chips - 1),
        jnp.where(q >= 3, q - 2, 0),
    )
    down = jnp.where(
        lax.rem(q, 2) == 0,
        jnp.where(q == 0, 1, q - 2),
        jnp.where(q + 2 < chips, q + 2, chips - 2),
    )
    onward = (2 * jnp.where(s == 0, up, down) + x, s)

    mats = (
        (w_qkv, m_qkv), (w_self_out, m_self_out), (w_memory, m_memory), (w_query, m_query),
        (w_cross_out, m_cross_out),
    )
    half = w_head.shape[2] // 2
    weights = [(src.at[0], dst) for src, dst in mats]
    weights += [(w_head.at[0, :, h * half : (h + 1) * half], m_head.at[h]) for h in range(2)]
    gain_refs = (g_self, g_query, g_memory, g_mlp, g_head)
    fcs = (w_fc1, w_fc2)

    def ring_view(step, kind, ring):
        return ring_w.at[lax.rem(kind, 2), 2 * (split * step + lax.div(kind, 2)) + ring]

    def own_fc(which, piece):
        if split == 1:
            return fcs[which].at[0]
        return fcs[which].at[0, pl.ds(pl.multiple_of(piece * rank, rank), rank)]

    own_win = pltpu.make_async_copy(features.at[0], win.at[x, s], f_local)
    own_win.start()

    @pl.when(at_home)
    def _():
        for at, ref in enumerate(gain_refs):
            pltpu.make_async_copy(ref, gains.at[at], g_recv.at[at]).start()
        for which in range(2):
            pltpu.make_async_copy(
                own_fc(which, s), ring_view(0, which, s), r_recv.at[0, which]
            ).start()
        for at, (src, dst) in enumerate(weights):
            pltpu.make_async_copy(src, dst, w_recv.at[at]).start()

    barrier = pltpu.get_barrier_semaphore()
    for step in range(-2, 3):
        for flip in range(2):
            if step or flip:
                pl.semaphore_signal(
                    barrier, inc=1, device_id=(pair_of(step, flip), s), device_id_type=MESH
                )
    pl.semaphore_signal(barrier, inc=1, device_id=sibling, device_id_type=MESH)

    @pl.when(jnp.logical_not(at_home))
    def _():
        pl.semaphore_signal(barrier, inc=1, device_id=partner, device_id_type=MESH)

    pl.semaphore_wait(barrier, 10 + (1 - at_home.astype(jnp.int32)))

    table_out = [
        remote(slot_images, table, t_send.at[0], t_recv.at[0], (pair_of(0, 1), s)),
        remote(slot_count, counts, t_send.at[1], t_recv.at[1], (pair_of(0, 1), s)),
    ]
    across = (2 * q + s, s)
    if split == 1:
        fc_home = []
        fc_out = [
            remote(own_fc(f, 0), ring_view(0, f, x), s_send.at[f], r_recv.at[0, f], partner)
            for f in range(2)
        ]
    else:
        fc_home = [
            remote(
                own_fc(f, 1 - s), ring_view(0, f, 1 - s), s_send.at[f], r_recv.at[0, f], sibling
            )
            for f in range(2)
        ]
        fc_out = [
            remote(
                own_fc(f, ring), ring_view(0, 2 + f, ring), s_send.at[2 * f + to],
                r_recv.at[0, 2 + f], device,
            )
            for f in range(2)
            for to, (ring, device) in enumerate(((x, partner), (s, across)))
        ]
    gains_out = [
        remote(ref, gains.at[at], g_send.at[at], g_recv.at[at], sibling)
        for at, ref in enumerate(gain_refs)
    ]
    weights_out = [
        remote(src, dst, w_send.at[at], w_recv.at[at], sibling)
        for at, (src, dst) in enumerate(weights)
    ]

    def feature_out(block, place, step, flip, at):
        return remote(
            block, win.at[place, s], f_send.at[at], f_recv.at[place], (pair_of(-step, flip), s)
        )

    own = features.at[0]
    passed = win.at[1 - x, s]
    even = lax.rem(q, 2) == 0
    feature_across = feature_out(own, x, 0, 1, 0)
    near_zero = [feature_out(block, 2, 1, 0, 1) for block in (own, passed)]
    near_one = [feature_out(block, 3, 1, 0, 2) for block in (passed, own)]
    far_zero = feature_out(own, WINDOW, 2, 0, 3)
    onto_next = feature_out(win.at[WINDOW, s], 2, -1, 0, 4)
    far_across = feature_out(win.at[WINDOW, s], WINDOW, 0, 1, 5)

    def relay(place, block=None):
        target = win.at[place, s]
        return remote(
            target if block is None else block, target, fr_send.at[place], fr_recv.at[place],
            sibling,
        )

    @pl.when(at_home)
    def _():
        for copy in fc_home:
            copy.start()

    for copy in table_out:
        copy.start()
    feature_across.start()

    @pl.when(x == 0)
    def _():
        far_zero.start()

        @pl.when(jnp.logical_not(even))
        def _():
            near_zero[0].start()

    @pl.when(x == 1)
    def _():
        near_one[1].start()

    relay(x, own).start()

    @pl.when(at_home)
    def _():
        for copy in gains_out:
            copy.start()
        weights_out[0].start()

    swapped = len(fc_out) // 2

    @pl.when(jnp.logical_not(at_home))
    def _():
        for copy in fc_out[:swapped]:
            copy.start()

        @pl.when(x == 1)
        def _():
            for copy in fc_out[swapped:]:
                copy.start()

    def piece(number):
        turn = lax.div(number, kinds // 2)
        last = turn == 2 * chips - 1
        ahead = jnp.logical_or(turn == 0, jnp.logical_and(lax.rem(turn, 2) == 1, turn < 2 * chips - 1))
        step = jnp.where(
            turn == 0,
            0,
            jnp.where(last, chips - 1, jnp.where(ahead, lax.div(turn + 1, 2), lax.div(turn, 2) - 1)),
        )
        kind = lax.rem(number, kinds // 2) + jnp.where(ahead, 0, kinds // 2)
        block = ring_view(step, kind, s)
        pltpu.make_async_copy(block, block, r_recv.at[step, kind]).wait()

        @pl.when(step < chips - 1)
        def _():
            remote(
                block, ring_view(step + 1, kind, s), r_send.at[step, kind],
                r_recv.at[step + 1, kind], onward,
            ).start()

        remote(block, block, x_send.at[step, kind], x_recv.at[step, kind], sibling).start()

    def pieces(low, high):
        def body(number, carry):
            piece(number)
            return carry

        lax.fori_loop(low, high, body, 0)

    def arrived(place):
        block = win.at[place, s]
        pltpu.make_async_copy(block, block, f_recv.at[place]).wait()
        relay(place).start()

    group = kinds // 2
    early = 5 * group
    pieces(0, group)
    arrived(1 - x)

    @pl.when(x == 0)
    def _():
        near_one[0].start()
        arrived(WINDOW)

        @pl.when(even)
        def _():
            onto_next.start()

        far_across.start()

        @pl.when(jnp.logical_not(at_home))
        def _():
            for copy in fc_out[swapped:]:
                copy.start()

    @pl.when(x == 1)
    def _():
        near_zero[1].start()

    @pl.when(at_home)
    def _():
        weights_out[1].start()

    pieces(group, 2 * group)
    arrived(3)

    @pl.when(x == 1)
    def _():
        arrived(WINDOW)

    pieces(2 * group, 4 * group)
    arrived(2)

    @pl.when(at_home)
    def _():
        for copy in weights_out[2:]:
            copy.start()

    pieces(4 * group, early)
    own_win.wait()
    for place in range(REACH):
        block = win.at[place, 1 - s]
        pltpu.make_async_copy(block, block, fr_recv.at[place]).wait()
    for copy in table_out:
        copy.wait_recv()
    for at, ref in enumerate(gain_refs):
        pltpu.make_async_copy(ref, gains.at[at], g_recv.at[at]).wait()

    def weight_wait(at):
        src, dst = weights[at]
        pltpu.make_async_copy(src, dst, w_recv.at[at]).wait()

    def first_wait(slot, at):
        @pl.when(slot == 0)
        def _():
            weight_wait(at)

    def entry(slot, column, core):
        local = slot_images[column, slot]
        return jnp.where(x == core, local, table[column, slot])

    def place_of(slot, column, core=None):
        core = s if core is None else core
        stored = image_slot[entry(slot, column, core)]
        ahead = lax.rem(stored - (2 * q + core) + devices, devices)
        return jnp.minimum(ahead, WINDOW - 1) + core

    def tokens_of(place):
        return jnp.concatenate([win[place, 0], win[place, 1]], axis=-1).astype(jnp.float32)

    stops = 4 * slots
    each = max((total_pieces * 26 // 32 - early) // stops, 0)
    fronted = early + each * stops

    def front(slot, carry):
        told = [0]

        def comm():
            base = early + (4 * slot + told[0]) * each
            told[0] += 1
            for at in range(each):
                piece(base + at)

        first_wait(slot, 0)
        tokens = tokens_of(place_of(slot, x))
        state = layer_norm(tokens, gains[0]).astype(jnp.bfloat16)
        triple[...] = matmul(state, m_qkv[...]).astype(jnp.bfloat16)
        comm()
        attend(triple, triple, triple, width, 2 * width, mixed, width, None)
        first_wait(slot, 1)
        first = tokens + matmul(mixed[...], m_self_out[...])
        second[slot, 0:rows, :] = first
        comm()
        first_wait(slot, 2)
        first_wait(slot, 3)
        query_in = layer_norm(first, gains[1]).astype(jnp.bfloat16)
        memory = tokens_of(place_of(slot, 1 - x))
        memory_in = layer_norm(memory, gains[2]).astype(jnp.bfloat16)
        queries[...] = matmul(query_in, m_query[...]).astype(jnp.bfloat16)
        kv[...] = matmul(memory_in, m_memory[...]).astype(jnp.bfloat16)
        attend(queries, kv, kv, 0, width, mixed, width, comm)
        first_wait(slot, 4)
        result = second[slot, 0:rows, :] + matmul(mixed[...], m_cross_out[...])
        second[slot, 0:rows, :] = result
        hidden[slot, 0:rows, :] = layer_norm(result, gains[3]).astype(jnp.bfloat16)
        comm()
        return carry

    second[...] = jnp.zeros_like(second)
    hidden[...] = jnp.zeros_like(hidden)
    lax.fori_loop(0, slots, front, 0)

    def relayed(first, count):
        def body(at, carry):
            turn, which = first + lax.div(at, 2), lax.rem(at, 2)
            step, kind = lax.div(turn, split), 2 * lax.rem(turn, split) + which
            view = ring_view(step, kind, 1 - s)
            pltpu.make_async_copy(view, view, x_recv.at[step, kind]).wait()
            return carry

        lax.fori_loop(0, 2 * count, body, 0)

    def expand(first, turns, slot):
        count = 2 * turns
        if rank % 16 == 0:
            groups = [
                [ring_w[f, pl.ds(2 * first, count)].reshape(count * rank, width) for f in range(2)]
            ]
        else:
            groups = [[ring_w[f, 2 * first + at] for f in range(2)] for at in range(count)]
        total = second[slot]
        for fc1, fc2 in groups:
            pre = matmul_t(hidden[slot], fc1)
            act = (pre * (1.0 + lax.erf(pre * 0.5**0.5)) * 0.5).astype(jnp.bfloat16)
            total = total + matmul(act, fc2)
        second[slot] = total

    turns = split * chips
    span = turns // BLOCKS
    whole = total_pieces - group
    left = whole - fronted
    places = (BLOCKS - 1) * slots
    pace = BLOCKS * slots

    def expand_early(turn, carry):
        block, slot = lax.div(turn, slots), lax.rem(turn, slots)

        @pl.when(slot == 0)
        def _():
            relayed(block * span, span)

        expand(block * span, span, slot)
        pieces(
            fronted + lax.div(turn * left, pace), fronted + lax.div((turn + 1) * left, pace)
        )
        return carry

    lax.fori_loop(0, places, expand_early, 0)
    pieces(fronted + places * left // pace, whole)
    relayed((BLOCKS - 1) * span, span - 1)

    early_rate = -(-group // (slots - 1))

    def expand_late(slot, carry):
        expand((BLOCKS - 1) * span, span - 1, slot)
        pieces(
            whole + jnp.minimum(slot * early_rate, group),
            whole + jnp.minimum((slot + 1) * early_rate, group),
        )
        return carry

    lax.fori_loop(0, slots, expand_late, 0)
    weight_wait(5)
    weight_wait(6)
    relayed(turns - 1, 1)
    pix = half // 4

    def terms(slot, which, target):
        raw[...] = matmul(hidden[slot], m_head[which])
        conf = 1.0 + jnp.exp(raw[0:rows, 3 * pix :])
        for comp in range(4):
            at = slice(comp * pix, (comp + 1) * pix)
            value = conf if comp == 3 else conf * raw[0:rows, at]
            target[slot, :, at] = value.astype(target.dtype)

    def away(slot):
        return remote(
            term_away.at[slot], term_in.at[slot], a_send.at[slot], a_recv.at[slot], sibling
        )

    def expand_last(slot, carry):
        hidden[slot] = layer_norm(second[slot], gains[4]).astype(jnp.bfloat16)
        terms(slot, 1 - s, term_away)
        away(slot).start()
        return carry

    def own_terms(slot, carry):
        terms(slot, s, term)
        return carry

    joined = hidden[...].reshape(slots * tall, width)
    for unit in range(2 * (turns - 1), 2 * turns) if rank % 16 else (None,):
        units = pl.ds(2 * (turns - 1), 2) if unit is None else pl.ds(unit, 1)
        fc1, fc2 = [ring_w[f, units].reshape(-1, width) for f in range(2)]
        pre = matmul_t(joined, fc1)
        act = (pre * (1.0 + lax.erf(pre * 0.5**0.5)) * 0.5).astype(jnp.bfloat16)
        second[...] = second[...] + matmul(act, fc2).reshape(slots, tall, width)
    for slot in range(slots):
        expand_last(slot, 0)
    for slot in range(slots):
        own_terms(slot, 0)
    for slot in range(slots):
        away(slot).wait_recv()

    sources = []
    for core, ref in ((s, term), (1 - s, term_in)):
        live = jnp.where(x == core, slot_count[0], counts[0])
        for slot in range(slots):
            sources.append((place_of(slot, x, core), slot < live, ref, slot))

    quarter = half // 2

    def sums_of(place, part):
        sums = jnp.zeros((rows, quarter), jnp.float32)
        for to, live, ref, slot in sources:
            chosen = jnp.logical_and(to == place, live)
            value = ref[slot, :, part * quarter : (part + 1) * quarter].astype(jnp.float32)
            sums = sums + jnp.where(chosen, value, 0.0)
        return sums

    def far_copy(at, part, step, flip):
        return remote(
            far_out.at[at, part], far_in.at[at, part], b_send.at[at, part], b_recv.at[at, part],
            (pair_of(step, flip), s),
        )

    def far_send(at, part, step, flip, sums):
        far_out[at, part] = sums.astype(jnp.bfloat16)
        far_copy(at, part, step, flip).start()

    def far_wait(at, part):
        block = far_in.at[at, part]
        pltpu.make_async_copy(block, block, b_recv.at[at, part]).wait()
        return block[...].astype(jnp.float32)

    for part in range(2):
        far_send(1, part, 0, 1, sums_of(3 - x, part))
    for part in range(2):
        far_send(0, part, 2, 0, sums_of(WINDOW, part))

    @pl.when(x == 0)
    def _():
        for part in range(2):
            far_send(3, part, 0, 1, sums_of(1, part))

    for copy in (feature_across, near_one[0]):
        copy.wait_send()

    @pl.when(x == 0)
    def _():
        far_zero.wait_send()
        far_across.wait_send()

        @pl.when(even)
        def _():
            onto_next.wait_send()

    @pl.when(jnp.logical_or(x == 1, jnp.logical_not(even)))
    def _():
        near_zero[0].wait_send()

    for place in range(REACH):
        relay(place).wait_send()

    @pl.when(at_home)
    def _():
        for copy in fc_home + gains_out + weights_out:
            copy.wait_send()

    @pl.when(jnp.logical_not(at_home))
    def _():
        for copy in fc_out:
            copy.wait_send()

    for copy in table_out:
        copy.wait_send()

    def drain(number, carry):
        step, kind = lax.div(number, kinds), lax.rem(number, kinds)
        block = ring_view(step, kind, s)

        @pl.when(step < chips - 1)
        def _():
            remote(
                block, block, r_send.at[step, kind], r_recv.at[step, kind], onward
            ).wait_send()

        remote(block, block, x_send.at[step, kind], x_recv.at[step, kind], sibling).wait_send()
        return carry

    lax.fori_loop(0, total_pieces, drain, 0)
    for part in range(2):
        final[part] = sums_of(2 + x, part)
    for part in range(2):
        far_send(2, part, 1, 0, final[part] + far_wait(1, part))
    for part in range(2):
        final[part] = sums_of(x, part)

    @pl.when(x == 1)
    def _():
        for part in range(2):
            far_send(3, part, 0, 1, sums_of(0, part) + far_wait(0, part))

    @pl.when(x == 0)
    def _():
        for part in range(2):
            final[part] = final[part] + far_wait(0, part)

    for part in range(2):
        final[part] = final[part] + far_wait(2, part)
    for part in range(2):
        final[part] = final[part] + far_wait(3, part)
    conf = jnp.maximum(final[1, :, pix:], 1.0)
    for comp in range(3):
        value = final[comp // 2, :, comp % 2 * pix : (comp % 2 + 1) * pix]
        out[0, :, comp * pix : (comp + 1) * pix] = (value / conf).astype(jnp.bfloat16)

    for slot in range(slots):
        away(slot).wait_send()
    for at, (step, flip) in enumerate(((2, 0), (0, 1), (1, 0), (0, 1))):
        for part in range(2):
            far_copy(at, part, step, flip).wait_send()


def on_device(
    features, image_slot, slot_images, slot_count, gain_self, gain_query, gain_memory, gain_mlp,
    gain_head, w_qkv, w_self_out, w_query, w_memory, w_cross_out, w_fc1, w_fc2, w_head,
):
    devices = lax.axis_size("pairs")
    chips = devices // 2
    blocks, rows, part = features.shape
    if blocks != 1 or chips % BLOCKS:
        raise ValueError("unsupported split")
    width = w_qkv.shape[1]
    slots = slot_images.shape[0]
    tall = padded(rows)
    shard = w_fc1.shape[1]
    split = 2 if shard % 32 == 0 else 1
    kinds = 2 * split
    half = w_head.shape[2] // 2
    bf16, f32 = jnp.bfloat16, jnp.float32
    dma = pltpu.SemaphoreType.DMA
    anywhere = pl.BlockSpec(memory_space=pl.ANY)
    return pl.pallas_call(
        decoder_kernel,
        out_shape=pltpu.VMEM((1, rows, half * 3 // 4), bf16),
        in_specs=[pl.BlockSpec(memory_space=pltpu.SMEM)] * 3 + [anywhere] * 14,
        out_specs=pl.BlockSpec(memory_space=pltpu.VMEM),
        scratch_shapes=[
            pltpu.VMEM((REACH, 2, rows, part), bf16),
            pltpu.SMEM(slot_images.shape[::-1], jnp.int32),
            pltpu.SMEM(slot_count.shape, jnp.int32),
            pltpu.VMEM((5, 1, width), f32),
            pltpu.VMEM(w_qkv.shape[1:], bf16),
            pltpu.VMEM(w_self_out.shape[1:], bf16),
            pltpu.VMEM(w_query.shape[1:], bf16),
            pltpu.VMEM(w_memory.shape[1:], bf16),
            pltpu.VMEM(w_cross_out.shape[1:], bf16),
            pltpu.VMEM((2, width, half), bf16),
            pltpu.VMEM((2, devices * split, shard // split, width), bf16),
            pltpu.VMEM((rows, 3 * width), bf16),
            pltpu.VMEM((rows, 2 * width), bf16),
            pltpu.VMEM((rows, width), bf16),
            pltpu.VMEM((rows, width), bf16),
            pltpu.VMEM((slots, tall, width), f32),
            pltpu.VMEM((slots, tall, width), bf16),
            pltpu.VMEM((tall, half), f32),
            pltpu.VMEM((slots, rows, half), f32),
            pltpu.VMEM((slots, rows, half), bf16),
            pltpu.VMEM((slots, rows, half), bf16),
            pltpu.VMEM((4, 2, rows, half // 2), bf16),
            pltpu.VMEM((4, 2, rows, half // 2), bf16),
            pltpu.VMEM((2, rows, half // 2), f32),
            dma, dma((6,)), dma((REACH,)), dma((REACH,)), dma((REACH,)),
            dma((2,)), dma((2,)), dma((5,)), dma((5,)), dma((7,)), dma((7,)),
            dma((kinds,)), dma((chips, kinds)), dma((chips, kinds)), dma((chips, kinds)),
            dma((chips, kinds)), dma((slots,)), dma((slots,)), dma((4, 2)), dma((4, 2)),
        ],
        compiler_params=pltpu.CompilerParams(
            collective_id=0, has_side_effects=True, vmem_limit_bytes=VMEM_LIMIT
        ),
    )(
        image_slot, slot_images.T, slot_count, features, gain_self, gain_query, gain_memory,
        gain_mlp, gain_head, w_qkv, w_self_out, w_query, w_memory, w_cross_out, w_fc1, w_fc2,
        w_head,
    )


def solution(mesh):
    placed = (
        P("pairs", None, "side"),
        P(),
        P("pairs", None),
        P("pairs"),
        P("side", None),
        P("side", None),
        P("side", None),
        P("side", None),
        P("side", None),
        P("side", None, None),
        P("side", None, None),
        P("side", None, None),
        P("side", None, None),
        P("side", None, None),
        P("side", "pairs", None),
        P("side", "pairs", None),
        P("side", None, None),
    )
    return jax.shard_map(
        on_device, mesh=mesh, in_specs=placed, out_specs=P("pairs", None, "side"), check_vma=False
    )
```

```python
import functools

import jax
import jax.numpy as jnp
from jax import lax
from jax.experimental import pallas as pl
from jax.experimental.pallas import tpu as pltpu
from jax.sharding import PartitionSpec as P

HEAD_DIM = 64
WINDOW = 4
PAIR = 2 * HEAD_DIM
BLOCKS = 4
REACH = WINDOW + 1
VMEM_LIMIT = 63 * 1024 * 1024
MESH = pl.DeviceIdType.MESH


def padded(rows):
    return -(-rows // 16) * 16


def layer_norm(values, gain):
    center = values - jnp.mean(values, axis=-1, keepdims=True)
    spread = jnp.mean(center * center, axis=-1, keepdims=True)
    return center * lax.rsqrt(spread + 1e-06) * gain


def matmul(left, right):
    return jnp.dot(left, right, preferred_element_type=jnp.float32)


def matmul_t(left, right):
    return lax.dot_general(
        left, right, (((1,), (1,)), ((), ())), preferred_element_type=jnp.float32
    )


def attend(q_ref, k_ref, v_ref, k_at, v_at, o_ref, width, comm):
    rows = q_ref.shape[0]
    low = lax.broadcasted_iota(jnp.int32, (rows, PAIR), 1) < HEAD_DIM
    for pair in range(width // PAIR):
        if comm is not None and pair * PAIR == width // 2:
            comm()
        q = q_ref[:, pair * PAIR : (pair + 1) * PAIR]
        k = k_ref[:, k_at + pair * PAIR : k_at + (pair + 1) * PAIR]
        v = v_ref[:, v_at + pair * PAIR : v_at + (pair + 1) * PAIR]
        mixed = None
        for keep in (low, jnp.logical_not(low)):
            q_head = jnp.where(keep, q, jnp.zeros_like(q))
            v_head = jnp.where(keep, v, jnp.zeros_like(v))
            scores = matmul_t(q_head, k) * HEAD_DIM ** (-0.5)
            expon = jnp.exp(scores)
            weights = (expon / jnp.sum(expon, axis=-1, keepdims=True)).astype(jnp.bfloat16)
            part = matmul(weights, v_head)
            mixed = part if mixed is None else mixed + part
        o_ref[:, pair * PAIR : (pair + 1) * PAIR] = mixed.astype(jnp.bfloat16)


def remote(src, dst, send, recv, device):
    return pltpu.make_async_remote_copy(
        src_ref=src, dst_ref=dst, send_sem=send, recv_sem=recv, device_id=device,
        device_id_type=MESH,
    )


def decoder_kernel(
    image_slot, slot_images, slot_count, features,
    g_self, g_query, g_memory, g_mlp, g_head,
    w_qkv, w_self_out, w_query, w_memory, w_cross_out, w_fc1, w_fc2, w_head,
    out,
    win, table, counts, gains, m_qkv, m_self_out, m_query, m_memory, m_cross_out, m_head, ring_w,
    triple, kv, queries, mixed, second, hidden, raw, term, term_away, term_in, far_out, far_in,
    final,
    f_local, f_send, f_recv, fr_send, fr_recv, t_send, t_recv, g_send, g_recv, w_send, w_recv,
    s_send, r_send, r_recv, x_send, x_recv, a_send, a_recv, b_send, b_recv,
):
    devices = lax.axis_size("pairs")
    chips = devices // 2
    here = lax.axis_index("pairs")
    s = lax.axis_index("side")
    x = lax.rem(here, 2)
    q = lax.div(here, 2)
    rows = features.shape[1]
    width = m_qkv.shape[0]
    slots = second.shape[0]
    tall = second.shape[1]
    shard = w_fc1.shape[1]
    rank = ring_w.shape[2]
    split = shard // rank
    kinds = 2 * split
    total_pieces = kinds * chips

    sibling = (here, 1 - s)
    partner = (2 * q + s, x)
    at_home = x == s

    def pair_of(step, flip):
        chip = lax.rem(q + (step + chips), chips)
        return 2 * chip + (1 - x if flip else x)

    up = jnp.where(
        lax.rem(q, 2) == 0,
        jnp.where(q + 2 < chips, q + 2, chips - 1),
        jnp.where(q >= 3, q - 2, 0),
    )
    down = jnp.where(
        lax.rem(q, 2) == 0,
        jnp.where(q == 0, 1, q - 2),
        jnp.where(q + 2 < chips, q + 2, chips - 2),
    )
    onward = (2 * jnp.where(s == 0, up, down) + x, s)

    mats = (
        (w_qkv, m_qkv), (w_self_out, m_self_out), (w_memory, m_memory), (w_query, m_query),
        (w_cross_out, m_cross_out),
    )
    half = w_head.shape[2] // 2
    weights = [(src.at[0], dst) for src, dst in mats]
    weights += [(w_head.at[0, :, h * half : (h + 1) * half], m_head.at[h]) for h in range(2)]
    gain_refs = (g_self, g_query, g_memory, g_mlp, g_head)
    fcs = (w_fc1, w_fc2)

    def ring_view(step, kind, ring):
        return ring_w.at[lax.rem(kind, 2), 2 * (split * step + lax.div(kind, 2)) + ring]

    def own_fc(which, piece):
        if split == 1:
            return fcs[which].at[0]
        return fcs[which].at[0, pl.ds(pl.multiple_of(piece * rank, rank), rank)]

    own_win = pltpu.make_async_copy(features.at[0], win.at[x, s], f_local)
    own_win.start()

    @pl.when(at_home)
    def _():
        for at, ref in enumerate(gain_refs):
            pltpu.make_async_copy(ref, gains.at[at], g_recv.at[at]).start()
        for which in range(2):
            pltpu.make_async_copy(
                own_fc(which, s), ring_view(0, which, s), r_recv.at[0, which]
            ).start()
        for at, (src, dst) in enumerate(weights):
            pltpu.make_async_copy(src, dst, w_recv.at[at]).start()

    barrier = pltpu.get_barrier_semaphore()
    for step in range(-2, 3):
        for flip in range(2):
            if (step == 0) == (flip == 1):
                pl.semaphore_signal(
                    barrier, inc=1, device_id=(pair_of(step, flip), s), device_id_type=MESH
                )
    pl.semaphore_signal(barrier, inc=1, device_id=sibling, device_id_type=MESH)

    @pl.when(jnp.logical_not(at_home))
    def _():
        pl.semaphore_signal(barrier, inc=1, device_id=partner, device_id_type=MESH)

    pl.semaphore_wait(barrier, 6 + (1 - at_home.astype(jnp.int32)))

    table_out = [
        remote(slot_images, table, t_send.at[0], t_recv.at[0], (pair_of(0, 1), s)),
        remote(slot_count, counts, t_send.at[1], t_recv.at[1], (pair_of(0, 1), s)),
    ]
    across = (2 * q + s, s)
    if split == 1:
        fc_home = []
        fc_out = [
            remote(own_fc(f, 0), ring_view(0, f, x), s_send.at[f], r_recv.at[0, f], partner)
            for f in range(2)
        ]
    else:
        fc_home = [
            remote(
                own_fc(f, 1 - s), ring_view(0, f, 1 - s), s_send.at[f], r_recv.at[0, f], sibling
            )
            for f in range(2)
        ]
        fc_out = [
            remote(
                own_fc(f, ring), ring_view(0, 2 + f, ring), s_send.at[2 * f + to],
                r_recv.at[0, 2 + f], device,
            )
            for f in range(2)
            for to, (ring, device) in enumerate(((x, partner), (s, across)))
        ]
    gains_out = [
        remote(ref, gains.at[at], g_send.at[at], g_recv.at[at], sibling)
        for at, ref in enumerate(gain_refs)
    ]
    weights_out = [
        remote(src, dst, w_send.at[at], w_recv.at[at], sibling)
        for at, (src, dst) in enumerate(weights)
    ]

    def feature_out(block, place, step, flip, at):
        return remote(
            block, win.at[place, s], f_send.at[at], f_recv.at[place], (pair_of(-step, flip), s)
        )

    own = features.at[0]
    passed = win.at[1 - x, s]
    even = lax.rem(q, 2) == 0
    feature_across = feature_out(own, x, 0, 1, 0)
    near_zero = [feature_out(block, 2, 1, 0, 1) for block in (own, passed)]
    near_one = [feature_out(block, 3, 1, 0, 2) for block in (passed, own)]
    far_zero = feature_out(own, WINDOW, 2, 0, 3)
    onto_next = feature_out(win.at[WINDOW, s], 2, -1, 0, 4)
    far_across = feature_out(win.at[WINDOW, s], WINDOW, 0, 1, 5)

    def relay(place, block=None):
        target = win.at[place, s]
        return remote(
            target if block is None else block, target, fr_send.at[place], fr_recv.at[place],
            sibling,
        )

    @pl.when(at_home)
    def _():
        for copy in fc_home:
            copy.start()

    for copy in table_out:
        copy.start()
    feature_across.start()

    @pl.when(x == 0)
    def _():
        far_zero.start()

        @pl.when(jnp.logical_not(even))
        def _():
            near_zero[0].start()

    @pl.when(x == 1)
    def _():
        near_one[1].start()

    def wanted(place):
        return jnp.logical_and(place >= 1 - s, place <= WINDOW - s)

    @pl.when(wanted(x))
    def _():
        relay(x, own).start()

    @pl.when(at_home)
    def _():
        for copy in gains_out:
            copy.start()
        weights_out[0].start()

    swapped = len(fc_out) // 2

    @pl.when(jnp.logical_not(at_home))
    def _():
        for copy in fc_out[:swapped]:
            copy.start()

        @pl.when(x == 1)
        def _():
            for copy in fc_out[swapped:]:
                copy.start()

    def piece(number):
        turn = lax.div(number, kinds // 2)
        last = turn == 2 * chips - 1
        ahead = jnp.logical_or(turn == 0, jnp.logical_and(lax.rem(turn, 2) == 1, turn < 2 * chips - 1))
        step = jnp.where(
            turn == 0,
            0,
            jnp.where(last, chips - 1, jnp.where(ahead, lax.div(turn + 1, 2), lax.div(turn, 2) - 1)),
        )
        kind = lax.rem(number, kinds // 2) + jnp.where(ahead, 0, kinds // 2)
        block = ring_view(step, kind, s)
        pltpu.make_async_copy(block, block, r_recv.at[step, kind]).wait()

        @pl.when(step < chips - 1)
        def _():
            remote(
                block, ring_view(step + 1, kind, s), r_send.at[step, kind],
                r_recv.at[step + 1, kind], onward,
            ).start()

        remote(block, block, x_send.at[step, kind], x_recv.at[step, kind], sibling).start()

    def pieces(low, high):
        def body(number, carry):
            piece(number)
            return carry

        lax.fori_loop(low, high, body, 0)

    def arrived(place):
        block = win.at[place, s]
        pltpu.make_async_copy(block, block, f_recv.at[place]).wait()

        @pl.when(wanted(place))
        def _():
            relay(place).start()

    group = kinds // 2
    early = 5 * group
    pieces(0, group)
    arrived(1 - x)

    @pl.when(x == 0)
    def _():
        near_one[0].start()
        arrived(WINDOW)

        @pl.when(even)
        def _():
            onto_next.start()

        far_across.start()

        @pl.when(jnp.logical_not(at_home))
        def _():
            for copy in fc_out[swapped:]:
                copy.start()

    @pl.when(x == 1)
    def _():
        near_zero[1].start()

    @pl.when(at_home)
    def _():
        weights_out[1].start()

    pieces(group, 2 * group)
    arrived(3)

    @pl.when(x == 1)
    def _():
        arrived(WINDOW)

    pieces(2 * group, 4 * group)
    arrived(2)

    @pl.when(at_home)
    def _():
        for copy in weights_out[2:]:
            copy.start()

    pieces(4 * group, early)
    own_win.wait()
    for place in [s + ahead for ahead in range(WINDOW)]:
        block = win.at[place, 1 - s]
        pltpu.make_async_copy(block, block, fr_recv.at[place]).wait()
    for copy in table_out:
        copy.wait_recv()
    for at, ref in enumerate(gain_refs):
        pltpu.make_async_copy(ref, gains.at[at], g_recv.at[at]).wait()

    def weight_wait(at):
        src, dst = weights[at]
        pltpu.make_async_copy(src, dst, w_recv.at[at]).wait()

    def first_wait(slot, at):
        @pl.when(slot == 0)
        def _():
            weight_wait(at)

    def entry(slot, column, core):
        local = slot_images[column, slot]
        return jnp.where(x == core, local, table[column, slot])

    def place_of(slot, column, core=None):
        core = s if core is None else core
        stored = image_slot[entry(slot, column, core)]
        ahead = lax.rem(stored - (2 * q + core) + devices, devices)
        return jnp.minimum(ahead, WINDOW - 1) + core

    def tokens_of(place):
        return jnp.concatenate([win[place, 0], win[place, 1]], axis=-1).astype(jnp.float32)

    stops = 4 * slots
    each = max((total_pieces * 26 // 32 - early) // stops, 0)
    fronted = early + each * stops

    def front(slot, carry):
        told = [0]

        def comm():
            base = early + (4 * slot + told[0]) * each
            told[0] += 1
            for at in range(each):
                piece(base + at)

        first_wait(slot, 0)
        tokens = tokens_of(place_of(slot, x))
        state = layer_norm(tokens, gains[0]).astype(jnp.bfloat16)
        triple[...] = matmul(state, m_qkv[...]).astype(jnp.bfloat16)
        comm()
        attend(triple, triple, triple, width, 2 * width, mixed, width, None)
        first_wait(slot, 1)
        first = tokens + matmul(mixed[...], m_self_out[...])
        second[slot, 0:rows, :] = first
        comm()
        first_wait(slot, 2)
        first_wait(slot, 3)
        query_in = layer_norm(first, gains[1]).astype(jnp.bfloat16)
        memory = tokens_of(place_of(slot, 1 - x))
        memory_in = layer_norm(memory, gains[2]).astype(jnp.bfloat16)
        queries[...] = matmul(query_in, m_query[...]).astype(jnp.bfloat16)
        kv[...] = matmul(memory_in, m_memory[...]).astype(jnp.bfloat16)
        attend(queries, kv, kv, 0, width, mixed, width, comm)
        first_wait(slot, 4)
        result = second[slot, 0:rows, :] + matmul(mixed[...], m_cross_out[...])
        second[slot, 0:rows, :] = result
        hidden[slot, 0:rows, :] = layer_norm(result, gains[3]).astype(jnp.bfloat16)
        comm()
        return carry

    second[...] = jnp.zeros_like(second)
    hidden[...] = jnp.zeros_like(hidden)
    lax.fori_loop(0, slots, front, 0)

    def relayed(first, count):
        def body(at, carry):
            turn, which = first + lax.div(at, 2), lax.rem(at, 2)
            step, kind = lax.div(turn, split), 2 * lax.rem(turn, split) + which
            view = ring_view(step, kind, 1 - s)
            pltpu.make_async_copy(view, view, x_recv.at[step, kind]).wait()
            return carry

        lax.fori_loop(0, 2 * count, body, 0)

    def expand(first, turns, slot):
        count = 2 * turns
        if rank % 16 == 0:
            groups = [
                [ring_w[f, pl.ds(2 * first, count)].reshape(count * rank, width) for f in range(2)]
            ]
        else:
            groups = [[ring_w[f, 2 * first + at] for f in range(2)] for at in range(count)]
        total = second[slot]
        for fc1, fc2 in groups:
            pre = matmul_t(hidden[slot], fc1)
            act = (pre * (1.0 + lax.erf(pre * 0.5**0.5)) * 0.5).astype(jnp.bfloat16)
            total = total + matmul(act, fc2)
        second[slot] = total

    turns = split * chips
    span = turns // BLOCKS
    whole = total_pieces - group
    left = whole - fronted
    places = (BLOCKS - 1) * slots
    pace = BLOCKS * slots

    def expand_early(turn, carry):
        block, slot = lax.div(turn, slots), lax.rem(turn, slots)

        @pl.when(slot == 0)
        def _():
            relayed(block * span, span)

        expand(block * span, span, slot)
        pieces(
            fronted + lax.div(turn * left, pace), fronted + lax.div((turn + 1) * left, pace)
        )
        return carry

    lax.fori_loop(0, places, expand_early, 0)
    pieces(fronted + places * left // pace, whole)
    relayed((BLOCKS - 1) * span, span - 1)

    early_rate = -(-group // (slots - 1))

    def expand_late(slot, carry):
        expand((BLOCKS - 1) * span, span - 1, slot)
        pieces(
            whole + jnp.minimum(slot * early_rate, group),
            whole + jnp.minimum((slot + 1) * early_rate, group),
        )
        return carry

    lax.fori_loop(0, slots, expand_late, 0)
    weight_wait(5)
    weight_wait(6)
    relayed(turns - 1, 1)
    pix = half // 4

    def terms(slot, which, target):
        raw[...] = matmul(hidden[slot], m_head[which])
        conf = 1.0 + jnp.exp(raw[0:rows, 3 * pix :])
        for comp in range(4):
            at = slice(comp * pix, (comp + 1) * pix)
            value = conf if comp == 3 else conf * raw[0:rows, at]
            target[slot, :, at] = value.astype(target.dtype)

    def away(slot):
        return remote(
            term_away.at[slot], term_in.at[slot], a_send.at[slot], a_recv.at[slot], sibling
        )

    def expand_last(slot, carry):
        hidden[slot] = layer_norm(second[slot], gains[4]).astype(jnp.bfloat16)
        terms(slot, 1 - s, term_away)
        away(slot).start()
        return carry

    def own_terms(slot, carry):
        terms(slot, s, term)
        return carry

    joined = hidden[...].reshape(slots * tall, width)
    for unit in range(2 * (turns - 1), 2 * turns) if rank % 16 else (None,):
        units = pl.ds(2 * (turns - 1), 2) if unit is None else pl.ds(unit, 1)
        fc1, fc2 = [ring_w[f, units].reshape(-1, width) for f in range(2)]
        pre = matmul_t(joined, fc1)
        act = (pre * (1.0 + lax.erf(pre * 0.5**0.5)) * 0.5).astype(jnp.bfloat16)
        second[...] = second[...] + matmul(act, fc2).reshape(slots, tall, width)
    for slot in range(slots):
        expand_last(slot, 0)
    for slot in range(slots):
        own_terms(slot, 0)
    for slot in range(slots):
        away(slot).wait_recv()

    sources = []
    for core, ref in ((s, term), (1 - s, term_in)):
        live = jnp.where(x == core, slot_count[0], counts[0])
        for slot in range(slots):
            sources.append((place_of(slot, x, core), slot < live, ref, slot))

    quarter = half // 2

    def sums_of(place, part):
        sums = jnp.zeros((rows, quarter), jnp.float32)
        for to, live, ref, slot in sources:
            chosen = jnp.logical_and(to == place, live)
            value = ref[slot, :, part * quarter : (part + 1) * quarter].astype(jnp.float32)
            sums = sums + jnp.where(chosen, value, 0.0)
        return sums

    def far_copy(at, part, step, flip):
        return remote(
            far_out.at[at, part], far_in.at[at, part], b_send.at[at, part], b_recv.at[at, part],
            (pair_of(step, flip), s),
        )

    def far_send(at, part, step, flip, sums):
        far_out[at, part] = sums.astype(jnp.bfloat16)
        far_copy(at, part, step, flip).start()

    def far_wait(at, part):
        block = far_in.at[at, part]
        pltpu.make_async_copy(block, block, b_recv.at[at, part]).wait()
        return block[...].astype(jnp.float32)

    for part in range(2):
        far_send(1, part, 0, 1, sums_of(3 - x, part))
    for part in range(2):
        far_send(0, part, 2, 0, sums_of(WINDOW, part))

    @pl.when(x == 0)
    def _():
        for part in range(2):
            far_send(3, part, 0, 1, sums_of(1, part))

    for copy in (feature_across, near_one[0]):
        copy.wait_send()

    @pl.when(x == 0)
    def _():
        far_zero.wait_send()
        far_across.wait_send()

        @pl.when(even)
        def _():
            onto_next.wait_send()

    @pl.when(jnp.logical_or(x == 1, jnp.logical_not(even)))
    def _():
        near_zero[0].wait_send()

    for place in [1 - s + ahead for ahead in range(WINDOW)]:
        relay(place).wait_send()

    @pl.when(at_home)
    def _():
        for copy in fc_home + gains_out + weights_out:
            copy.wait_send()

    @pl.when(jnp.logical_not(at_home))
    def _():
        for copy in fc_out:
            copy.wait_send()

    for copy in table_out:
        copy.wait_send()

    def drain(number, carry):
        step, kind = lax.div(number, kinds), lax.rem(number, kinds)
        block = ring_view(step, kind, s)

        @pl.when(step < chips - 1)
        def _():
            remote(
                block, block, r_send.at[step, kind], r_recv.at[step, kind], onward
            ).wait_send()

        remote(block, block, x_send.at[step, kind], x_recv.at[step, kind], sibling).wait_send()
        return carry

    lax.fori_loop(0, total_pieces, drain, 0)
    for part in range(2):
        final[part] = sums_of(2 + x, part)
    for part in range(2):
        far_send(2, part, 1, 0, final[part] + far_wait(1, part))
    for part in range(2):
        final[part] = sums_of(x, part)

    @pl.when(x == 1)
    def _():
        for part in range(2):
            far_send(3, part, 0, 1, sums_of(0, part) + far_wait(0, part))

    @pl.when(x == 0)
    def _():
        for part in range(2):
            final[part] = final[part] + far_wait(0, part)

    for part in range(2):
        final[part] = final[part] + far_wait(2, part)
    for part in range(2):
        final[part] = final[part] + far_wait(3, part)
    conf = jnp.maximum(final[1, :, pix:], 1.0)
    for comp in range(3):
        value = final[comp // 2, :, comp % 2 * pix : (comp % 2 + 1) * pix]
        out[0, :, comp * pix : (comp + 1) * pix] = (value / conf).astype(jnp.bfloat16)

    for slot in range(slots):
        away(slot).wait_send()
    for at, (step, flip) in enumerate(((2, 0), (0, 1), (1, 0), (0, 1))):
        for part in range(2):
            far_copy(at, part, step, flip).wait_send()


def on_device(
    features, image_slot, slot_images, slot_count, gain_self, gain_query, gain_memory, gain_mlp,
    gain_head, w_qkv, w_self_out, w_query, w_memory, w_cross_out, w_fc1, w_fc2, w_head,
):
    devices = lax.axis_size("pairs")
    chips = devices // 2
    blocks, rows, part = features.shape
    if blocks != 1 or chips % BLOCKS:
        raise ValueError("unsupported split")
    width = w_qkv.shape[1]
    slots = slot_images.shape[0]
    tall = padded(rows)
    shard = w_fc1.shape[1]
    split = 2 if shard % 32 == 0 else 1
    kinds = 2 * split
    half = w_head.shape[2] // 2
    bf16, f32 = jnp.bfloat16, jnp.float32
    dma = pltpu.SemaphoreType.DMA
    anywhere = pl.BlockSpec(memory_space=pl.ANY)
    return pl.pallas_call(
        decoder_kernel,
        out_shape=pltpu.VMEM((1, rows, half * 3 // 4), bf16),
        in_specs=[pl.BlockSpec(memory_space=pltpu.SMEM)] * 3 + [anywhere] * 14,
        out_specs=pl.BlockSpec(memory_space=pltpu.VMEM),
        scratch_shapes=[
            pltpu.VMEM((REACH, 2, rows, part), bf16),
            pltpu.SMEM(slot_images.shape[::-1], jnp.int32),
            pltpu.SMEM(slot_count.shape, jnp.int32),
            pltpu.VMEM((5, 1, width), f32),
            pltpu.VMEM(w_qkv.shape[1:], bf16),
            pltpu.VMEM(w_self_out.shape[1:], bf16),
            pltpu.VMEM(w_query.shape[1:], bf16),
            pltpu.VMEM(w_memory.shape[1:], bf16),
            pltpu.VMEM(w_cross_out.shape[1:], bf16),
            pltpu.VMEM((2, width, half), bf16),
            pltpu.VMEM((2, devices * split, shard // split, width), bf16),
            pltpu.VMEM((rows, 3 * width), bf16),
            pltpu.VMEM((rows, 2 * width), bf16),
            pltpu.VMEM((rows, width), bf16),
            pltpu.VMEM((rows, width), bf16),
            pltpu.VMEM((slots, tall, width), f32),
            pltpu.VMEM((slots, tall, width), bf16),
            pltpu.VMEM((tall, half), f32),
            pltpu.VMEM((slots, rows, half), f32),
            pltpu.VMEM((slots, rows, half), bf16),
            pltpu.VMEM((slots, rows, half), bf16),
            pltpu.VMEM((4, 2, rows, half // 2), bf16),
            pltpu.VMEM((4, 2, rows, half // 2), bf16),
            pltpu.VMEM((2, rows, half // 2), f32),
            dma, dma((6,)), dma((REACH,)), dma((REACH,)), dma((REACH,)),
            dma((2,)), dma((2,)), dma((5,)), dma((5,)), dma((7,)), dma((7,)),
            dma((kinds,)), dma((chips, kinds)), dma((chips, kinds)), dma((chips, kinds)),
            dma((chips, kinds)), dma((slots,)), dma((slots,)), dma((4, 2)), dma((4, 2)),
        ],
        compiler_params=pltpu.CompilerParams(
            collective_id=0, has_side_effects=True, vmem_limit_bytes=VMEM_LIMIT
        ),
    )(
        image_slot, slot_images.T, slot_count, features, gain_self, gain_query, gain_memory,
        gain_mlp, gain_head, w_qkv, w_self_out, w_query, w_memory, w_cross_out, w_fc1, w_fc2,
        w_head,
    )


def solution(mesh):
    placed = (
        P("pairs", None, "side"),
        P(),
        P("pairs", None),
        P("pairs"),
        P("side", None),
        P("side", None),
        P("side", None),
        P("side", None),
        P("side", None),
        P("side", None, None),
        P("side", None, None),
        P("side", None, None),
        P("side", None, None),
        P("side", None, None),
        P("side", "pairs", None),
        P("side", "pairs", None),
        P("side", None, None),
    )
    return jax.shard_map(
        on_device, mesh=mesh, in_specs=placed, out_specs=P("pairs", None, "side"), check_vma=False
    )
```
